128 devices in a mesh: rows: 16 (over z, y), cols: 8 (over x, core).
Axes of the slice: x: 4, y: 4, z: 4, core: 2. Of those that a mesh axis runs over, the one named last changes fastest.
Arguments:
- train_query: bfloat16 [8192, 8192], P('rows', 'cols'), may hold values from -0.0625 to 0.0625
- low_query: bfloat16 [8192, 64], P('rows'), may hold values from -0.0625 to 0.0625
- high_query: bfloat16 [64, 8192], P(None, 'cols'), may hold values from -0.75 to 0.75
- train_key: bfloat16 [8192, 512], P('rows', 'cols'), may hold values from -0.0625 to 0.0625
- low_key: bfloat16 [8192, 64], P('rows'), may hold values from -0.0625 to 0.0625
- high_key: bfloat16 [64, 512], P(None, 'cols'), may hold values from -0.75 to 0.75
- train_value: bfloat16 [8192, 512], P('rows', 'cols'), may hold values from -0.0625 to 0.0625
- low_value: bfloat16 [8192, 64], P('rows'), may hold values from -0.0625 to 0.0625
- high_value: bfloat16 [64, 512], P(None, 'cols'), may hold values from -0.75 to 0.75
- norm_train: float32 [8192], P(('rows', 'cols')), may hold values from 0.25 to 1.75
- norm_step: float32 [8192], P(('rows', 'cols')), may hold values from -0.3 to 0.3
Outputs:
- serving_query: bfloat16 [8192, 8192], P('cols')
- serving_key: bfloat16 [512, 8192], P('cols')
- serving_value: bfloat16 [512, 8192], P('cols')
- serve_norm: bfloat16 [8192], replicated
The draws below stay inside these ranges and needn't reach their ends.
All inputs are finite; a program needn't handle non-finite values.
Results may differ from the reference program's by a relative error of at most 0.001.
Values may be sent and summed in bfloat16 or wider, within the bound.
A program may use at most 128 MiB of HBM per device.

```python
import jax
import jax.numpy as jnp

D_MODEL = 8192
Q_DIM = 8192
KV_DIM = 512
RANK = 64


def steps_of(own_key, extent, cuts, smallest, high):
    def one(dim, shards_of):
        draws = jax.random.uniform(jax.random.fold_in(jax.random.fold_in(own_key, 6), dim), (shards_of,), jnp.float32, smallest / len(cuts), high / len(cuts))
        return jnp.repeat(jnp.exp(draws), extent[dim] // shards_of).reshape((-1,) + (1,) * (len(extent) - dim - 1))

    level = one(*cuts[0])
    for cut in cuts[1:]:
        level = level * one(*cut)
    return level


def normal_values(rng, extent, scale, limit, split=(), kind=jnp.bfloat16):
    gain = steps_of(rng, extent, split, -0.22, 0.18) if split else 1.0
    values = jax.random.normal(rng, extent, jnp.float32) * scale * gain
    return jnp.minimum(jnp.maximum(values, -limit), limit).astype(kind)


def setup_inputs(seed: int = 0) -> dict:
    splits = jax.random.split(jax.random.key(seed), 12)
    return {
        "train_query": normal_values(splits[0], (D_MODEL, Q_DIM), D_MODEL ** -0.5, 0.0625, ((0, 16), (1, 8))),
        "low_query": normal_values(splits[1], (D_MODEL, RANK), D_MODEL ** -0.5, 0.0625, ((0, 16),)),
        "high_query": normal_values(splits[2], (RANK, Q_DIM), RANK ** -0.5, 0.75, ((1, 8),)),
        "train_key": normal_values(splits[3], (D_MODEL, KV_DIM), D_MODEL ** -0.5, 0.0625, ((0, 16), (1, 8))),
        "low_key": normal_values(splits[4], (D_MODEL, RANK), D_MODEL ** -0.5, 0.0625, ((0, 16),)),
        "high_key": normal_values(splits[5], (RANK, KV_DIM), RANK ** -0.5, 0.75, ((1, 8),)),
        "train_value": normal_values(splits[6], (D_MODEL, KV_DIM), D_MODEL ** -0.5, 0.0625, ((0, 16), (1, 8))),
        "low_value": normal_values(splits[7], (D_MODEL, RANK), D_MODEL ** -0.5, 0.0625, ((0, 16),)),
        "high_value": normal_values(splits[8], (RANK, KV_DIM), RANK ** -0.5, 0.75, ((1, 8),)),
        "norm_train": jnp.clip(1.0 + 0.15 * jax.random.normal(splits[9], (D_MODEL,), jnp.float32), 0.25, 1.75),
        "norm_step": jnp.clip(jax.random.uniform(splits[10], (D_MODEL,), jnp.float32, -0.3, 0.3) * steps_of(splits[10], (D_MODEL,), ((0, 128),), -0.4, 0.0), -0.3, 0.3),
    }


mix_rate = 1.0


def reference(train_query, low_query, high_query, train_key, low_key, high_key, train_value, low_value, high_value, norm_train, norm_step):
    whole_query = train_query.astype(jnp.float32) + mix_rate * jnp.dot(low_query, high_query, preferred_element_type=jnp.float32)
    whole_key = train_key.astype(jnp.float32) + mix_rate * jnp.dot(low_key, high_key, preferred_element_type=jnp.float32)
    whole_value = train_value.astype(jnp.float32) + mix_rate * jnp.dot(low_value, high_value, preferred_element_type=jnp.float32)
    serving_query = whole_query.T.astype(jnp.bfloat16)
    serving_key = whole_key.T.astype(jnp.bfloat16)
    serving_value = whole_value.T.astype(jnp.bfloat16)
    serve_norm = (norm_train + norm_step).astype(jnp.bfloat16)
    return serving_query, serving_key, serving_value, serve_norm
```

```python
import jax
import jax.numpy as jnp
from jax import lax
from jax.experimental import pallas as pl
from jax.experimental.pallas import tpu as pltpu
from jax.sharding import PartitionSpec as P

MESH = pl.DeviceIdType.MESH

SIDE = 4
QUARTERS = 4
LINKS = ((0, 1), (0, -1), (1, 0), (-1, 0))


def shift(off, d, sign=1):
    return ((off[0] + sign * d[0]) % SIDE, (off[1] + sign * d[1]) % SIDE)


def sends_of(link):
    d = LINKS[link]
    along_y = d[0] == 0
    first = (0, 1) if along_y else (2, 3)
    second = (2, 3) if along_y else (0, 1)
    positive = sum(d) > 0
    fwd_first = first[0] if positive else first[1]
    fwd_second = second[0] if positive else second[1]

    def across(n):
        return (n % SIDE, 0) if along_y else (0, n % SIDE)

    def behind(off):
        return shift(off, d, -1)

    own = (0, 0)
    return (
        (own, first[0]),
        (own, first[1]),
        (own, second[0]),
        (own, second[1]),
        (behind(own), fwd_first),
        (across(-1), second[0]),
        (across(1), second[0]),
        (across(-1), second[1]),
        (across(1), second[1]),
        (behind(own), fwd_second),
        (across(2), second[0]),
        (across(2), second[1]),
        (behind(across(-1)), fwd_second),
        (behind(across(1)), fwd_second),
        (behind(across(2)), fwd_second),
    )


SENDS = tuple(sends_of(link) for link in range(len(LINKS)))
SLOTS = len(SENDS[0])
ARRIVES = {
    (shift(off, LINKS[link], -1), quarter): (link, slot)
    for link in range(len(LINKS))
    for slot, (off, quarter) in enumerate(SENDS[link])
}
assert len(ARRIVES) == len(LINKS) * SLOTS == (SIDE * SIDE - 1) * QUARTERS
ORDER = (0, 2, 1, 3)


def gather_kernel(
    wide, tall,
    train_query, low_query, high_query,
    train_key, low_key, high_key,
    train_value, low_value, high_value,
    norm_train, norm_step,
    whole, norm,
    tq, lq, hq, tk, lk, hk, tv, lv, hv, nt, ns, near, ring,
    load_sem, send_sem, recv_sem, near_send, near_recv, ring_send, ring_recv,
):
    row, col = lax.axis_index("rows"), lax.axis_index("cols")
    z, y = row // SIDE, row % SIDE
    part = wide // QUARTERS
    width = tq.shape[1]

    def device(d):
        return (((z + d[0]) % SIDE) * SIDE + (y + d[1]) % SIDE, col)

    def at(off):
        return ((z + off[0]) % SIDE) * SIDE + (y + off[1]) % SIDE

    barrier = pltpu.get_barrier_semaphore()
    n_cols = near.shape[0]
    peers = [device(d) for d in LINKS] + [(row, (col + j) % n_cols) for j in range(1, n_cols)]
    for peer in peers:
        pl.semaphore_signal(barrier, inc=1, device_id=peer, device_id_type=MESH)

    loads = {}

    def load(name, src, dst):
        copy = pltpu.make_async_copy(src, dst, load_sem.at[len(loads)])
        copy.start()
        loads[name] = copy

    load("lq", low_query, lq)
    load("hq", high_query, hq)
    for q in ORDER:
        cols = pl.ds(q * part, part)
        load(q, train_query.at[:, cols], tq.at[:, cols])
        if q == ORDER[0]:
            load("tk", train_key, tk)
            load("lk", low_key, lk)
            load("hk", high_key, hk)
        if q == ORDER[1]:
            load("tv", train_value, tv)
            load("lv", low_value, lv)
            load("hv", high_value, hv)
    load("nt", norm_train, nt)
    load("ns", norm_step, ns)

    def merged(train, high, low):
        return train.astype(jnp.float32) + lax.dot_general(
            high, low, (((0,), (0,)), ((), ())), preferred_element_type=jnp.float32
        )

    def compute(q):
        cols = pl.ds(q * part, part)
        loads[q].wait()
        whole[row, q, 0:part, :] = merged(tq[:, cols].T, hq[:, cols], lq[...]).astype(whole.dtype)
        train, low, high = (tk, lk, hk) if q < 2 else (tv, lv, hv)
        small = merged(train[...], high[...], low[...]).astype(whole.dtype)
        half = small.shape[0] // 2
        whole[row, q, part:, :] = small[(q % 2) * half : (q % 2 + 1) * half, :]

    sent = []

    def send(link, slot):
        off, q = SENDS[link][slot]
        unit = whole.at[at(off), q]
        copy = pltpu.make_async_remote_copy(
            src_ref=unit,
            dst_ref=unit,
            send_sem=send_sem.at[link, slot],
            recv_sem=recv_sem.at[link, slot],
            device_id=device(LINKS[link]),
            device_id_type=MESH,
        )
        copy.start()
        sent.append(copy)

    arrived = set()

    def wait_unit(link, slot):
        if (link, slot) in arrived:
            return
        arrived.add((link, slot))
        off, q = SENDS[link][slot]
        unit = whole.at[at(shift(off, LINKS[link], -1)), q]
        pltpu.make_async_remote_copy(
            src_ref=unit,
            dst_ref=unit,
            send_sem=send_sem.at[link, slot],
            recv_sem=recv_sem.at[link, slot],
            device_id=device(LINKS[link]),
            device_id_type=MESH,
        ).wait_recv()

    loads["lq"].wait()
    loads["hq"].wait()
    for n, q in enumerate(ORDER):
        if n == 0:
            for name in ("tk", "lk", "hk"):
                loads[name].wait()
        if n == 1:
            for name in ("tv", "lv", "hv"):
                loads[name].wait()
        compute(q)
        if n == 0:
            pl.semaphore_wait(barrier, len(peers))
        for link in range(len(LINKS)):
            for slot in range(QUARTERS):
                if SENDS[link][slot][1] == q and slot < 2:
                    send(link, slot)
    for slot in (2, 3):
        for link in range(len(LINKS)):
            send(link, slot)

    loads["nt"].wait()
    loads["ns"].wait()
    fresh = nt[...] + ns[...]
    near[col] = jnp.concatenate([fresh, fresh], axis=1)

    def near_copy(j):
        return pltpu.make_async_remote_copy(
            src_ref=near.at[col],
            dst_ref=near.at[col],
            send_sem=near_send.at[j],
            recv_sem=near_recv.at[j],
            device_id=(row, (col + j) % n_cols),
            device_id_type=MESH,
        )

    def near_wait(j):
        slot = (col + n_cols - j) % n_cols
        pltpu.make_async_remote_copy(
            src_ref=near.at[slot],
            dst_ref=near.at[slot],
            send_sem=near_send.at[j],
            recv_sem=near_recv.at[j],
            device_id=(row, (col + j) % n_cols),
            device_id_type=MESH,
        ).wait_recv()

    near_copies = [near_copy(j) for j in range(1, n_cols)]
    for copy in near_copies:
        copy.start()

    def ring_copy(n, src, d):
        return pltpu.make_async_remote_copy(
            src_ref=src,
            dst_ref=src,
            send_sem=ring_send.at[n],
            recv_sem=ring_recv.at[n],
            device_id=device(d),
            device_id_type=MESH,
        )

    def column(dz):
        return ring.at[pl.ds(((z + dz) % SIDE) * SIDE, SIDE)]

    ring_copies = []

    def ring_start(n, src, d):
        copy = ring_copy(n, src, d)
        copy.start()
        ring_copies.append(copy)

    for slot in range(QUARTERS, SLOTS):
        for link in range(len(LINKS)):
            wait_unit(*ARRIVES[SENDS[link][slot]])
            send(link, slot)
        if slot == QUARTERS:
            for j in range(1, n_cols):
                near_wait(j)
            lane = lax.broadcasted_iota(jnp.int32, (1, near.shape[2]), 1)
            lines = [
                jnp.where(lane < near.shape[2] // 2, near[2 * k], near[2 * k + 1])
                for k in range(n_cols // 2)
            ]
            ring[row] = jnp.concatenate(lines, axis=0)
        if slot == QUARTERS + 1:
            ring_start(0, ring.at[row], (0, 1))
            ring_start(1, ring.at[row], (0, -1))
        if slot == QUARTERS + 2:
            ring_copy(0, ring.at[at((0, -1))], (0, 1)).wait_recv()
            ring_copy(1, ring.at[at((0, 1))], (0, -1)).wait_recv()
            ring_start(2, ring.at[at((0, -1))], (0, 1))
        if slot == QUARTERS + 3:
            ring_copy(2, ring.at[at((0, -2))], (0, 1)).wait_recv()
            ring_start(3, column(0), (1, 0))
            ring_start(4, column(0), (-1, 0))
        if slot == QUARTERS + 4:
            ring_copy(3, column(-1), (1, 0)).wait_recv()
            ring_copy(4, column(1), (-1, 0)).wait_recv()
            ring_start(5, column(-1), (1, 0))
        if slot == QUARTERS + 5:
            ring_copy(5, column(-2), (1, 0)).wait_recv()
            norm[...] = jnp.concatenate([ring[i] for i in range(SIDE * SIDE)], axis=0).astype(norm.dtype)

    for slot in range(SLOTS):
        for link in range(len(LINKS)):
            wait_unit(link, slot)
    for copy in sent + near_copies + ring_copies:
        copy.wait_send()


def write_kernel(whole, norm, out_query, out_key, out_value, out_norm, sem, norm_sem):
    blocks, quarters, rows, cols = whole.shape
    part = out_query.shape[0] // quarters
    last = pltpu.make_async_copy(norm, out_norm, norm_sem)
    last.start()

    def copies(r):
        at = pl.ds(pl.multiple_of(r * cols, cols), cols)
        half = rows - part
        for q in range(quarters):
            yield pltpu.make_async_copy(
                whole.at[r, q, pl.ds(0, part)], out_query.at[pl.ds(q * part, part), at], sem.at[r, q]
            )
        for q in range(quarters):
            target = out_key if q < 2 else out_value
            yield pltpu.make_async_copy(
                whole.at[r, q, pl.ds(part, half)], target.at[pl.ds((q % 2) * half, half), at], sem.at[r, quarters + q]
            )

    @pl.loop(0, blocks)
    def _(r):
        for copy in copies(r):
            copy.start()

    @pl.loop(0, blocks)
    def _(r):
        for copy in copies(r):
            copy.wait()

    last.wait()


def body(
    train_query, low_query, high_query,
    train_key, low_key, high_key,
    train_value, low_value, high_value,
    norm_train, norm_step,
):
    n_rows, n_cols = lax.axis_size("rows"), lax.axis_size("cols")
    depth, wide = train_query.shape
    tall = train_key.shape[1]
    rank = low_query.shape[1]
    unit = (wide + 2 * tall) // QUARTERS
    line = 2 * norm_train.shape[0]
    dtype = train_query.dtype
    anywhere = pl.BlockSpec(memory_space=pl.ANY)
    dma = pltpu.SemaphoreType.DMA

    def kernel(*refs):
        gather_kernel(wide, tall, *refs)

    whole, norm = pl.pallas_call(
        kernel,
        out_shape=(
            jax.ShapeDtypeStruct((n_rows, QUARTERS, unit, depth), dtype),
            jax.ShapeDtypeStruct((n_rows * n_cols // 2, line), dtype),
        ),
        in_specs=[anywhere] * 11,
        out_specs=(pl.BlockSpec(memory_space=pltpu.VMEM), pl.BlockSpec(memory_space=pltpu.VMEM)),
        scratch_shapes=[
            pltpu.VMEM((depth, wide), dtype),
            pltpu.VMEM((rank, depth), dtype),
            pltpu.VMEM((rank, wide), dtype),
            pltpu.VMEM((tall, depth), dtype),
            pltpu.VMEM((rank, depth), dtype),
            pltpu.VMEM((rank, tall), dtype),
            pltpu.VMEM((tall, depth), dtype),
            pltpu.VMEM((rank, depth), dtype),
            pltpu.VMEM((rank, tall), dtype),
            pltpu.VMEM((1, line // 2), jnp.float32),
            pltpu.VMEM((1, line // 2), jnp.float32),
            pltpu.VMEM((n_cols, 1, line), jnp.float32),
            pltpu.VMEM((n_rows, n_cols // 2, line), jnp.float32),
            dma((15,)),
            dma((len(LINKS), SLOTS)),
            dma((len(LINKS), SLOTS)),
            dma((n_cols,)),
            dma((n_cols,)),
            dma((6,)),
            dma((6,)),
        ],
        compiler_params=pltpu.CompilerParams(
            collective_id=0, has_side_effects=True, vmem_limit_bytes=32 * 2**20
        ),
        name="gather",
    )(
        *(
            pltpu.with_memory_space_constraint(x, pltpu.HBM)
            for x in (
                train_query, low_query.T, high_query,
                train_key.T, low_key.T, high_key,
                train_value.T, low_value.T, high_value,
                norm_train.reshape(1, -1), norm_step.reshape(1, -1),
            )
        )
    )
    out_query, out_key, out_value, out_norm = pl.pallas_call(
        write_kernel,
        out_shape=(
            jax.ShapeDtypeStruct((wide, n_rows * depth), dtype),
            jax.ShapeDtypeStruct((tall, n_rows * depth), dtype),
            jax.ShapeDtypeStruct((tall, n_rows * depth), dtype),
            jax.ShapeDtypeStruct(norm.shape, dtype),
        ),
        in_specs=[anywhere] * 2,
        out_specs=[anywhere] * 4,
        scratch_shapes=[dma((n_rows, 2 * QUARTERS)), dma(())],
        compiler_params=pltpu.CompilerParams(vmem_limit_bytes=4 * 2**20),
        name="write",
    )(whole, norm)
    return out_query, out_key, out_value, out_norm.reshape(-1)


def solution(mesh):
    return jax.shard_map(
        body,
        mesh=mesh,
        in_specs=(
            P("rows", "cols"),
            P("rows", None),
            P(None, "cols"),
            P("rows", "cols"),
            P("rows", None),
            P(None, "cols"),
            P("rows", "cols"),
            P("rows", None),
            P(None, "cols"),
            P(("rows", "cols")),
            P(("rows", "cols")),
        ),
        out_specs=(P("cols", None), P("cols", None), P("cols", None), P()),
        check_vma=False,
    )
```

```python
import jax
import jax.numpy as jnp
from jax import lax
from jax.experimental import pallas as pl
from jax.experimental.pallas import tpu as pltpu
from jax.sharding import PartitionSpec as P

MESH = pl.DeviceIdType.MESH

SIDE = 4
QUARTERS = 4
CORES = 2
LINKS = ((0, 1), (0, -1), (1, 0), (-1, 0))
ORDER = (0, 2, 1, 3)
LATE = 1
SPLIT = 12


def shift(off, d, sign=1):
    return ((off[0] + sign * d[0]) % SIDE, (off[1] + sign * d[1]) % SIDE)


def sends_of(link):
    d = LINKS[link]
    along_y = d[0] == 0
    first = (0, 1) if along_y else (2, 3)
    second = (2, 3) if along_y else (0, 1)
    positive = sum(d) > 0
    fwd_first = first[0] if positive else first[1]
    fwd_second = second[0] if positive else second[1]

    def across(n):
        return (n % SIDE, 0) if along_y else (0, n % SIDE)

    def behind(off):
        return shift(off, d, -1)

    own = (0, 0)
    return tuple((own, q) for q in ORDER) + (
        (behind(own), fwd_first),
        (across(-1), second[0]),
        (across(1), second[0]),
        (across(-1), second[1]),
        (across(1), second[1]),
        (behind(own), fwd_second),
        (across(2), second[0]),
        (across(2), second[1]),
        (behind(across(-1)), fwd_second),
        (behind(across(1)), fwd_second),
        (behind(across(2)), fwd_second),
    )


SENDS = tuple(sends_of(link) for link in range(len(LINKS)))
SLOTS = len(SENDS[0])
UNITS = [(link, slot) for slot in range(SLOTS) for link in range(len(LINKS))]


def arriving(link, slot):
    off, quarter = SENDS[link][slot]
    return shift(off, LINKS[link], -1), quarter


ARRIVES = {arriving(*unit): unit for unit in UNITS}
assert len(ARRIVES) == len(UNITS) == (SIDE * SIDE - 1) * QUARTERS
LAST = [unit for unit in UNITS if unit[1] >= SPLIT]
assert all(ARRIVES[SENDS[link][slot]][1] < SPLIT for link, slot in LAST)


class Place:
    def __init__(self):
        self.row, self.col = lax.axis_index("rows"), lax.axis_index("cols")
        self.z, self.y = self.row // SIDE, self.row % SIDE
        self.x, self.core = self.col // CORES, self.col % CORES

    def at(self, off):
        return ((self.z + off[0]) % SIDE) * SIDE + (self.y + off[1]) % SIDE

    def neighbour(self, d):
        return (self.at(d), self.col)

    def partner(self):
        return (self.row, self.x * CORES + 1 - self.core)

    def along_x(self, n):
        return (self.row, ((self.x + n) % SIDE) * CORES + self.core)


def remote(src, dst, send_sem, recv_sem, device):
    return pltpu.make_async_remote_copy(
        src_ref=src, dst_ref=dst, send_sem=send_sem, recv_sem=recv_sem, device_id=device, device_id_type=MESH
    )


def signal_all(barrier, devices):
    for device in devices:
        pl.semaphore_signal(barrier, inc=1, device_id=device, device_id_type=MESH)


def gather_kernel(
    train_query, low_query, high_query,
    train_key, low_key, high_key,
    train_value, low_value, high_value,
    norm_train, norm_step,
    whole, lines,
    tq, lq, hq, tk, lk, hk, tv, lv, hv, nt, ns, pair, ring,
    load_sem, send_sem, recv_sem, pair_sem, ring_send, ring_recv,
):
    me = Place()
    wide = tq.shape[1]
    part = wide // QUARTERS

    barrier = pltpu.get_barrier_semaphore()
    peers = [me.neighbour(d) for d in LINKS] + [me.partner()]
    signal_all(barrier, peers)

    loads = {}

    def load(name, src, dst):
        copy = pltpu.make_async_copy(src, dst, load_sem.at[len(loads)])
        copy.start()
        loads[name] = copy

    load("lq", low_query, lq)
    load("hq", high_query, hq)
    for n, q in enumerate(ORDER):
        cols = pl.ds(q * part, part)
        load(q, train_query.at[:, cols], tq.at[:, cols])
        if n == 0:
            load("tk", train_key, tk)
            load("lk", low_key, lk)
            load("hk", high_key, hk)
        if n == 1:
            load("tv", train_value, tv)
            load("lv", low_value, lv)
            load("hv", high_value, hv)
    load("nt", norm_train, nt)
    load("ns", norm_step, ns)

    def merged(train, high, low):
        return train.astype(jnp.float32) + lax.dot_general(
            high, low, (((0,), (0,)), ((), ())), preferred_element_type=jnp.float32
        )

    def compute(q):
        cols = pl.ds(q * part, part)
        loads[q].wait()
        whole[me.row, q, 0:part, :] = merged(tq[:, cols].T, hq[:, cols], lq[...]).astype(whole.dtype)
        train, low, high = (tk, lk, hk) if q < 2 else (tv, lv, hv)
        small = merged(train[...], high[...], low[...]).astype(whole.dtype)
        half = small.shape[0] // 2
        whole[me.row, q, part:, :] = small[(q % 2) * half : (q % 2 + 1) * half, :]

    def unit_copy(link, slot, what):
        off, q = what
        unit = whole.at[me.at(off), q]
        return remote(unit, unit, send_sem.at[link, slot], recv_sem.at[link, slot], me.neighbour(LINKS[link]))

    def send(link, slot):
        unit_copy(link, slot, SENDS[link][slot]).start()

    def arrive(link, slot):
        unit_copy(link, slot, arriving(link, slot)).wait_recv()

    loads["lq"].wait()
    loads["hq"].wait()
    for n, q in enumerate(ORDER):
        if n == 0:
            for name in ("tk", "lk", "hk"):
                loads[name].wait()
        if n == 1:
            for name in ("tv", "lv", "hv"):
                loads[name].wait()
        compute(q)
        if n == 0:
            pl.semaphore_wait(barrier, len(peers))
        for link in range(len(LINKS)):
            send(link, n)

    loads["nt"].wait()
    loads["ns"].wait()
    fresh = nt[...] + ns[...]
    pair[me.core] = jnp.concatenate([fresh, fresh], axis=1)

    def pair_copy(slot):
        return remote(pair.at[slot], pair.at[slot], pair_sem.at[0], pair_sem.at[1], me.partner())

    pair_copy(me.core).start()

    def ring_copy(n, src, d):
        return remote(src, src, ring_send.at[n], ring_recv.at[n], me.neighbour(d))

    def column(dz):
        return ring.at[pl.ds(((me.z + dz) % SIDE) * SIDE, SIDE)]

    ring_copies = []

    def ring_start(n, src, d):
        copy = ring_copy(n, src, d)
        copy.start()
        ring_copies.append(copy)

    def norm_step_of(slot):
        step = slot - QUARTERS
        if step == 0:
            pair_copy(1 - me.core).wait_recv()
            lane = lax.broadcasted_iota(jnp.int32, (1, pair.shape[2]), 1)
            ring[me.row] = jnp.where(lane < pair.shape[2] // CORES, pair[0], pair[1])
        if step == 1:
            ring_start(0, ring.at[me.row], (0, 1))
            ring_start(1, ring.at[me.row], (0, -1))
        if step == 2:
            ring_copy(0, ring.at[me.at((0, -1))], (0, 1)).wait_recv()
            ring_copy(1, ring.at[me.at((0, 1))], (0, -1)).wait_recv()
            ring_start(2, ring.at[me.at((0, -1))], (0, 1))
        if step == 3:
            ring_copy(2, ring.at[me.at((0, -2))], (0, 1)).wait_recv()
            ring_start(3, column(0), (1, 0))
            ring_start(4, column(0), (-1, 0))
        if step == 4:
            ring_copy(3, column(-1), (1, 0)).wait_recv()
            ring_copy(4, column(1), (-1, 0)).wait_recv()
            ring_start(5, column(-1), (1, 0))
        if step == 5:
            ring_copy(5, column(-2), (1, 0)).wait_recv()
            lines[...] = jnp.concatenate([ring[i] for i in range(SIDE * SIDE)], axis=0)

    arrived = set()

    def arrive_once(unit):
        if unit not in arrived:
            arrived.add(unit)
            arrive(*unit)

    for slot in range(QUARTERS, SPLIT):
        for link in range(len(LINKS)):
            arrive_once(ARRIVES[SENDS[link][slot]])
            send(link, slot)
        norm_step_of(slot)
    for unit in LAST:
        arrive_once(ARRIVES[SENDS[unit[0]][unit[1]]])

    @pl.when(me.core != LATE)
    def _():
        for unit in LAST:
            send(*unit)

    for unit in UNITS:
        if unit not in LAST:
            arrive_once(unit)

    @pl.when(me.core != LATE)
    def _():
        for unit in LAST:
            arrive(*unit)
        for unit in LAST:
            unit_copy(*unit, SENDS[unit[0]][unit[1]]).wait_send()

    for unit in UNITS:
        if unit not in LAST:
            unit_copy(*unit, SENDS[unit[0]][unit[1]]).wait_send()
    pair_copy(me.core).wait_send()
    for copy in ring_copies:
        copy.wait_send()


def finish_kernel(
    whole, lines, token,
    rest, norm,
    all_lines, ordered, send_sem, recv_sem, line_send, line_recv, norm_sem,
):
    del token
    me = Place()
    barrier = pltpu.get_barrier_semaphore()
    norm_copy = remote(norm, norm, norm_sem.at[0], norm_sem.at[1], me.partner())

    @pl.when(me.core == LATE)
    def _():
        signal_all(barrier, [me.neighbour(d) for d in LINKS] + [me.partner()])
        pl.semaphore_wait(barrier, len(LINKS))
        copies = []
        for link, slot in LAST:
            off, q = SENDS[link][slot]
            n = slot - SPLIT
            copy = remote(
                whole.at[me.at(off), q],
                rest.at[link, n],
                send_sem.at[link, n],
                recv_sem.at[link, n],
                me.neighbour(LINKS[link]),
            )
            copy.start()
            copies.append(copy)
        norm_copy.wait_recv()
        for copy in copies:
            copy.wait()

    @pl.when(me.core != LATE)
    def _():
        steps = range(1, SIDE)
        signal_all(barrier, [me.along_x(n) for n in steps])
        pl.semaphore_wait(barrier, len(steps) + 1)

        def line_copy(n, x):
            return remote(lines, all_lines.at[x], line_send.at[n - 1], line_recv.at[n - 1], me.along_x(n))

        for n in steps:
            line_copy(n, me.x).start()
        all_lines[me.x] = lines[...]
        for n in steps:
            line_copy(n, (me.x - n) % SIDE).wait_recv()
        for x in range(SIDE):
            ordered[pl.Slice(x, SIDE * SIDE, SIDE), :] = all_lines[x]
        norm[...] = ordered[...].astype(norm.dtype)
        norm_copy.start()
        for n in steps:
            line_copy(n, me.x).wait_send()
        norm_copy.wait_send()


def out_copies(source, block, quarter, outs, sem):
    out_query, out_key, out_value = outs
    rows, depth = source.shape
    part = out_query.shape[0] // QUARTERS
    half = rows - part
    at = pl.ds(pl.multiple_of(block * depth, depth), depth)
    small = (out_key if quarter < 2 else out_value).at[pl.ds((quarter % 2) * half, half), at]
    return (
        pltpu.make_async_copy(source.at[pl.ds(0, part)], out_query.at[pl.ds(quarter * part, part), at], sem.at[0]),
        pltpu.make_async_copy(source.at[pl.ds(part, half)], small, sem.at[1]),
    )


def run_copies(copies):
    for copy in copies:
        copy.start()
    for copy in copies:
        copy.wait()


BLOCKS = [(dz, dy) for dz in range(SIDE) for dy in range(SIDE)]
PIECES = [(off, q) for off in BLOCKS for q in range(QUARTERS)]


def write_kernel(whole, out_query, out_key, out_value, token, sem):
    me = Place()
    outs = (out_query, out_key, out_value)
    token[...] = jnp.zeros_like(token)
    late = {arriving(*unit) for unit in LAST}

    @pl.when(me.core == LATE)
    def _():
        copies = []
        for n, (off, q) in enumerate(PIECES):
            if (off, q) not in late:
                block = me.at(off)
                copies.extend(out_copies(whole.at[block, q], block, q, outs, sem.at[n]))
        run_copies(copies)


def write_rest_kernel(
    whole, rest, norm, in_query, in_key, in_value, out_query, out_key, out_value, out_norm, sem, norm_sem
):
    del in_query, in_key, in_value
    me = Place()
    outs = (out_query, out_key, out_value)
    norm_copy = pltpu.make_async_copy(norm, out_norm, norm_sem)
    norm_copy.start()

    @pl.when(me.core == LATE)
    def _():
        copies = []
        for n, (link, slot) in enumerate(LAST):
            off, q = arriving(link, slot)
            copies.extend(out_copies(rest.at[link, slot - SPLIT], me.at(off), q, outs, sem.at[n]))
        run_copies(copies)

    @pl.when(me.core != LATE)
    def _():
        copies = []
        for n, (off, q) in enumerate(PIECES):
            block = me.at(off)
            copies.extend(out_copies(whole.at[block, q], block, q, outs, sem.at[n]))
        run_copies(copies)

    norm_copy.wait()


def body(
    train_query, low_query, high_query,
    train_key, low_key, high_key,
    train_value, low_value, high_value,
    norm_train, norm_step,
):
    n_rows, n_cols = lax.axis_size("rows"), lax.axis_size("cols")
    depth, wide = train_query.shape
    tall = train_key.shape[1]
    rank = low_query.shape[1]
    unit = (wide + 2 * tall) // QUARTERS
    values = norm_train.shape[0]
    line = CORES * values
    dtype = train_query.dtype
    f32 = jnp.float32
    anywhere = pl.BlockSpec(memory_space=pl.ANY)
    vmem = pl.BlockSpec(memory_space=pltpu.VMEM)
    dma = pltpu.SemaphoreType.DMA
    shape = jax.ShapeDtypeStruct
    outs = [shape((wide, n_rows * depth), dtype)] + [shape((tall, n_rows * depth), dtype)] * 2

    def pin(space, *arrays):
        return [pltpu.with_memory_space_constraint(a, space) for a in arrays]

    whole, lines = pl.pallas_call(
        gather_kernel,
        out_shape=(shape((n_rows, QUARTERS, unit, depth), dtype), shape((n_rows, line), f32)),
        in_specs=[anywhere] * 11,
        out_specs=(vmem, vmem),
        scratch_shapes=[
            pltpu.VMEM((depth, wide), dtype),
            pltpu.VMEM((rank, depth), dtype),
            pltpu.VMEM((rank, wide), dtype),
            pltpu.VMEM((tall, depth), dtype),
            pltpu.VMEM((rank, depth), dtype),
            pltpu.VMEM((rank, tall), dtype),
            pltpu.VMEM((tall, depth), dtype),
            pltpu.VMEM((rank, depth), dtype),
            pltpu.VMEM((rank, tall), dtype),
            pltpu.VMEM((1, values), f32),
            pltpu.VMEM((1, values), f32),
            pltpu.VMEM((CORES, 1, line), f32),
            pltpu.VMEM((n_rows, 1, line), f32),
            dma((14,)),
            dma((len(LINKS), SLOTS)),
            dma((len(LINKS), SLOTS)),
            dma((2,)),
            dma((6,)),
            dma((6,)),
        ],
        compiler_params=pltpu.CompilerParams(
            collective_id=0, has_side_effects=True, vmem_limit_bytes=24 * 2**20
        ),
        name="gather",
    )(
        *pin(
            pltpu.HBM,
            train_query, low_query.T, high_query,
            train_key.T, low_key.T, high_key,
            train_value.T, low_value.T, high_value,
            norm_train.reshape(1, -1), norm_step.reshape(1, -1),
        )
    )
    out_query, out_key, out_value, token = pl.pallas_call(
        write_kernel,
        out_shape=(*outs, shape((8, 128), f32)),
        in_specs=[vmem],
        out_specs=[anywhere] * 3 + [vmem],
        scratch_shapes=[dma((len(PIECES), 2))],
        compiler_params=pltpu.CompilerParams(vmem_limit_bytes=4 * 2**20),
        name="write",
    )(*pin(pltpu.VMEM, whole))
    rest, norm = pl.pallas_call(
        finish_kernel,
        out_shape=(
            shape((len(LINKS), SLOTS - SPLIT, unit, depth), dtype),
            shape((n_rows * n_cols // CORES, line), dtype),
        ),
        in_specs=[vmem] * 3,
        out_specs=(vmem, vmem),
        scratch_shapes=[
            pltpu.VMEM((SIDE, n_rows, line), f32),
            pltpu.VMEM((n_rows * SIDE, line), f32),
            dma((len(LINKS), SLOTS - SPLIT)),
            dma((len(LINKS), SLOTS - SPLIT)),
            dma((SIDE - 1,)),
            dma((SIDE - 1,)),
            dma((2,)),
        ],
        compiler_params=pltpu.CompilerParams(
            collective_id=1, has_side_effects=True, vmem_limit_bytes=8 * 2**20
        ),
        name="finish",
    )(*pin(pltpu.VMEM, whole, lines, token))
    out_query, out_key, out_value, out_norm = pl.pallas_call(
        write_rest_kernel,
        out_shape=(*outs, shape(norm.shape, dtype)),
        in_specs=[vmem] * 3 + [anywhere] * 3,
        out_specs=[anywhere] * 4,
        input_output_aliases={3: 0, 4: 1, 5: 2},
        scratch_shapes=[dma((len(PIECES), 2)), dma(())],
        compiler_params=pltpu.CompilerParams(vmem_limit_bytes=4 * 2**20),
        name="write_rest",
    )(*pin(pltpu.VMEM, whole, rest, norm), *pin(pltpu.HBM, out_query, out_key, out_value))
    return out_query, out_key, out_value, out_norm.reshape(-1)


def solution(mesh):
    return jax.shard_map(
        body,
        mesh=mesh,
        in_specs=(
            P("rows", "cols"),
            P("rows", None),
            P(None, "cols"),
            P("rows", "cols"),
            P("rows", None),
            P(None, "cols"),
            P("rows", "cols"),
            P("rows", None),
            P(None, "cols"),
            P(("rows", "cols")),
            P(("rows", "cols")),
        ),
        out_specs=(P("cols", None), P("cols", None), P("cols", None), P()),
        check_vma=False,
    )
```

```python
import jax
import jax.numpy as jnp
from jax import lax
from jax.experimental import pallas as pl
from jax.experimental.pallas import tpu as pltpu
from jax.sharding import PartitionSpec as P

MESH = pl.DeviceIdType.MESH

SIDE = 4
QUARTERS = 4
CORES = 2
LINKS = ((0, 1), (0, -1), (1, 0), (-1, 0))
ORDER = (0, 2, 1, 3)


def shift(off, d, sign=1):
    return ((off[0] + sign * d[0]) % SIDE, (off[1] + sign * d[1]) % SIDE)


def sends_of(link):
    d = LINKS[link]
    along_y = d[0] == 0
    first = (0, 1) if along_y else (2, 3)
    second = (2, 3) if along_y else (0, 1)
    positive = sum(d) > 0
    fwd_first = first[0] if positive else first[1]
    fwd_second = second[0] if positive else second[1]

    def across(n):
        return (n % SIDE, 0) if along_y else (0, n % SIDE)

    def behind(off):
        return shift(off, d, -1)

    own = (0, 0)
    return tuple((own, q) for q in ORDER) + (
        (behind(own), fwd_first),
        (across(-1), second[0]),
        (across(1), second[0]),
        (across(-1), second[1]),
        (across(1), second[1]),
        (behind(own), fwd_second),
        (across(2), second[0]),
        (across(2), second[1]),
        (behind(across(-1)), fwd_second),
        (behind(across(1)), fwd_second),
        (behind(across(2)), fwd_second),
    )


SENDS = tuple(sends_of(link) for link in range(len(LINKS)))
SLOTS = len(SENDS[0])
UNITS = [(link, slot) for slot in range(SLOTS) for link in range(len(LINKS))]


def arriving(link, slot):
    off, quarter = SENDS[link][slot]
    return shift(off, LINKS[link], -1), quarter


ARRIVES = {arriving(*unit): unit for unit in UNITS}
assert len(ARRIVES) == len(UNITS) == (SIDE * SIDE - 1) * QUARTERS
PASSED = []
for _link, _slot in UNITS:
    _what = SENDS[_link][_slot]
    if _what[0] != (0, 0) and ARRIVES[_what] not in PASSED:
        PASSED.append(ARRIVES[_what])
KEPT = [unit for unit in UNITS if unit not in PASSED]
assert len(KEPT) % QUARTERS == 0


class Place:
    def __init__(self):
        self.row, self.col = lax.axis_index("rows"), lax.axis_index("cols")
        self.z, self.y = self.row // SIDE, self.row % SIDE
        self.x, self.core = self.col // CORES, self.col % CORES

    def at(self, off):
        return ((self.z + off[0]) % SIDE) * SIDE + (self.y + off[1]) % SIDE

    def neighbour(self, d):
        return (self.at(d), self.col)

    def partner(self):
        return (self.row, self.x * CORES + 1 - self.core)

    def along_x(self, n):
        return (self.row, ((self.x + n) % SIDE) * CORES + self.core)


def remote(src, dst, send_sem, recv_sem, device):
    return pltpu.make_async_remote_copy(
        src_ref=src, dst_ref=dst, send_sem=send_sem, recv_sem=recv_sem, device_id=device, device_id_type=MESH
    )


def signal_all(barrier, devices):
    for device in devices:
        pl.semaphore_signal(barrier, inc=1, device_id=device, device_id_type=MESH)


def gather_kernel(
    train_query, low_query, high_query,
    train_key, low_key, high_key,
    train_value, low_value, high_value,
    norm_train, norm_step,
    whole, norm,
    tq, lq, hq, tk, lk, hk, tv, lv, hv, nt, ns, pair, ring, lines, all_lines, ordered,
    load_sem, send_sem, recv_sem, kept_sem, pair_sem, ring_send, ring_recv, line_sem, norm_send, norm_recv,
):
    me = Place()
    wide = tq.shape[1]
    part = wide // QUARTERS
    blocks = whole.shape[0]
    leader = (me.z == 0) & (me.y == 0)
    steps = range(1, SIDE)

    barrier = pltpu.get_barrier_semaphore()
    peers = [me.neighbour(d) for d in LINKS] + [me.partner()]
    signal_all(barrier, peers)

    @pl.when(leader)
    def _():
        signal_all(barrier, [me.along_x(n) for n in steps])

    loads = {}

    def load(name, src, dst):
        copy = pltpu.make_async_copy(src, dst, load_sem.at[len(loads)])
        copy.start()
        loads[name] = copy

    pieces = [(ORDER[0], 0, part // 2), (ORDER[0], part // 2, part)] + [(q, 0, part) for q in ORDER[1:]]
    load("lq", low_query, lq)
    load("hq", high_query, hq)
    for n, (q, start, end) in enumerate(pieces):
        cols = pl.ds(q * part + start, end - start)
        load(n, train_query.at[:, cols], tq.at[:, cols])
        if n == 1:
            load("tk", train_key, tk)
            load("lk", low_key, lk)
            load("hk", high_key, hk)
        if n == 2:
            load("tv", train_value, tv)
            load("lv", low_value, lv)
            load("hv", high_value, hv)
    load("nt", norm_train, nt)
    load("ns", norm_step, ns)

    def merged(train, high, low):
        return train.astype(jnp.float32) + lax.dot_general(
            high, low, (((0,), (0,)), ((), ())), preferred_element_type=jnp.float32
        )

    def unit_copy(link, slot, what, rows=slice(None)):
        off, q = what
        unit = whole.at[me.at(off), q, rows]
        sem = recv_sem.at[PASSED.index((link, slot))] if (link, slot) in PASSED else kept_sem
        return remote(unit, unit, send_sem, sem, me.neighbour(LINKS[link]))

    def send(link, slot, rows=slice(None)):
        unit_copy(link, slot, SENDS[link][slot], rows).start()

    arrived = set()

    def arrive(unit):
        if unit not in arrived:
            arrived.add(unit)
            unit_copy(*unit, arriving(*unit)).wait_recv()

    loads["lq"].wait()
    loads["hq"].wait()
    for n, (q, start, end) in enumerate(pieces):
        cols = pl.ds(q * part + start, end - start)
        loads[n].wait()
        whole[me.row, q, start:end, :] = merged(tq[:, cols].T, hq[:, cols], lq[...]).astype(whole.dtype)
        if n == 0:

            @pl.when(leader)
            def _():
                pl.semaphore_wait(barrier, len(peers) + len(steps))

            @pl.when(jnp.logical_not(leader))
            def _():
                pl.semaphore_wait(barrier, len(peers))

        if end == part:
            if n == 1:
                for name in ("tk", "lk", "hk"):
                    loads[name].wait()
            if n == 2:
                for name in ("tv", "lv", "hv"):
                    loads[name].wait()
            train, low, high = (tk, lk, hk) if q < 2 else (tv, lv, hv)
            small = merged(train[...], high[...], low[...]).astype(whole.dtype)
            half = small.shape[0] // 2
            whole[me.row, q, part:, :] = small[(q % 2) * half : (q % 2 + 1) * half, :]
        for link in range(len(LINKS)):
            if n == 0:
                send(link, 0, pl.ds(0, end))
            elif n == 1:
                send(link, 0, pl.ds(start, whole.shape[2] - start))
            else:
                send(link, ORDER.index(q))

    loads["nt"].wait()
    loads["ns"].wait()
    fresh = nt[...] + ns[...]
    pair[me.core] = jnp.concatenate([fresh, fresh], axis=1)

    def pair_copy(slot):
        return remote(pair.at[slot], pair.at[slot], pair_sem.at[0], pair_sem.at[1], me.partner())

    pair_copy(me.core).start()

    def ring_copy(n, src, d):
        return remote(src, src, ring_send, ring_recv.at[n], me.neighbour(d))

    def column(dz):
        return ring.at[pl.ds(((me.z + dz) % SIDE) * SIDE, SIDE)]

    def line_copy(n):
        return remote(lines, all_lines.at[me.x], line_sem.at[0], line_sem.at[1], me.along_x(n))

    def norm_copy(link):
        return remote(norm, norm, norm_send.at[link], norm_recv, me.neighbour(LINKS[link]))

    passes = [((0, 0), (0, 1, 2, 3)), ((0, 1), (0, 2, 3)), ((0, 3), (2, 3)), ((0, 2), (2, 3))]
    passes += [((1, y), (2,)) for y in range(SIDE)]

    def pass_norm(places):
        for (z, y), links in passes:
            if (z, y) in places:

                @pl.when((me.z == z) & (me.y == y))
                def _():
                    if (z, y) != (0, 0):
                        norm_copy(0).wait_recv()
                    for link in links:
                        norm_copy(link).start()

    def norm_step_of(step):
        if step == 0:
            pair_copy(1 - me.core).wait_recv()
            lane = lax.broadcasted_iota(jnp.int32, (1, pair.shape[2]), 1)
            ring[me.row] = jnp.where(lane < pair.shape[2] // CORES, pair[0], pair[1])
        if step == 1:
            ring_copy(0, ring.at[me.row], (0, 1)).start()
            ring_copy(1, ring.at[me.row], (0, -1)).start()
        if step == 2:
            ring_copy(0, ring.at[me.at((0, -1))], (0, 1)).wait_recv()
            ring_copy(1, ring.at[me.at((0, 1))], (0, -1)).wait_recv()
            ring_copy(2, ring.at[me.at((0, -1))], (0, 1)).start()
        if step == 3:
            ring_copy(2, ring.at[me.at((0, -2))], (0, 1)).wait_recv()
            ring_copy(3, column(0), (1, 0)).start()
            ring_copy(4, column(0), (-1, 0)).start()
        if step == 4:
            ring_copy(3, column(-1), (1, 0)).wait_recv()
            ring_copy(4, column(1), (-1, 0)).wait_recv()
            ring_copy(5, column(-1), (1, 0)).start()
        if step == 5:
            ring_copy(5, column(-2), (1, 0)).wait_recv()

            @pl.when(leader)
            def _():
                lines[...] = jnp.concatenate([ring[i] for i in range(blocks)], axis=0)
                all_lines[me.x] = lines[...]
                for n in steps:
                    line_copy(n).start()

        if step == 7:

            @pl.when(leader)
            def _():
                three = all_lines.at[pl.ds(0, len(steps))]
                every = remote(three, three, line_sem.at[0], line_sem.at[1], me.along_x(1))
                every.wait_recv()
                for x in range(SIDE):
                    ordered[pl.Slice(x, blocks, SIDE), :] = all_lines[x]
                norm[...] = ordered[...].astype(norm.dtype)

            pass_norm([(0, 0)])
        if step == 8:
            pass_norm([(0, 1), (0, 3)])
        if step == 9:
            pass_norm([(0, 2)])
        if step == 10:
            pass_norm([(1, y) for y in range(SIDE)])

    for slot in range(QUARTERS, SLOTS):
        for link in range(len(LINKS)):
            arrive(ARRIVES[SENDS[link][slot]])
            send(link, slot)
        norm_step_of(slot - QUARTERS)

    @pl.when(me.z >= 2)
    def _():
        norm_copy(0).wait_recv()

    for unit in PASSED:
        arrive(unit)
    kept = whole.at[pl.ds(0, len(KEPT) // QUARTERS)]
    remote(kept, kept, send_sem, kept_sem, me.partner()).wait_recv()
    sent = whole.at[pl.ds(0, len(UNITS) // QUARTERS)]
    remote(sent, sent, send_sem, kept_sem, me.partner()).wait_send()
    pair_copy(me.core).wait_send()
    around = ring.at[pl.ds(0, blocks - 1)]
    remote(around, around, ring_send, ring_recv.at[0], me.partner()).wait_send()

    @pl.when(leader)
    def _():
        three = all_lines.at[pl.ds(0, len(steps))]
        remote(three, three, line_sem.at[0], line_sem.at[1], me.along_x(1)).wait_send()

    for (z, y), links in passes:

        @pl.when((me.z == z) & (me.y == y))
        def _():
            for link in links:
                norm_copy(link).wait_send()


def write_kernel(whole, norm, out_query, out_key, out_value, out_norm, sem):
    blocks, quarters, rows, depth = whole.shape
    part = out_query.shape[0] // quarters
    half = rows - part
    outs = (out_query, out_key, out_value, out_norm)
    pltpu.make_async_copy(norm, out_norm, sem.at[3]).start()

    @pl.loop(0, blocks)
    def _(r):
        at = pl.ds(pl.multiple_of(r * depth, depth), depth)
        for q in range(quarters):
            pltpu.make_async_copy(
                whole.at[r, q, pl.ds(0, part)], out_query.at[pl.ds(q * part, part), at], sem.at[0]
            ).start()
        for q in range(quarters):
            n = 1 + q // 2
            pltpu.make_async_copy(
                whole.at[r, q, pl.ds(part, half)], outs[n].at[pl.ds((q % 2) * half, half), at], sem.at[n]
            ).start()

    for n, out in enumerate(outs):
        pltpu.make_async_copy(out, out, sem.at[n]).wait()


def body(
    train_query, low_query, high_query,
    train_key, low_key, high_key,
    train_value, low_value, high_value,
    norm_train, norm_step,
):
    n_rows, n_cols = lax.axis_size("rows"), lax.axis_size("cols")
    depth, wide = train_query.shape
    tall = train_key.shape[1]
    rank = low_query.shape[1]
    unit = (wide + 2 * tall) // QUARTERS
    values = norm_train.shape[0]
    line = CORES * values
    dtype = train_query.dtype
    f32 = jnp.float32
    anywhere = pl.BlockSpec(memory_space=pl.ANY)
    vmem = pl.BlockSpec(memory_space=pltpu.VMEM)
    dma = pltpu.SemaphoreType.DMA
    shape = jax.ShapeDtypeStruct

    def pin(space, *arrays):
        return [pltpu.with_memory_space_constraint(a, space) for a in arrays]

    whole, norm = pl.pallas_call(
        gather_kernel,
        out_shape=(
            shape((n_rows, QUARTERS, unit, depth), dtype),
            shape((n_rows * n_cols // CORES, line), dtype),
        ),
        in_specs=[anywhere] * 11,
        out_specs=(vmem, vmem),
        scratch_shapes=[
            pltpu.VMEM((depth, wide), dtype),
            pltpu.VMEM((rank, depth), dtype),
            pltpu.VMEM((rank, wide), dtype),
            pltpu.VMEM((tall, depth), dtype),
            pltpu.VMEM((rank, depth), dtype),
            pltpu.VMEM((rank, tall), dtype),
            pltpu.VMEM((tall, depth), dtype),
            pltpu.VMEM((rank, depth), dtype),
            pltpu.VMEM((rank, tall), dtype),
            pltpu.VMEM((1, values), f32),
            pltpu.VMEM((1, values), f32),
            pltpu.VMEM((CORES, 1, line), f32),
            pltpu.VMEM((n_rows, 1, line), f32),
            pltpu.VMEM((n_rows, line), f32),
            pltpu.VMEM((SIDE, n_rows, line), f32),
            pltpu.VMEM((SIDE * n_rows, line), f32),
            dma((15,)),
            dma(()),
            dma((len(PASSED),)),
            dma(()),
            dma((2,)),
            dma(()),
            dma((6,)),
            dma((2,)),
            dma((len(LINKS),)),
            dma(()),
        ],
        compiler_params=pltpu.CompilerParams(
            collective_id=0, has_side_effects=True, vmem_limit_bytes=24 * 2**20
        ),
        name="gather",
    )(
        *pin(
            pltpu.HBM,
            train_query, low_query.T, high_query,
            train_key.T, low_key.T, high_key,
            train_value.T, low_value.T, high_value,
            norm_train.reshape(1, -1), norm_step.reshape(1, -1),
        )
    )
    out_query, out_key, out_value, out_norm = pl.pallas_call(
        write_kernel,
        out_shape=(
            shape((wide, n_rows * depth), dtype),
            shape((tall, n_rows * depth), dtype),
            shape((tall, n_rows * depth), dtype),
            shape(norm.shape, dtype),
        ),
        in_specs=[vmem] * 2,
        out_specs=[anywhere] * 4,
        scratch_shapes=[dma((4,))],
        compiler_params=pltpu.CompilerParams(vmem_limit_bytes=4 * 2**20),
        name="write",
    )(*pin(pltpu.VMEM, whole, norm))
    return out_query, out_key, out_value, out_norm.reshape(-1)


def solution(mesh):
    return jax.shard_map(
        body,
        mesh=mesh,
        in_specs=(
            P("rows", "cols"),
            P("rows", None),
            P(None, "cols"),
            P("rows", "cols"),
            P("rows", None),
            P(None, "cols"),
            P("rows", "cols"),
            P("rows", None),
            P(None, "cols"),
            P(("rows", "cols")),
            P(("rows", "cols")),
        ),
        out_specs=(P("cols", None), P("cols", None), P("cols", None), P()),
        check_vma=False,
    )
```

```python
import jax
import jax.numpy as jnp
from jax import lax
from jax.experimental import pallas as pl
from jax.experimental.pallas import tpu as pltpu
from jax.sharding import PartitionSpec as P

MESH = pl.DeviceIdType.MESH

SIDE = 4
QUARTERS = 4
CORES = 2
LINKS = ((0, 1), (0, -1), (1, 0), (-1, 0))
LEADER = 2
ORDER = (0, 2, 1, 3)


def shift(off, d, sign=1):
    return ((off[0] + sign * d[0]) % SIDE, (off[1] + sign * d[1]) % SIDE)


def sends_of(link):
    d = LINKS[link]
    along_y = d[0] == 0
    first = (0, 1) if along_y else (2, 3)
    second = (2, 3) if along_y else (0, 1)
    positive = sum(d) > 0
    fwd_first = first[0] if positive else first[1]
    fwd_second = second[0] if positive else second[1]

    def across(n):
        return (n % SIDE, 0) if along_y else (0, n % SIDE)

    def behind(off):
        return shift(off, d, -1)

    own = (0, 0)
    return tuple((own, q) for q in ORDER) + (
        (behind(own), fwd_first),
        (across(-1), second[0]),
        (across(1), second[0]),
        (across(-1), second[1]),
        (across(1), second[1]),
        (behind(own), fwd_second),
        (across(2), second[0]),
        (across(2), second[1]),
        (behind(across(-1)), fwd_second),
        (behind(across(1)), fwd_second),
        (behind(across(2)), fwd_second),
    )


SENDS = tuple(sends_of(link) for link in range(len(LINKS)))
SLOTS = len(SENDS[0])
UNITS = [(link, slot) for slot in range(SLOTS) for link in range(len(LINKS))]


def arriving(link, slot):
    off, quarter = SENDS[link][slot]
    return shift(off, LINKS[link], -1), quarter


ARRIVES = {arriving(*unit): unit for unit in UNITS}
assert len(ARRIVES) == len(UNITS) == (SIDE * SIDE - 1) * QUARTERS
PASSED = []
for _link, _slot in UNITS:
    _what = SENDS[_link][_slot]
    if _what[0] != (0, 0) and ARRIVES[_what] not in PASSED:
        PASSED.append(ARRIVES[_what])
KEPT = [unit for unit in UNITS if unit not in PASSED]
assert len(KEPT) % QUARTERS == 0


class Place:
    def __init__(self):
        self.row, self.col = lax.axis_index("rows"), lax.axis_index("cols")
        self.z, self.y = self.row // SIDE, self.row % SIDE
        self.x, self.core = self.col // CORES, self.col % CORES

    def at(self, off):
        return ((self.z + off[0]) % SIDE) * SIDE + (self.y + off[1]) % SIDE

    def neighbour(self, d):
        return (self.at(d), self.col)

    def partner(self):
        return (self.row, self.x * CORES + 1 - self.core)

    def along_x(self, n):
        return (self.row, ((self.x + n) % SIDE) * CORES + self.core)


def remote(src, dst, send_sem, recv_sem, device):
    return pltpu.make_async_remote_copy(
        src_ref=src, dst_ref=dst, send_sem=send_sem, recv_sem=recv_sem, device_id=device, device_id_type=MESH
    )


def signal_all(barrier, devices):
    for device in devices:
        pl.semaphore_signal(barrier, inc=1, device_id=device, device_id_type=MESH)


def gather_kernel(
    train_query, low_query, high_query,
    train_key, low_key, high_key,
    train_value, low_value, high_value,
    norm_train, norm_step,
    whole, norm,
    tq, lq, hq, tk, lk, hk, tv, lv, hv, nt, ns, pair, ring, lines, all_lines, ordered,
    load_sem, send_sem, recv_sem, kept_sem, pair_sem, ring_send, ring_recv, line_sem, norm_send, norm_recv,
):
    me = Place()
    wide = tq.shape[1]
    part = wide // QUARTERS
    blocks = whole.shape[0]
    leader = (me.z == LEADER) & (me.y == LEADER)
    steps = range(1, SIDE)

    barrier = pltpu.get_barrier_semaphore()
    peers = [me.neighbour(d) for d in LINKS] + [me.partner()]
    signal_all(barrier, peers)

    @pl.when(leader)
    def _():
        signal_all(barrier, [me.along_x(n) for n in steps])

    loads = {}

    def load(name, src, dst):
        copy = pltpu.make_async_copy(src, dst, load_sem.at[len(loads)])
        copy.start()
        loads[name] = copy

    pieces = [(ORDER[0], 0, part // 2), (ORDER[0], part // 2, part)] + [(q, 0, part) for q in ORDER[1:]]
    load("lq", low_query, lq)
    load("hq", high_query, hq)
    for n, (q, start, end) in enumerate(pieces):
        cols = pl.ds(q * part + start, end - start)
        load(n, train_query.at[:, cols], tq.at[:, cols])
        if n == 1:
            load("tk", train_key, tk)
            load("lk", low_key, lk)
            load("hk", high_key, hk)
        if n == 2:
            load("tv", train_value, tv)
            load("lv", low_value, lv)
            load("hv", high_value, hv)
    load("nt", norm_train, nt)
    load("ns", norm_step, ns)

    def merged(train, high, low):
        return train.astype(jnp.float32) + lax.dot_general(
            high, low, (((0,), (0,)), ((), ())), preferred_element_type=jnp.float32
        )

    def unit_copy(link, slot, what, rows=slice(None)):
        off, q = what
        unit = whole.at[me.at(off), q, rows]
        sem = recv_sem.at[PASSED.index((link, slot))] if (link, slot) in PASSED else kept_sem
        return remote(unit, unit, send_sem, sem, me.neighbour(LINKS[link]))

    def send(link, slot, rows=slice(None)):
        unit_copy(link, slot, SENDS[link][slot], rows).start()

    arrived = set()

    def arrive(unit):
        if unit not in arrived:
            arrived.add(unit)
            unit_copy(*unit, arriving(*unit)).wait_recv()

    loads["lq"].wait()
    loads["hq"].wait()
    for n, (q, start, end) in enumerate(pieces):
        cols = pl.ds(q * part + start, end - start)
        loads[n].wait()
        whole[me.row, q, start:end, :] = merged(tq[:, cols].T, hq[:, cols], lq[...]).astype(whole.dtype)
        if n == 0:

            @pl.when(leader)
            def _():
                pl.semaphore_wait(barrier, len(peers) + len(steps))

            @pl.when(jnp.logical_not(leader))
            def _():
                pl.semaphore_wait(barrier, len(peers))

        if end == part:
            if n == 1:
                for name in ("tk", "lk", "hk"):
                    loads[name].wait()
            if n == 2:
                for name in ("tv", "lv", "hv"):
                    loads[name].wait()
            train, low, high = (tk, lk, hk) if q < 2 else (tv, lv, hv)
            small = merged(train[...], high[...], low[...]).astype(whole.dtype)
            half = small.shape[0] // 2
            whole[me.row, q, part:, :] = small[(q % 2) * half : (q % 2 + 1) * half, :]
        for link in range(len(LINKS)):
            if n == 0:
                send(link, 0, pl.ds(0, end))
            elif n == 1:
                send(link, 0, pl.ds(start, whole.shape[2] - start))
            else:
                send(link, ORDER.index(q))

    loads["nt"].wait()
    loads["ns"].wait()
    fresh = nt[...] + ns[...]
    pair[me.core] = jnp.concatenate([fresh, fresh], axis=1)

    def pair_copy(slot):
        return remote(pair.at[slot], pair.at[slot], pair_sem.at[0], pair_sem.at[1], me.partner())

    pair_copy(me.core).start()

    def ring_copy(n, src, d):
        return remote(src, src, ring_send, ring_recv.at[n], me.neighbour(d))

    def column(dz):
        return ring.at[pl.ds(((me.z + dz) % SIDE) * SIDE, SIDE)]

    def line_copy(n):
        return remote(lines, all_lines.at[me.x], line_sem.at[0], line_sem.at[1], me.along_x(n))

    def norm_copy(link):
        return remote(norm, norm, norm_send.at[link], norm_recv, me.neighbour(LINKS[link]))

    from_leader = ((me.z - LEADER) % SIDE, (me.y - LEADER) % SIDE)
    passes = [((0, 0), (0, 1, 2, 3)), ((0, 1), (0, 2, 3)), ((0, 3), (2, 3)), ((0, 2), (2, 3))]
    passes += [((1, y), (2,)) for y in range(SIDE)]

    def pass_norm(places):
        for (z, y), links in passes:
            if (z, y) in places:

                @pl.when((from_leader[0] == z) & (from_leader[1] == y))
                def _():
                    if (z, y) != (0, 0):
                        norm_copy(0).wait_recv()
                    for link in links:
                        norm_copy(link).start()

    def norm_step_of(step):
        if step == 0:
            pair_copy(1 - me.core).wait_recv()
            lane = lax.broadcasted_iota(jnp.int32, (1, pair.shape[2]), 1)
            ring[me.row] = jnp.where(lane < pair.shape[2] // CORES, pair[0], pair[1])
        if step == 1:
            ring_copy(0, ring.at[me.row], (0, 1)).start()
            ring_copy(1, ring.at[me.row], (0, -1)).start()
        if step == 2:
            ring_copy(0, ring.at[me.at((0, -1))], (0, 1)).wait_recv()
            ring_copy(1, ring.at[me.at((0, 1))], (0, -1)).wait_recv()
            ring_copy(2, ring.at[me.at((0, -1))], (0, 1)).start()
        if step == 3:
            ring_copy(2, ring.at[me.at((0, -2))], (0, 1)).wait_recv()
            ring_copy(3, column(0), (1, 0)).start()
            ring_copy(4, column(0), (-1, 0)).start()
        if step == 4:
            ring_copy(3, column(-1), (1, 0)).wait_recv()
            ring_copy(4, column(1), (-1, 0)).wait_recv()
            ring_copy(5, column(-1), (1, 0)).start()
        if step == 5:
            ring_copy(5, column(-2), (1, 0)).wait_recv()

            @pl.when(leader)
            def _():
                lines[...] = jnp.concatenate([ring[i] for i in range(blocks)], axis=0)
                all_lines[me.x] = lines[...]
                for n in steps:
                    line_copy(n).start()

        if step == 7:

            @pl.when(leader)
            def _():
                three = all_lines.at[pl.ds(0, len(steps))]
                every = remote(three, three, line_sem.at[0], line_sem.at[1], me.along_x(1))
                every.wait_recv()
                for x in range(SIDE):
                    ordered[pl.Slice(x, blocks, SIDE), :] = all_lines[x]
                norm[...] = ordered[...].astype(norm.dtype)

            pass_norm([(0, 0)])
        if step == 8:
            pass_norm([(0, 1), (0, 3)])
        if step == 9:
            pass_norm([(0, 2)])
        if step == 10:
            pass_norm([(1, y) for y in range(SIDE)])

    for slot in range(QUARTERS, SLOTS):
        for link in range(len(LINKS)):
            arrive(ARRIVES[SENDS[link][slot]])
            send(link, slot)
        norm_step_of(slot - QUARTERS)

    @pl.when(from_leader[0] >= 2)
    def _():
        norm_copy(0).wait_recv()

    for unit in PASSED:
        arrive(unit)
    kept = whole.at[pl.ds(0, len(KEPT) // QUARTERS)]
    remote(kept, kept, send_sem, kept_sem, me.partner()).wait_recv()
    sent = whole.at[pl.ds(0, len(UNITS) // QUARTERS)]
    remote(sent, sent, send_sem, kept_sem, me.partner()).wait_send()
    pair_copy(me.core).wait_send()
    around = ring.at[pl.ds(0, blocks - 1)]
    remote(around, around, ring_send, ring_recv.at[0], me.partner()).wait_send()

    @pl.when(leader)
    def _():
        three = all_lines.at[pl.ds(0, len(steps))]
        remote(three, three, line_sem.at[0], line_sem.at[1], me.along_x(1)).wait_send()

    for (z, y), links in passes:

        @pl.when((from_leader[0] == z) & (from_leader[1] == y))
        def _():
            for link in links:
                norm_copy(link).wait_send()


def write_kernel(whole, norm, out_query, out_key, out_value, out_norm, sem):
    blocks, quarters, rows, depth = whole.shape
    part = out_query.shape[0] // quarters
    half = rows - part
    outs = (out_query, out_key, out_value, out_norm)
    pltpu.make_async_copy(norm, out_norm, sem.at[3]).start()

    @pl.loop(0, blocks)
    def _(r):
        at = pl.ds(pl.multiple_of(r * depth, depth), depth)
        for q in range(quarters):
            pltpu.make_async_copy(
                whole.at[r, q, pl.ds(0, part)], out_query.at[pl.ds(q * part, part), at], sem.at[0]
            ).start()
        for q in range(quarters):
            n = 1 + q // 2
            pltpu.make_async_copy(
                whole.at[r, q, pl.ds(part, half)], outs[n].at[pl.ds((q % 2) * half, half), at], sem.at[n]
            ).start()

    for n, out in enumerate(outs):
        pltpu.make_async_copy(out, out, sem.at[n]).wait()


def body(
    train_query, low_query, high_query,
    train_key, low_key, high_key,
    train_value, low_value, high_value,
    norm_train, norm_step,
):
    n_rows, n_cols = lax.axis_size("rows"), lax.axis_size("cols")
    depth, wide = train_query.shape
    tall = train_key.shape[1]
    rank = low_query.shape[1]
    unit = (wide + 2 * tall) // QUARTERS
    values = norm_train.shape[0]
    line = CORES * values
    dtype = train_query.dtype
    f32 = jnp.float32
    anywhere = pl.BlockSpec(memory_space=pl.ANY)
    vmem = pl.BlockSpec(memory_space=pltpu.VMEM)
    dma = pltpu.SemaphoreType.DMA
    shape = jax.ShapeDtypeStruct

    def pin(space, *arrays):
        return [pltpu.with_memory_space_constraint(a, space) for a in arrays]

    whole, norm = pl.pallas_call(
        gather_kernel,
        out_shape=(
            shape((n_rows, QUARTERS, unit, depth), dtype),
            shape((n_rows * n_cols // CORES, line), dtype),
        ),
        in_specs=[anywhere] * 11,
        out_specs=(vmem, vmem),
        scratch_shapes=[
            pltpu.VMEM((depth, wide), dtype),
            pltpu.VMEM((rank, depth), dtype),
            pltpu.VMEM((rank, wide), dtype),
            pltpu.VMEM((tall, depth), dtype),
            pltpu.VMEM((rank, depth), dtype),
            pltpu.VMEM((rank, tall), dtype),
            pltpu.VMEM((tall, depth), dtype),
            pltpu.VMEM((rank, depth), dtype),
            pltpu.VMEM((rank, tall), dtype),
            pltpu.VMEM((1, values), f32),
            pltpu.VMEM((1, values), f32),
            pltpu.VMEM((CORES, 1, line), f32),
            pltpu.VMEM((n_rows, 1, line), f32),
            pltpu.VMEM((n_rows, line), f32),
            pltpu.VMEM((SIDE, n_rows, line), f32),
            pltpu.VMEM((SIDE * n_rows, line), f32),
            dma((15,)),
            dma(()),
            dma((len(PASSED),)),
            dma(()),
            dma((2,)),
            dma(()),
            dma((6,)),
            dma((2,)),
            dma((len(LINKS),)),
            dma(()),
        ],
        compiler_params=pltpu.CompilerParams(
            collective_id=0, has_side_effects=True, vmem_limit_bytes=24 * 2**20
        ),
        name="gather",
    )(
        *pin(
            pltpu.HBM,
            train_query, low_query.T, high_query,
            train_key.T, low_key.T, high_key,
            train_value.T, low_value.T, high_value,
            norm_train.reshape(1, -1), norm_step.reshape(1, -1),
        )
    )
    out_query, out_key, out_value, out_norm = pl.pallas_call(
        write_kernel,
        out_shape=(
            shape((wide, n_rows * depth), dtype),
            shape((tall, n_rows * depth), dtype),
            shape((tall, n_rows * depth), dtype),
            shape(norm.shape, dtype),
        ),
        in_specs=[vmem] * 2,
        out_specs=[anywhere] * 4,
        scratch_shapes=[dma((4,))],
        compiler_params=pltpu.CompilerParams(vmem_limit_bytes=4 * 2**20),
        name="write",
    )(*pin(pltpu.VMEM, whole, norm))
    return out_query, out_key, out_value, out_norm.reshape(-1)


def solution(mesh):
    return jax.shard_map(
        body,
        mesh=mesh,
        in_specs=(
            P("rows", "cols"),
            P("rows", None),
            P(None, "cols"),
            P("rows", "cols"),
            P("rows", None),
            P(None, "cols"),
            P("rows", "cols"),
            P("rows", None),
            P(None, "cols"),
            P(("rows", "cols")),
            P(("rows", "cols")),
        ),
        out_specs=(P("cols", None), P("cols", None), P("cols", None), P()),
        check_vma=False,
    )
```

```python
import jax
import jax.numpy as jnp
from jax import lax
from jax.experimental import pallas as pl
from jax.experimental.pallas import tpu as pltpu
from jax.sharding import PartitionSpec as P

MESH = pl.DeviceIdType.MESH

SIDE = 4
QUARTERS = 4
CORES = 2
LINKS = ((0, 1), (0, -1), (1, 0), (-1, 0))
LATE = 1
SPLIT = 12
ORDER = (0, 2, 1, 3)


def shift(off, d, sign=1):
    return ((off[0] + sign * d[0]) % SIDE, (off[1] + sign * d[1]) % SIDE)


def sends_of(link):
    d = LINKS[link]
    along_y = d[0] == 0
    first = (0, 1) if along_y else (2, 3)
    second = (2, 3) if along_y else (0, 1)
    positive = sum(d) > 0
    fwd_first = first[0] if positive else first[1]
    fwd_second = second[0] if positive else second[1]

    def across(n):
        return (n % SIDE, 0) if along_y else (0, n % SIDE)

    def behind(off):
        return shift(off, d, -1)

    own = (0, 0)
    return tuple((own, q) for q in ORDER) + (
        (across(-1), second[0]),
        (across(1), second[0]),
        (behind(own), fwd_first),
        (across(-1), second[1]),
        (across(1), second[1]),
        (behind(own), fwd_second),
        (across(2), second[0]),
        (across(2), second[1]),
        (behind(across(-1)), fwd_second),
        (behind(across(1)), fwd_second),
        (behind(across(2)), fwd_second),
    )


SENDS = tuple(sends_of(link) for link in range(len(LINKS)))
SLOTS = len(SENDS[0])
UNITS = [(link, slot) for slot in range(SLOTS) for link in range(len(LINKS))]


def arriving(link, slot):
    off, quarter = SENDS[link][slot]
    return shift(off, LINKS[link], -1), quarter


ARRIVES = {arriving(*unit): unit for unit in UNITS}
assert len(ARRIVES) == len(UNITS) == (SIDE * SIDE - 1) * QUARTERS
LAST = [unit for unit in UNITS if unit[1] >= SPLIT]
GROUPS = ((0, 1), (2, 3), (6,), (4, 5, 7, 8), (10, 11), (9,), (12, 13, 14))
GROUP_OF = {slot: group for group, slots in enumerate(GROUPS) for slot in slots}
assert sorted(GROUP_OF) == list(range(SLOTS)) and GROUPS[-1] == tuple(range(SPLIT, SLOTS))
AFTER = ((4, 5), (6, 7, 8, 9), (10, 11), (12, 13), (14,))
for _group, _slots in enumerate(AFTER):
    for _slot in _slots:
        for _link in range(len(LINKS)):
            assert GROUP_OF[ARRIVES[SENDS[_link][_slot]][1]] <= _group


class Place:
    def __init__(self):
        self.row, self.col = lax.axis_index("rows"), lax.axis_index("cols")
        self.z, self.y = self.row // SIDE, self.row % SIDE
        self.x, self.core = self.col // CORES, self.col % CORES

    def at(self, off):
        return ((self.z + off[0]) % SIDE) * SIDE + (self.y + off[1]) % SIDE

    def neighbour(self, d):
        return (self.at(d), self.col)

    def partner(self):
        return (self.row, self.x * CORES + 1 - self.core)

    def along_x(self, n):
        return (self.row, ((self.x + n) % SIDE) * CORES + self.core)


def remote(src, dst, send_sem, recv_sem, device):
    return pltpu.make_async_remote_copy(
        src_ref=src, dst_ref=dst, send_sem=send_sem, recv_sem=recv_sem, device_id=device, device_id_type=MESH
    )


def signal_all(barrier, devices):
    for device in devices:
        pl.semaphore_signal(barrier, inc=1, device_id=device, device_id_type=MESH)


def gather_kernel(
    train_query, low_query, high_query,
    train_key, low_key, high_key,
    train_value, low_value, high_value,
    norm_train, norm_step,
    whole, norm,
    tq, lq, hq, tk, lk, hk, tv, lv, hv, nt, ns, pair, ring, lines, all_lines, ordered,
    load_sem, send_sem, recv_sem, pair_sem, ring_send, ring_recv, line_sem, norm_send, norm_recv,
):
    me = Place()
    wide = tq.shape[1]
    part = wide // QUARTERS
    blocks = whole.shape[0]
    leader = (me.z == 0) & (me.y == 0)
    steps = range(1, SIDE)

    barrier = pltpu.get_barrier_semaphore()
    peers = [me.neighbour(d) for d in LINKS] + [me.partner()]
    signal_all(barrier, peers)

    @pl.when(leader)
    def _():
        signal_all(barrier, [me.along_x(n) for n in steps])

    loads = {}

    def load(name, src, dst):
        copy = pltpu.make_async_copy(src, dst, load_sem.at[len(loads)])
        copy.start()
        loads[name] = copy

    pieces = [(ORDER[0], 0, part // 2), (ORDER[0], part // 2, part)] + [(q, 0, part) for q in ORDER[1:]]
    load("lq", low_query, lq)
    load("hq", high_query, hq)
    for n, (q, start, end) in enumerate(pieces):
        cols = pl.ds(q * part + start, end - start)
        load(n, train_query.at[:, cols], tq.at[:, cols])
        if n == 1:
            load("tk", train_key, tk)
            load("lk", low_key, lk)
            load("hk", high_key, hk)
        if n == 2:
            load("tv", train_value, tv)
            load("lv", low_value, lv)
            load("hv", high_value, hv)
    load("nt", norm_train, nt)
    load("ns", norm_step, ns)

    def merged(train, high, low):
        return train.astype(jnp.float32) + lax.dot_general(
            high, low, (((0,), (0,)), ((), ())), preferred_element_type=jnp.float32
        )

    def unit_copy(link, slot, what, rows=slice(None)):
        off, q = what
        unit = whole.at[me.at(off), q, rows]
        return remote(unit, unit, send_sem, recv_sem.at[GROUP_OF[slot]], me.neighbour(LINKS[link]))

    def send(link, slot, rows=slice(None)):
        unit_copy(link, slot, SENDS[link][slot], rows).start()

    def units(slots, sem):
        some = whole.at[pl.ds(0, slots * len(LINKS) // QUARTERS)]
        return remote(some, some, send_sem, sem, me.partner())

    def arrive(group):
        units(len(GROUPS[group]), recv_sem.at[group]).wait_recv()

    def only(core):
        return pl.when(me.core == LATE if core == LATE else me.core != LATE)

    loads["lq"].wait()
    loads["hq"].wait()
    for n, (q, start, end) in enumerate(pieces):
        cols = pl.ds(q * part + start, end - start)
        loads[n].wait()
        whole[me.row, q, start:end, :] = merged(tq[:, cols].T, hq[:, cols], lq[...]).astype(whole.dtype)
        if n == 0:

            @pl.when(leader)
            def _():
                pl.semaphore_wait(barrier, len(peers) + len(steps))

            @pl.when(jnp.logical_not(leader))
            def _():
                pl.semaphore_wait(barrier, len(peers))

        if end == part:
            if n == 1:
                for name in ("tk", "lk", "hk"):
                    loads[name].wait()
            if n == 2:
                for name in ("tv", "lv", "hv"):
                    loads[name].wait()
            train, low, high = (tk, lk, hk) if q < 2 else (tv, lv, hv)
            small = merged(train[...], high[...], low[...]).astype(whole.dtype)
            half = small.shape[0] // 2
            whole[me.row, q, part:, :] = small[(q % 2) * half : (q % 2 + 1) * half, :]
        for link in range(len(LINKS)):
            if n == 0:
                send(link, 0, pl.ds(0, end))
            elif n == 1:
                send(link, 0, pl.ds(start, whole.shape[2] - start))
            else:
                send(link, ORDER.index(q))

    loads["nt"].wait()
    loads["ns"].wait()
    fresh = nt[...] + ns[...]
    pair[me.core] = jnp.concatenate([fresh, fresh], axis=1)

    def pair_copy(slot):
        return remote(pair.at[slot], pair.at[slot], pair_sem.at[0], pair_sem.at[1], me.partner())

    pair_copy(me.core).start()

    def ring_copy(n, src, d):
        return remote(src, src, ring_send, ring_recv.at[n], me.neighbour(d))

    def column(dz):
        return ring.at[pl.ds(((me.z + dz) % SIDE) * SIDE, SIDE)]

    def line_copy(n):
        return remote(lines, all_lines.at[me.x], line_sem.at[0], line_sem.at[1], me.along_x(n))

    def norm_copy(link):
        return remote(norm, norm, norm_send.at[link], norm_recv, me.neighbour(LINKS[link]))

    passes = [((0, 0), (0, 1, 2, 3)), ((0, 1), (0, 2, 3)), ((0, 3), (2, 3)), ((0, 2), (2, 3))]
    passes += [((1, y), (2,)) for y in range(SIDE)]

    def pass_norm(places):
        for (z, y), links in passes:
            if (z, y) in places:

                @pl.when((me.z == z) & (me.y == y))
                def _():
                    if (z, y) != (0, 0):
                        norm_copy(0).wait_recv()
                    for link in links:
                        norm_copy(link).start()

    def norm_step_of(step):
        if step == 0:
            pair_copy(1 - me.core).wait_recv()
            lane = lax.broadcasted_iota(jnp.int32, (1, pair.shape[2]), 1)
            ring[me.row] = jnp.where(lane < pair.shape[2] // CORES, pair[0], pair[1])
        if step == 1:
            ring_copy(0, ring.at[me.row], (0, 1)).start()
            ring_copy(1, ring.at[me.row], (0, -1)).start()
        if step == 2:
            ring_copy(0, ring.at[me.at((0, -1))], (0, 1)).wait_recv()
            ring_copy(1, ring.at[me.at((0, 1))], (0, -1)).wait_recv()
            ring_copy(2, ring.at[me.at((0, -1))], (0, 1)).start()
        if step == 3:
            ring_copy(2, ring.at[me.at((0, -2))], (0, 1)).wait_recv()
            ring_copy(3, column(0), (1, 0)).start()
            ring_copy(4, column(0), (-1, 0)).start()
        if step == 4:
            ring_copy(3, column(-1), (1, 0)).wait_recv()
            ring_copy(4, column(1), (-1, 0)).wait_recv()
            ring_copy(5, column(-1), (1, 0)).start()
        if step == 5:
            ring_copy(5, column(-2), (1, 0)).wait_recv()

            @pl.when(leader)
            def _():
                lines[...] = jnp.concatenate([ring[i] for i in range(blocks)], axis=0)
                all_lines[me.x] = lines[...]
                for n in steps:
                    line_copy(n).start()

        if step == 7:

            @pl.when(leader)
            def _():
                three = all_lines.at[pl.ds(0, len(steps))]
                every = remote(three, three, line_sem.at[0], line_sem.at[1], me.along_x(1))
                every.wait_recv()
                for x in range(SIDE):
                    ordered[pl.Slice(x, blocks, SIDE), :] = all_lines[x]
                norm[...] = ordered[...].astype(norm.dtype)

            pass_norm([(0, 0)])
        if step == 8:
            pass_norm([(0, 1), (0, 3)])
        if step == 9:
            pass_norm([(0, 2)])
        if step == 10:
            pass_norm([(1, y) for y in range(SIDE)])

    def send_slots(slots):
        for slot in slots:
            for link in range(len(LINKS)):
                send(link, slot)

    norm_steps = ((0, 1), (2, 3), (4, 5, 7), (8, 9, 10), ())
    for group, slots in enumerate(AFTER):
        arrive(group)
        if slots[0] < SPLIT:
            send_slots(slots)
        else:

            @only(1 - LATE)
            def _():
                send_slots(slots)

        for step in norm_steps[group]:
            norm_step_of(step)
        if 10 in norm_steps[group]:

            @pl.when(me.z >= 2)
            def _():
                norm_copy(0).wait_recv()

    arrive(5)

    @only(1 - LATE)
    def _():
        arrive(6)
        units(SLOTS, recv_sem.at[0]).wait_send()

    @only(LATE)
    def _():
        units(SPLIT, recv_sem.at[0]).wait_send()

    pair_copy(me.core).wait_send()
    around = ring.at[pl.ds(0, blocks - 1)]
    remote(around, around, ring_send, ring_recv.at[0], me.partner()).wait_send()

    @pl.when(leader)
    def _():
        three = all_lines.at[pl.ds(0, len(steps))]
        remote(three, three, line_sem.at[0], line_sem.at[1], me.along_x(1)).wait_send()

    for (z, y), links in passes:

        @pl.when((me.z == z) & (me.y == y))
        def _():
            for link in links:
                norm_copy(link).wait_send()


def finish_kernel(whole, token, rest, send_sem, recv_sem):
    del token
    me = Place()

    @pl.when(me.core == LATE)
    def _():
        barrier = pltpu.get_barrier_semaphore()
        signal_all(barrier, [me.neighbour(d) for d in LINKS])
        pl.semaphore_wait(barrier, len(LINKS))
        for link, slot in LAST:
            off, q = SENDS[link][slot]
            unit = whole.at[me.at(off), q]
            remote(unit, rest.at[link, slot - SPLIT], send_sem, recv_sem, me.neighbour(LINKS[link])).start()
        remote(rest, rest, send_sem, recv_sem, me.partner()).wait()


def write_unit(source, block, quarter, outs, sems):
    out_query, out_key, out_value = outs
    rows, depth = source.shape
    part = out_query.shape[0] // QUARTERS
    half = rows - part
    at = pl.ds(pl.multiple_of(block * depth, depth), depth)
    small = (out_key if quarter < 2 else out_value).at[pl.ds((quarter % 2) * half, half), at]
    pltpu.make_async_copy(source.at[pl.ds(0, part)], out_query.at[pl.ds(quarter * part, part), at], sems[0]).start()
    pltpu.make_async_copy(source.at[pl.ds(part, half)], small, sems[1 + quarter // 2]).start()


def wait_units(count, unit_bytes, out, sem):
    rows = count * unit_bytes // (out.shape[1] * out.dtype.itemsize)
    same = out.at[pl.ds(0, rows)]
    pltpu.make_async_copy(same, same, sem).wait()


def unit_bytes_of(whole):
    return whole.shape[-2] * whole.shape[-1] * whole.dtype.itemsize


def write_kernel(whole, out_query, out_key, out_value, token, sem):
    me = Place()
    outs = (out_query, out_key, out_value)
    token[...] = jnp.zeros_like(token)
    late = {arriving(*unit) for unit in LAST}

    @pl.when(me.core == LATE)
    def _():
        count = 0
        for off in [(dz, dy) for dz in range(SIDE) for dy in range(SIDE)]:
            for q in range(QUARTERS):
                if (off, q) not in late:
                    count += 1
                    block = me.at(off)
                    write_unit(whole.at[block, q], block, q, outs, (sem, sem, sem))
        wait_units(count, unit_bytes_of(whole), out_query, sem)


def write_rest_kernel(
    whole, rest, norm, in_query, in_key, in_value, out_query, out_key, out_value, out_norm, sem, norm_sem
):
    del in_query, in_key, in_value
    me = Place()
    outs = (out_query, out_key, out_value)
    norm_copy = pltpu.make_async_copy(norm, out_norm, norm_sem)
    norm_copy.start()

    @pl.when(me.core == LATE)
    def _():
        first = sem.at[0]
        for link, slot in LAST:
            off, q = arriving(link, slot)
            write_unit(rest.at[link, slot - SPLIT], me.at(off), q, outs, (first, first, first))
        wait_units(len(LAST), unit_bytes_of(whole), out_query, first)

    @pl.when(me.core != LATE)
    def _():
        @pl.loop(0, whole.shape[0])
        def _(block):
            for q in range(QUARTERS):
                write_unit(whole.at[block, q], block, q, outs, [sem.at[n] for n in range(len(outs))])

        for n, out in enumerate(outs):
            pltpu.make_async_copy(out, out, sem.at[n]).wait()

    norm_copy.wait()


def body(
    train_query, low_query, high_query,
    train_key, low_key, high_key,
    train_value, low_value, high_value,
    norm_train, norm_step,
):
    n_rows, n_cols = lax.axis_size("rows"), lax.axis_size("cols")
    depth, wide = train_query.shape
    tall = train_key.shape[1]
    rank = low_query.shape[1]
    unit = (wide + 2 * tall) // QUARTERS
    values = norm_train.shape[0]
    line = CORES * values
    dtype = train_query.dtype
    f32 = jnp.float32
    anywhere = pl.BlockSpec(memory_space=pl.ANY)
    vmem = pl.BlockSpec(memory_space=pltpu.VMEM)
    dma = pltpu.SemaphoreType.DMA
    shape = jax.ShapeDtypeStruct

    def pin(space, *arrays):
        return [pltpu.with_memory_space_constraint(a, space) for a in arrays]

    whole, norm = pl.pallas_call(
        gather_kernel,
        out_shape=(
            shape((n_rows, QUARTERS, unit, depth), dtype),
            shape((n_rows * n_cols // CORES, line), dtype),
        ),
        in_specs=[anywhere] * 11,
        out_specs=(vmem, vmem),
        scratch_shapes=[
            pltpu.VMEM((depth, wide), dtype),
            pltpu.VMEM((rank, depth), dtype),
            pltpu.VMEM((rank, wide), dtype),
            pltpu.VMEM((tall, depth), dtype),
            pltpu.VMEM((rank, depth), dtype),
            pltpu.VMEM((rank, tall), dtype),
            pltpu.VMEM((tall, depth), dtype),
            pltpu.VMEM((rank, depth), dtype),
            pltpu.VMEM((rank, tall), dtype),
            pltpu.VMEM((1, values), f32),
            pltpu.VMEM((1, values), f32),
            pltpu.VMEM((CORES, 1, line), f32),
            pltpu.VMEM((n_rows, 1, line), f32),
            pltpu.VMEM((n_rows, line), f32),
            pltpu.VMEM((SIDE, n_rows, line), f32),
            pltpu.VMEM((SIDE * n_rows, line), f32),
            dma((15,)),
            dma(()),
            dma((len(GROUPS),)),
            dma((2,)),
            dma(()),
            dma((6,)),
            dma((2,)),
            dma((len(LINKS),)),
            dma(()),
        ],
        compiler_params=pltpu.CompilerParams(
            collective_id=0, has_side_effects=True, vmem_limit_bytes=24 * 2**20
        ),
        name="gather",
    )(
        *pin(
            pltpu.HBM,
            train_query, low_query.T, high_query,
            train_key.T, low_key.T, high_key,
            train_value.T, low_value.T, high_value,
            norm_train.reshape(1, -1), norm_step.reshape(1, -1),
        )
    )
    outs = [shape((wide, n_rows * depth), dtype)] + [shape((tall, n_rows * depth), dtype)] * 2
    out_query, out_key, out_value, token = pl.pallas_call(
        write_kernel,
        out_shape=(*outs, shape((8, 128), f32)),
        in_specs=[vmem],
        out_specs=[anywhere] * 3 + [vmem],
        scratch_shapes=[dma(())],
        compiler_params=pltpu.CompilerParams(vmem_limit_bytes=4 * 2**20),
        name="write",
    )(*pin(pltpu.VMEM, whole))
    (rest,) = pl.pallas_call(
        finish_kernel,
        out_shape=(shape((len(LINKS), SLOTS - SPLIT, unit, depth), dtype),),
        in_specs=[vmem] * 2,
        out_specs=(vmem,),
        scratch_shapes=[dma(()), dma(())],
        compiler_params=pltpu.CompilerParams(
            collective_id=1, has_side_effects=True, vmem_limit_bytes=8 * 2**20
        ),
        name="finish",
    )(*pin(pltpu.VMEM, whole, token))
    out_query, out_key, out_value, out_norm = pl.pallas_call(
        write_rest_kernel,
        out_shape=(*outs, shape(norm.shape, dtype)),
        in_specs=[vmem] * 3 + [anywhere] * 3,
        out_specs=[anywhere] * 4,
        input_output_aliases={3: 0, 4: 1, 5: 2},
        scratch_shapes=[dma((len(outs),)), dma(())],
        compiler_params=pltpu.CompilerParams(vmem_limit_bytes=4 * 2**20),
        name="write_rest",
    )(*pin(pltpu.VMEM, whole, rest, norm), *pin(pltpu.HBM, out_query, out_key, out_value))
    return out_query, out_key, out_value, out_norm.reshape(-1)


def solution(mesh):
    return jax.shard_map(
        body,
        mesh=mesh,
        in_specs=(
            P("rows", "cols"),
            P("rows", None),
            P(None, "cols"),
            P("rows", "cols"),
            P("rows", None),
            P(None, "cols"),
            P("rows", "cols"),
            P("rows", None),
            P(None, "cols"),
            P(("rows", "cols")),
            P(("rows", "cols")),
        ),
        out_specs=(P("cols", None), P("cols", None), P("cols", None), P()),
        check_vma=False,
    )
```

```python
import jax
import jax.numpy as jnp
from jax import lax
from jax.experimental import pallas as pl
from jax.experimental.pallas import tpu as pltpu
from jax.sharding import PartitionSpec as P

MESH = pl.DeviceIdType.MESH

SIDE = 4
QUARTERS = 4
CORES = 2
LINKS = ((0, 1), (0, -1), (1, 0), (-1, 0))
LATE = 1
SPLIT = 12
ORDER = (0, 2, 1, 3)


def shift(off, d, sign=1):
    return ((off[0] + sign * d[0]) % SIDE, (off[1] + sign * d[1]) % SIDE)


def sends_of(link):
    d = LINKS[link]
    along_y = d[0] == 0
    first = (0, 1) if along_y else (2, 3)
    second = (2, 3) if along_y else (0, 1)
    positive = sum(d) > 0
    fwd_first = first[0] if positive else first[1]
    fwd_second = second[0] if positive else second[1]

    def across(n):
        return (n % SIDE, 0) if along_y else (0, n % SIDE)

    def behind(off):
        return shift(off, d, -1)

    own = (0, 0)
    return tuple((own, q) for q in ORDER) + (
        (across(-1), second[0]),
        (across(1), second[0]),
        (behind(own), fwd_first),
        (across(-1), second[1]),
        (across(1), second[1]),
        (behind(own), fwd_second),
        (across(2), second[0]),
        (across(2), second[1]),
        (behind(across(-1)), fwd_second),
        (behind(across(1)), fwd_second),
        (behind(across(2)), fwd_second),
    )


SENDS = tuple(sends_of(link) for link in range(len(LINKS)))
SLOTS = len(SENDS[0])
UNITS = [(link, slot) for slot in range(SLOTS) for link in range(len(LINKS))]


def arriving(link, slot):
    off, quarter = SENDS[link][slot]
    return shift(off, LINKS[link], -1), quarter


ARRIVES = {arriving(*unit): unit for unit in UNITS}
assert len(ARRIVES) == len(UNITS) == (SIDE * SIDE - 1) * QUARTERS
LAST = [unit for unit in UNITS if unit[1] >= SPLIT]
GROUPS = ((0, 1), (2, 3), (6,), (4, 5, 7, 8), (10, 11), (9,), (12, 13, 14))
GROUP_OF = {slot: group for group, slots in enumerate(GROUPS) for slot in slots}
assert sorted(GROUP_OF) == list(range(SLOTS)) and GROUPS[-1] == tuple(range(SPLIT, SLOTS))
AFTER = ((4, 5), (6, 7, 8, 9), (10, 11), (12, 13), (14,))
for _group, _slots in enumerate(AFTER):
    for _slot in _slots:
        for _link in range(len(LINKS)):
            assert GROUP_OF[ARRIVES[SENDS[_link][_slot]][1]] <= _group


class Place:
    def __init__(self):
        self.row, self.col = lax.axis_index("rows"), lax.axis_index("cols")
        self.z, self.y = self.row // SIDE, self.row % SIDE
        self.x, self.core = self.col // CORES, self.col % CORES

    def at(self, off):
        return ((self.z + off[0]) % SIDE) * SIDE + (self.y + off[1]) % SIDE

    def neighbour(self, d):
        return (self.at(d), self.col)

    def partner(self):
        return (self.row, self.x * CORES + 1 - self.core)

    def plane(self, n):
        return (self.row, (self.col + n) % (SIDE * CORES))


def remote(src, dst, send_sem, recv_sem, device):
    return pltpu.make_async_remote_copy(
        src_ref=src, dst_ref=dst, send_sem=send_sem, recv_sem=recv_sem, device_id=device, device_id_type=MESH
    )


def signal_all(barrier, devices):
    for device in devices:
        pl.semaphore_signal(barrier, inc=1, device_id=device, device_id_type=MESH)


def gather_kernel(
    train_query, low_query, high_query,
    train_key, low_key, high_key,
    train_value, low_value, high_value,
    norm_train, norm_step,
    whole, norm,
    tq, lq, hq, tk, lk, hk, tv, lv, hv, nt, ns, fresh, ring, lines, ordered,
    load_sem, send_sem, recv_sem, fresh_sem, line_sem, norm_sem,
):
    me = Place()
    wide = tq.shape[1]
    part = wide // QUARTERS
    blocks = whole.shape[0]
    leader = (me.z == 0) & (me.y == 0)
    n_planes = lines.shape[0]
    others = [(dz, dy) for dz in range(SIDE) for dy in range(SIDE) if (dz, dy) != (0, 0)]

    barrier = pltpu.get_barrier_semaphore()
    peers = [me.neighbour(d) for d in LINKS] + [me.partner()]
    signal_all(barrier, peers)

    @pl.when(leader)
    def _():
        signal_all(barrier, [me.neighbour(off) for off in others] + [me.plane(n) for n in range(1, n_planes)])

    loads = {}

    def load(name, src, dst):
        copy = pltpu.make_async_copy(src, dst, load_sem.at[len(loads)])
        copy.start()
        loads[name] = copy

    pieces = [(ORDER[0], 0, part // 2), (ORDER[0], part // 2, part)] + [(q, 0, part) for q in ORDER[1:]]
    load("nt", norm_train, nt)
    load("ns", norm_step, ns)
    load("lq", low_query, lq)
    load("hq", high_query, hq)
    for n, (q, start, end) in enumerate(pieces):
        cols = pl.ds(q * part + start, end - start)
        load(n, train_query.at[:, cols], tq.at[:, cols])
        if n == 1:
            load("tk", train_key, tk)
            load("lk", low_key, lk)
            load("hk", high_key, hk)
        if n == 2:
            load("tv", train_value, tv)
            load("lv", low_value, lv)
            load("hv", high_value, hv)

    def merged(train, high, low):
        return train.astype(jnp.float32) + lax.dot_general(
            high, low, (((0,), (0,)), ((), ())), preferred_element_type=jnp.float32
        )

    def unit_copy(link, slot, what, rows=slice(None)):
        off, q = what
        unit = whole.at[me.at(off), q, rows]
        return remote(unit, unit, send_sem, recv_sem.at[GROUP_OF[slot]], me.neighbour(LINKS[link]))

    def send(link, slot, rows=slice(None)):
        unit_copy(link, slot, SENDS[link][slot], rows).start()

    def units(slots, sem):
        some = whole.at[pl.ds(0, slots * len(LINKS) // QUARTERS)]
        return remote(some, some, send_sem, sem, me.partner())

    def arrive(group):
        units(len(GROUPS[group]), recv_sem.at[group]).wait_recv()

    def only(core):
        return pl.when(me.core == LATE if core == LATE else me.core != LATE)

    def fresh_copy():
        return remote(fresh, ring.at[me.row], fresh_sem.at[0], fresh_sem.at[1], (0, me.col))

    def make_fresh():
        loads["nt"].wait()
        loads["ns"].wait()
        values = nt[...] + ns[...]
        fresh[...] = jnp.concatenate([values, values], axis=1)

    def send_fresh():
        @pl.when(leader)
        def _():
            ring[me.row] = fresh[...]

        @pl.when(jnp.logical_not(leader))
        def _():
            fresh_copy().start()

    loads["lq"].wait()
    loads["hq"].wait()
    for n, (q, start, end) in enumerate(pieces):
        cols = pl.ds(q * part + start, end - start)
        loads[n].wait()
        if n == 1:
            make_fresh()
        whole[me.row, q, start:end, :] = merged(tq[:, cols].T, hq[:, cols], lq[...]).astype(whole.dtype)
        if n == 0:

            @pl.when(leader)
            def _():
                pl.semaphore_wait(barrier, len(peers) + n_planes - 1)

            @pl.when(jnp.logical_not(leader))
            def _():
                pl.semaphore_wait(barrier, len(peers) + 1)

        if end == part:
            if n == 1:
                for name in ("tk", "lk", "hk"):
                    loads[name].wait()
            if n == 2:
                for name in ("tv", "lv", "hv"):
                    loads[name].wait()
            train, low, high = (tk, lk, hk) if q < 2 else (tv, lv, hv)
            small = merged(train[...], high[...], low[...]).astype(whole.dtype)
            half = small.shape[0] // 2
            whole[me.row, q, part:, :] = small[(q % 2) * half : (q % 2 + 1) * half, :]
        for link in range(len(LINKS)):
            if n == 0:
                send(link, 0, pl.ds(0, end))
            elif n == 1:
                send(link, 0, pl.ds(start, whole.shape[2] - start))
            else:
                send(link, ORDER.index(q))
        if n == 1:
            send_fresh()

    def norm_at_leader(group):
        if group == 0:
            some = ring.at[pl.ds(0, blocks - 1)]
            remote(some, some, fresh_sem.at[0], fresh_sem.at[1], me.partner()).wait_recv()
            lines[me.col] = jnp.concatenate([ring[i] for i in range(blocks)], axis=0)
            for n in range(1, n_planes):
                remote(lines.at[me.col], lines.at[me.col], line_sem.at[0], line_sem.at[1], me.plane(n)).start()
        if group == 1:
            some = lines.at[pl.ds(0, n_planes - 1)]
            remote(some, some, line_sem.at[0], line_sem.at[1], me.partner()).wait()
            lane = lax.broadcasted_iota(jnp.int32, lines.shape[1:], 1)
            for x in range(SIDE):
                both = jnp.where(lane < lines.shape[2] // CORES, lines[CORES * x], lines[CORES * x + 1])
                ordered[pl.Slice(x, blocks, SIDE), :] = both
            norm[...] = ordered[...].astype(norm.dtype)
            for off in others:
                remote(norm, norm, norm_sem.at[0], norm_sem.at[1], me.neighbour(off)).start()

    def send_slots(slots):
        for slot in slots:
            for link in range(len(LINKS)):
                send(link, slot)

    for group, slots in enumerate(AFTER):
        arrive(group)
        if slots[0] < SPLIT:
            send_slots(slots)
        else:

            @only(1 - LATE)
            def _():
                send_slots(slots)

        if group < 2:

            @pl.when(leader)
            def _():
                norm_at_leader(group)

    arrive(5)

    @only(1 - LATE)
    def _():
        arrive(6)
        units(SLOTS, recv_sem.at[0]).wait_send()

    @only(LATE)
    def _():
        units(SPLIT, recv_sem.at[0]).wait_send()

    @pl.when(leader)
    def _():
        some = whole.at[0, 0, pl.ds(0, (blocks - 1) * (norm.shape[0] * norm.shape[1] // whole.shape[3]))]
        remote(some, some, norm_sem.at[0], norm_sem.at[1], me.partner()).wait_send()

    @pl.when(jnp.logical_not(leader))
    def _():
        fresh_copy().wait_send()
        remote(norm, norm, norm_sem.at[0], norm_sem.at[1], me.partner()).wait_recv()


def finish_kernel(whole, token, rest, send_sem, recv_sem):
    del token
    me = Place()

    @pl.when(me.core == LATE)
    def _():
        barrier = pltpu.get_barrier_semaphore()
        signal_all(barrier, [me.neighbour(d) for d in LINKS])
        pl.semaphore_wait(barrier, len(LINKS))
        for link, slot in LAST:
            off, q = SENDS[link][slot]
            unit = whole.at[me.at(off), q]
            remote(unit, rest.at[link, slot - SPLIT], send_sem, recv_sem, me.neighbour(LINKS[link])).start()
        remote(rest, rest, send_sem, recv_sem, me.partner()).wait()


def write_unit(source, block, quarter, outs, sems):
    out_query, out_key, out_value = outs
    rows, depth = source.shape
    part = out_query.shape[0] // QUARTERS
    half = rows - part
    at = pl.ds(pl.multiple_of(block * depth, depth), depth)
    small = (out_key if quarter < 2 else out_value).at[pl.ds((quarter % 2) * half, half), at]
    pltpu.make_async_copy(source.at[pl.ds(0, part)], out_query.at[pl.ds(quarter * part, part), at], sems[0]).start()
    pltpu.make_async_copy(source.at[pl.ds(part, half)], small, sems[1 + quarter // 2]).start()


def wait_units(count, unit_bytes, out, sem):
    rows = count * unit_bytes // (out.shape[1] * out.dtype.itemsize)
    same = out.at[pl.ds(0, rows)]
    pltpu.make_async_copy(same, same, sem).wait()


def unit_bytes_of(whole):
    return whole.shape[-2] * whole.shape[-1] * whole.dtype.itemsize


def write_kernel(whole, out_query, out_key, out_value, token, sem):
    me = Place()
    outs = (out_query, out_key, out_value)
    token[...] = jnp.zeros_like(token)
    late = {arriving(*unit) for unit in LAST}

    @pl.when(me.core == LATE)
    def _():
        count = 0
        for off in [(dz, dy) for dz in range(SIDE) for dy in range(SIDE)]:
            for q in range(QUARTERS):
                if (off, q) not in late:
                    count += 1
                    block = me.at(off)
                    write_unit(whole.at[block, q], block, q, outs, (sem, sem, sem))
        wait_units(count, unit_bytes_of(whole), out_query, sem)


def write_rest_kernel(
    whole, rest, norm, in_query, in_key, in_value, out_query, out_key, out_value, out_norm, sem, norm_sem
):
    del in_query, in_key, in_value
    me = Place()
    outs = (out_query, out_key, out_value)
    norm_copy = pltpu.make_async_copy(norm, out_norm, norm_sem)
    norm_copy.start()

    @pl.when(me.core == LATE)
    def _():
        first = sem.at[0]
        for link, slot in LAST:
            off, q = arriving(link, slot)
            write_unit(rest.at[link, slot - SPLIT], me.at(off), q, outs, (first, first, first))
        wait_units(len(LAST), unit_bytes_of(whole), out_query, first)

    @pl.when(me.core != LATE)
    def _():
        @pl.loop(0, whole.shape[0])
        def _(block):
            for q in range(QUARTERS):
                write_unit(whole.at[block, q], block, q, outs, [sem.at[n] for n in range(len(outs))])

        for n, out in enumerate(outs):
            pltpu.make_async_copy(out, out, sem.at[n]).wait()

    norm_copy.wait()


def body(
    train_query, low_query, high_query,
    train_key, low_key, high_key,
    train_value, low_value, high_value,
    norm_train, norm_step,
):
    n_rows, n_cols = lax.axis_size("rows"), lax.axis_size("cols")
    depth, wide = train_query.shape
    tall = train_key.shape[1]
    rank = low_query.shape[1]
    unit = (wide + 2 * tall) // QUARTERS
    values = norm_train.shape[0]
    line = CORES * values
    dtype = train_query.dtype
    f32 = jnp.float32
    anywhere = pl.BlockSpec(memory_space=pl.ANY)
    vmem = pl.BlockSpec(memory_space=pltpu.VMEM)
    dma = pltpu.SemaphoreType.DMA
    shape = jax.ShapeDtypeStruct

    def pin(space, *arrays):
        return [pltpu.with_memory_space_constraint(a, space) for a in arrays]

    whole, norm = pl.pallas_call(
        gather_kernel,
        out_shape=(
            shape((n_rows, QUARTERS, unit, depth), dtype),
            shape((n_rows * n_cols // CORES, line), dtype),
        ),
        in_specs=[anywhere] * 11,
        out_specs=(vmem, vmem),
        scratch_shapes=[
            pltpu.VMEM((depth, wide), dtype),
            pltpu.VMEM((rank, depth), dtype),
            pltpu.VMEM((rank, wide), dtype),
            pltpu.VMEM((tall, depth), dtype),
            pltpu.VMEM((rank, depth), dtype),
            pltpu.VMEM((rank, tall), dtype),
            pltpu.VMEM((tall, depth), dtype),
            pltpu.VMEM((rank, depth), dtype),
            pltpu.VMEM((rank, tall), dtype),
            pltpu.VMEM((1, values), f32),
            pltpu.VMEM((1, values), f32),
            pltpu.VMEM((1, line), f32),
            pltpu.VMEM((n_rows, 1, line), f32),
            pltpu.VMEM((n_cols, n_rows, line), f32),
            pltpu.VMEM((SIDE * n_rows, line), f32),
            dma((15,)),
            dma(()),
            dma((len(GROUPS),)),
            dma((2,)),
            dma((2,)),
            dma((2,)),
        ],
        compiler_params=pltpu.CompilerParams(
            collective_id=0, has_side_effects=True, vmem_limit_bytes=24 * 2**20
        ),
        name="gather",
    )(
        *pin(
            pltpu.HBM,
            train_query, low_query.T, high_query,
            train_key.T, low_key.T, high_key,
            train_value.T, low_value.T, high_value,
            norm_train.reshape(1, -1), norm_step.reshape(1, -1),
        )
    )
    outs = [shape((wide, n_rows * depth), dtype)] + [shape((tall, n_rows * depth), dtype)] * 2
    out_query, out_key, out_value, token = pl.pallas_call(
        write_kernel,
        out_shape=(*outs, shape((8, 128), f32)),
        in_specs=[vmem],
        out_specs=[anywhere] * 3 + [vmem],
        scratch_shapes=[dma(())],
        compiler_params=pltpu.CompilerParams(vmem_limit_bytes=4 * 2**20),
        name="write",
    )(*pin(pltpu.VMEM, whole))
    (rest,) = pl.pallas_call(
        finish_kernel,
        out_shape=(shape((len(LINKS), SLOTS - SPLIT, unit, depth), dtype),),
        in_specs=[vmem] * 2,
        out_specs=(vmem,),
        scratch_shapes=[dma(()), dma(())],
        compiler_params=pltpu.CompilerParams(
            collective_id=1, has_side_effects=True, vmem_limit_bytes=8 * 2**20
        ),
        name="finish",
    )(*pin(pltpu.VMEM, whole, token))
    out_query, out_key, out_value, out_norm = pl.pallas_call(
        write_rest_kernel,
        out_shape=(*outs, shape(norm.shape, dtype)),
        in_specs=[vmem] * 3 + [anywhere] * 3,
        out_specs=[anywhere] * 4,
        input_output_aliases={3: 0, 4: 1, 5: 2},
        scratch_shapes=[dma((len(outs),)), dma(())],
        compiler_params=pltpu.CompilerParams(vmem_limit_bytes=4 * 2**20),
        name="write_rest",
    )(*pin(pltpu.VMEM, whole, rest, norm), *pin(pltpu.HBM, out_query, out_key, out_value))
    return out_query, out_key, out_value, out_norm.reshape(-1)


def solution(mesh):
    return jax.shard_map(
        body,
        mesh=mesh,
        in_specs=(
            P("rows", "cols"),
            P("rows", None),
            P(None, "cols"),
            P("rows", "cols"),
            P("rows", None),
            P(None, "cols"),
            P("rows", "cols"),
            P("rows", None),
            P(None, "cols"),
            P(("rows", "cols")),
            P(("rows", "cols")),
        ),
        out_specs=(P("cols", None), P("cols", None), P("cols", None), P()),
        check_vma=False,
    )
```

```python
import jax
import jax.numpy as jnp
from jax import lax
from jax.experimental import pallas as pl
from jax.experimental.pallas import tpu as pltpu
from jax.sharding import PartitionSpec as P

MESH = pl.DeviceIdType.MESH

SIDE = 4
QUARTERS = 4
CORES = 2
LINKS = ((0, 1), (0, -1), (1, 0), (-1, 0))
LATE = 1
SPLIT = 12
ORDER = (0, 2, 1, 3)


def shift(off, d, sign=1):
    return ((off[0] + sign * d[0]) % SIDE, (off[1] + sign * d[1]) % SIDE)


def sends_of(link):
    d = LINKS[link]
    along_y = d[0] == 0
    first = (0, 1) if along_y else (2, 3)
    second = (2, 3) if along_y else (0, 1)
    positive = sum(d) > 0
    fwd_first = first[0] if positive else first[1]
    fwd_second = second[0] if positive else second[1]

    def across(n):
        return (n % SIDE, 0) if along_y else (0, n % SIDE)

    def behind(off):
        return shift(off, d, -1)

    own = (0, 0)
    return tuple((own, q) for q in ORDER) + (
        (across(-1), second[0]),
        (across(1), second[0]),
        (behind(own), fwd_first),
        (across(-1), second[1]),
        (across(1), second[1]),
        (behind(own), fwd_second),
        (across(2), second[0]),
        (across(2), second[1]),
        (behind(across(-1)), fwd_second),
        (behind(across(1)), fwd_second),
        (behind(across(2)), fwd_second),
    )


SENDS = tuple(sends_of(link) for link in range(len(LINKS)))
SLOTS = len(SENDS[0])
UNITS = [(link, slot) for slot in range(SLOTS) for link in range(len(LINKS))]


def arriving(link, slot):
    off, quarter = SENDS[link][slot]
    return shift(off, LINKS[link], -1), quarter


ARRIVES = {arriving(*unit): unit for unit in UNITS}
assert len(ARRIVES) == len(UNITS) == (SIDE * SIDE - 1) * QUARTERS
LAST = [unit for unit in UNITS if unit[1] >= SPLIT]
GROUPS = ((0, 1), (2, 3), (6,), (4, 5, 7, 8), (10, 11), (9,), (12, 13, 14))
GROUP_OF = {slot: group for group, slots in enumerate(GROUPS) for slot in slots}
assert sorted(GROUP_OF) == list(range(SLOTS)) and GROUPS[-1] == tuple(range(SPLIT, SLOTS))
AFTER = ((4, 5), (6, 7, 8, 9), (10, 11), (12, 13), (14,))
for _group, _slots in enumerate(AFTER):
    for _slot in _slots:
        for _link in range(len(LINKS)):
            assert GROUP_OF[ARRIVES[SENDS[_link][_slot]][1]] <= _group


class Place:
    def __init__(self):
        self.row, self.col = lax.axis_index("rows"), lax.axis_index("cols")
        self.z, self.y = self.row // SIDE, self.row % SIDE
        self.x, self.core = self.col // CORES, self.col % CORES

    def at(self, off):
        return ((self.z + off[0]) % SIDE) * SIDE + (self.y + off[1]) % SIDE

    def neighbour(self, d):
        return (self.at(d), self.col)

    def partner(self):
        return (self.row, self.x * CORES + 1 - self.core)

    def plane(self, n):
        return (self.row, (self.col + n) % (SIDE * CORES))


def remote(src, dst, send_sem, recv_sem, device):
    return pltpu.make_async_remote_copy(
        src_ref=src, dst_ref=dst, send_sem=send_sem, recv_sem=recv_sem, device_id=device, device_id_type=MESH
    )


def signal_all(barrier, devices):
    for device in devices:
        pl.semaphore_signal(barrier, inc=1, device_id=device, device_id_type=MESH)


def gather_kernel(
    train_query, low_query, high_query,
    train_key, low_key, high_key,
    train_value, low_value, high_value,
    norm_train, norm_step,
    whole, norm,
    tq, lq, hq, tk, lk, hk, tv, lv, hv, nt, ns, fresh, ring, lines, ordered,
    load_sem, send_sem, recv_sem, fresh_sem, column_sem, line_sem, norm_sem,
):
    me = Place()
    wide = tq.shape[1]
    part = wide // QUARTERS
    blocks = whole.shape[0]
    top = me.z == 0
    leader = top & (me.y == 0)
    head = top & (me.y != 0)
    n_planes = lines.shape[0]
    column = [(dz, 0) for dz in range(1, SIDE)]
    heads = [(0, dy) for dy in range(1, SIDE)]

    barrier = pltpu.get_barrier_semaphore()
    peers = [me.neighbour(d) for d in LINKS] + [me.partner()]
    signal_all(barrier, peers)

    @pl.when(top)
    def _():
        signal_all(barrier, [me.neighbour((2, 0))])

    @pl.when(leader)
    def _():
        signal_all(barrier, [me.neighbour((0, 2))] + [me.plane(n) for n in range(1, n_planes)])

    loads = {}

    def load(name, src, dst):
        copy = pltpu.make_async_copy(src, dst, load_sem.at[len(loads)])
        copy.start()
        loads[name] = copy

    pieces = [(ORDER[0], 0, part // 2), (ORDER[0], part // 2, part)] + [(q, 0, part) for q in ORDER[1:]]
    load("nt", norm_train, nt)
    load("ns", norm_step, ns)
    load("lq", low_query, lq)
    load("hq", high_query, hq)
    for n, (q, start, end) in enumerate(pieces):
        cols = pl.ds(q * part + start, end - start)
        load(n, train_query.at[:, cols], tq.at[:, cols])
        if n == 1:
            load("tk", train_key, tk)
            load("lk", low_key, lk)
            load("hk", high_key, hk)
        if n == 2:
            load("tv", train_value, tv)
            load("lv", low_value, lv)
            load("hv", high_value, hv)

    def merged(train, high, low):
        return train.astype(jnp.float32) + lax.dot_general(
            high, low, (((0,), (0,)), ((), ())), preferred_element_type=jnp.float32
        )

    def unit_copy(link, slot, what, rows=slice(None)):
        off, q = what
        unit = whole.at[me.at(off), q, rows]
        return remote(unit, unit, send_sem, recv_sem.at[GROUP_OF[slot]], me.neighbour(LINKS[link]))

    def send(link, slot, rows=slice(None)):
        unit_copy(link, slot, SENDS[link][slot], rows).start()

    def units(slots, sem):
        some = whole.at[pl.ds(0, slots * len(LINKS) // QUARTERS)]
        return remote(some, some, send_sem, sem, me.partner())

    def arrive(group):
        units(len(GROUPS[group]), recv_sem.at[group]).wait_recv()

    def only(core):
        return pl.when(me.core == LATE if core == LATE else me.core != LATE)

    def fresh_copy():
        return remote(fresh, ring.at[me.y * SIDE + me.z], fresh_sem.at[0], fresh_sem.at[1], (me.y, me.col))

    def column_copy():
        part_of_ring = ring.at[pl.ds(me.y * SIDE, SIDE)]
        return remote(part_of_ring, part_of_ring, column_sem.at[0], column_sem.at[1], (0, me.col))

    def ring_lines(count, sem):
        some = ring.at[pl.ds(0, count)]
        return remote(some, some, sem.at[0], sem.at[1], me.partner())

    def norm_copy(off):
        return remote(norm, norm, norm_sem.at[0], norm_sem.at[1], me.neighbour(off))

    def norm_sent(count):
        some = whole.at[0, 0, pl.ds(0, count * norm.shape[0] * norm.shape[1] // whole.shape[3])]
        remote(some, some, norm_sem.at[0], norm_sem.at[1], me.partner()).wait_send()

    def make_fresh():
        loads["nt"].wait()
        loads["ns"].wait()
        values = nt[...] + ns[...]
        fresh[...] = jnp.concatenate([values, values], axis=1)

    def send_fresh():
        @pl.when(top)
        def _():
            ring[me.y * SIDE + me.z] = fresh[...]

        @pl.when(jnp.logical_not(top))
        def _():
            fresh_copy().start()

    loads["lq"].wait()
    loads["hq"].wait()
    for n, (q, start, end) in enumerate(pieces):
        cols = pl.ds(q * part + start, end - start)
        loads[n].wait()
        if n == 1:
            make_fresh()
        whole[me.row, q, start:end, :] = merged(tq[:, cols].T, hq[:, cols], lq[...]).astype(whole.dtype)
        if n == 0:

            @pl.when(leader)
            def _():
                pl.semaphore_wait(barrier, len(peers) + n_planes - 1)

            far = (me.z == 2) | (top & (me.y == 2))

            @pl.when(far)
            def _():
                pl.semaphore_wait(barrier, len(peers) + 1)

            @pl.when(jnp.logical_not(leader | far))
            def _():
                pl.semaphore_wait(barrier, len(peers))

        if end == part:
            if n == 1:
                for name in ("tk", "lk", "hk"):
                    loads[name].wait()
            if n == 2:
                for name in ("tv", "lv", "hv"):
                    loads[name].wait()
            train, low, high = (tk, lk, hk) if q < 2 else (tv, lv, hv)
            small = merged(train[...], high[...], low[...]).astype(whole.dtype)
            half = small.shape[0] // 2
            whole[me.row, q, part:, :] = small[(q % 2) * half : (q % 2 + 1) * half, :]
        for link in range(len(LINKS)):
            if n == 0:
                send(link, 0, pl.ds(0, end))
            elif n == 1:
                send(link, 0, pl.ds(start, whole.shape[2] - start))
            else:
                send(link, ORDER.index(q))
        if n == 1:
            send_fresh()

    def norm_on_its_way(group):
        if group == 0:

            @pl.when(top)
            def _():
                ring_lines(len(column), fresh_sem).wait_recv()

            @pl.when(head)
            def _():
                column_copy().start()

        if group == 1:

            @pl.when(leader)
            def _():
                ring_lines(len(heads) * SIDE, column_sem).wait_recv()
                in_order = [ring[(i % SIDE) * SIDE + i // SIDE] for i in range(blocks)]
                lines[me.col] = jnp.concatenate(in_order, axis=0)
                for n in range(1, n_planes):
                    remote(lines.at[me.col], lines.at[me.col], line_sem.at[0], line_sem.at[1], me.plane(n)).start()
                some = lines.at[pl.ds(0, n_planes - 1)]
                remote(some, some, line_sem.at[0], line_sem.at[1], me.partner()).wait()
                lane = lax.broadcasted_iota(jnp.int32, lines.shape[1:], 1)
                for x in range(SIDE):
                    both = jnp.where(lane < lines.shape[2] // CORES, lines[CORES * x], lines[CORES * x + 1])
                    ordered[pl.Slice(x, blocks, SIDE), :] = both
                norm[...] = ordered[...].astype(norm.dtype)
                for off in heads + column:
                    norm_copy(off).start()

        if group == 2:

            @pl.when(head)
            def _():
                norm_copy((1, 0)).wait_recv()
                for off in column:
                    norm_copy(off).start()

    def send_slots(slots):
        for slot in slots:
            for link in range(len(LINKS)):
                send(link, slot)

    for group, slots in enumerate(AFTER):
        arrive(group)
        norm_on_its_way(group)
        if slots[0] < SPLIT:
            send_slots(slots)
        else:

            @only(1 - LATE)
            def _():
                send_slots(slots)

    arrive(5)

    @only(1 - LATE)
    def _():
        arrive(6)
        units(SLOTS, recv_sem.at[0]).wait_send()

    @only(LATE)
    def _():
        units(SPLIT, recv_sem.at[0]).wait_send()

    @pl.when(leader)
    def _():
        norm_sent(len(heads) + len(column))

    @pl.when(head)
    def _():
        column_copy().wait_send()
        norm_sent(len(column))

    @pl.when(jnp.logical_not(top))
    def _():
        fresh_copy().wait_send()
        norm_copy((1, 0)).wait_recv()


def finish_kernel(whole, token, rest, send_sem, recv_sem):
    del token
    me = Place()

    @pl.when(me.core == LATE)
    def _():
        barrier = pltpu.get_barrier_semaphore()
        signal_all(barrier, [me.neighbour(d) for d in LINKS])
        pl.semaphore_wait(barrier, len(LINKS))
        for link, slot in LAST:
            off, q = SENDS[link][slot]
            unit = whole.at[me.at(off), q]
            remote(unit, rest.at[link, slot - SPLIT], send_sem, recv_sem, me.neighbour(LINKS[link])).start()
        remote(rest, rest, send_sem, recv_sem, me.partner()).wait()


def write_unit(source, block, quarter, outs, sems):
    out_query, out_key, out_value = outs
    rows, depth = source.shape
    part = out_query.shape[0] // QUARTERS
    half = rows - part
    at = pl.ds(pl.multiple_of(block * depth, depth), depth)
    small = (out_key if quarter < 2 else out_value).at[pl.ds((quarter % 2) * half, half), at]
    pltpu.make_async_copy(source.at[pl.ds(0, part)], out_query.at[pl.ds(quarter * part, part), at], sems[0]).start()
    pltpu.make_async_copy(source.at[pl.ds(part, half)], small, sems[1 + quarter // 2]).start()


def wait_units(count, unit_bytes, out, sem):
    rows = count * unit_bytes // (out.shape[1] * out.dtype.itemsize)
    same = out.at[pl.ds(0, rows)]
    pltpu.make_async_copy(same, same, sem).wait()


def unit_bytes_of(whole):
    return whole.shape[-2] * whole.shape[-1] * whole.dtype.itemsize


def write_kernel(whole, out_query, out_key, out_value, token, sem):
    me = Place()
    outs = (out_query, out_key, out_value)
    token[...] = jnp.zeros_like(token)
    late = {arriving(*unit) for unit in LAST}

    @pl.when(me.core == LATE)
    def _():
        count = 0
        for off in [(dz, dy) for dz in range(SIDE) for dy in range(SIDE)]:
            for q in range(QUARTERS):
                if (off, q) not in late:
                    count += 1
                    block = me.at(off)
                    write_unit(whole.at[block, q], block, q, outs, (sem, sem, sem))
        wait_units(count, unit_bytes_of(whole), out_query, sem)


def write_rest_kernel(
    whole, rest, norm, in_query, in_key, in_value, out_query, out_key, out_value, out_norm, sem, norm_sem
):
    del in_query, in_key, in_value
    me = Place()
    outs = (out_query, out_key, out_value)
    norm_copy = pltpu.make_async_copy(norm, out_norm, norm_sem)
    norm_copy.start()

    @pl.when(me.core == LATE)
    def _():
        first = sem.at[0]
        for link, slot in LAST:
            off, q = arriving(link, slot)
            write_unit(rest.at[link, slot - SPLIT], me.at(off), q, outs, (first, first, first))
        wait_units(len(LAST), unit_bytes_of(whole), out_query, first)

    @pl.when(me.core != LATE)
    def _():
        @pl.loop(0, whole.shape[0])
        def _(block):
            for q in range(QUARTERS):
                write_unit(whole.at[block, q], block, q, outs, [sem.at[n] for n in range(len(outs))])

        for n, out in enumerate(outs):
            pltpu.make_async_copy(out, out, sem.at[n]).wait()

    norm_copy.wait()


def body(
    train_query, low_query, high_query,
    train_key, low_key, high_key,
    train_value, low_value, high_value,
    norm_train, norm_step,
):
    n_rows, n_cols = lax.axis_size("rows"), lax.axis_size("cols")
    depth, wide = train_query.shape
    tall = train_key.shape[1]
    rank = low_query.shape[1]
    unit = (wide + 2 * tall) // QUARTERS
    values = norm_train.shape[0]
    line = CORES * values
    dtype = train_query.dtype
    f32 = jnp.float32
    anywhere = pl.BlockSpec(memory_space=pl.ANY)
    vmem = pl.BlockSpec(memory_space=pltpu.VMEM)
    dma = pltpu.SemaphoreType.DMA
    shape = jax.ShapeDtypeStruct

    def pin(space, *arrays):
        return [pltpu.with_memory_space_constraint(a, space) for a in arrays]

    whole, norm = pl.pallas_call(
        gather_kernel,
        out_shape=(
            shape((n_rows, QUARTERS, unit, depth), dtype),
            shape((n_rows * n_cols // CORES, line), dtype),
        ),
        in_specs=[anywhere] * 11,
        out_specs=(vmem, vmem),
        scratch_shapes=[
            pltpu.VMEM((depth, wide), dtype),
            pltpu.VMEM((rank, depth), dtype),
            pltpu.VMEM((rank, wide), dtype),
            pltpu.VMEM((tall, depth), dtype),
            pltpu.VMEM((rank, depth), dtype),
            pltpu.VMEM((rank, tall), dtype),
            pltpu.VMEM((tall, depth), dtype),
            pltpu.VMEM((rank, depth), dtype),
            pltpu.VMEM((rank, tall), dtype),
            pltpu.VMEM((1, values), f32),
            pltpu.VMEM((1, values), f32),
            pltpu.VMEM((1, line), f32),
            pltpu.VMEM((n_rows, 1, line), f32),
            pltpu.VMEM((n_cols, n_rows, line), f32),
            pltpu.VMEM((SIDE * n_rows, line), f32),
            dma((15,)),
            dma(()),
            dma((len(GROUPS),)),
            dma((2,)),
            dma((2,)),
            dma((2,)),
            dma((2,)),
        ],
        compiler_params=pltpu.CompilerParams(
            collective_id=0, has_side_effects=True, vmem_limit_bytes=24 * 2**20
        ),
        name="gather",
    )(
        *pin(
            pltpu.HBM,
            train_query, low_query.T, high_query,
            train_key.T, low_key.T, high_key,
            train_value.T, low_value.T, high_value,
            norm_train.reshape(1, -1), norm_step.reshape(1, -1),
        )
    )
    outs = [shape((wide, n_rows * depth), dtype)] + [shape((tall, n_rows * depth), dtype)] * 2
    out_query, out_key, out_value, token = pl.pallas_call(
        write_kernel,
        out_shape=(*outs, shape((8, 128), f32)),
        in_specs=[vmem],
        out_specs=[anywhere] * 3 + [vmem],
        scratch_shapes=[dma(())],
        compiler_params=pltpu.CompilerParams(vmem_limit_bytes=4 * 2**20),
        name="write",
    )(*pin(pltpu.VMEM, whole))
    (rest,) = pl.pallas_call(
        finish_kernel,
        out_shape=(shape((len(LINKS), SLOTS - SPLIT, unit, depth), dtype),),
        in_specs=[vmem] * 2,
        out_specs=(vmem,),
        scratch_shapes=[dma(()), dma(())],
        compiler_params=pltpu.CompilerParams(
            collective_id=1, has_side_effects=True, vmem_limit_bytes=8 * 2**20
        ),
        name="finish",
    )(*pin(pltpu.VMEM, whole, token))
    out_query, out_key, out_value, out_norm = pl.pallas_call(
        write_rest_kernel,
        out_shape=(*outs, shape(norm.shape, dtype)),
        in_specs=[vmem] * 3 + [anywhere] * 3,
        out_specs=[anywhere] * 4,
        input_output_aliases={3: 0, 4: 1, 5: 2},
        scratch_shapes=[dma((len(outs),)), dma(())],
        compiler_params=pltpu.CompilerParams(vmem_limit_bytes=4 * 2**20),
        name="write_rest",
    )(*pin(pltpu.VMEM, whole, rest, norm), *pin(pltpu.HBM, out_query, out_key, out_value))
    return out_query, out_key, out_value, out_norm.reshape(-1)


def solution(mesh):
    return jax.shard_map(
        body,
        mesh=mesh,
        in_specs=(
            P("rows", "cols"),
            P("rows", None),
            P(None, "cols"),
            P("rows", "cols"),
            P("rows", None),
            P(None, "cols"),
            P("rows", "cols"),
            P("rows", None),
            P(None, "cols"),
            P(("rows", "cols")),
            P(("rows", "cols")),
        ),
        out_specs=(P("cols", None), P("cols", None), P("cols", None), P()),
        check_vma=False,
    )
```

```python
import jax
import jax.numpy as jnp
from jax import lax
from jax.experimental import pallas as pl
from jax.experimental.pallas import tpu as pltpu
from jax.sharding import PartitionSpec as P

MESH = pl.DeviceIdType.MESH

SIDE = 4
QUARTERS = 4
CORES = 2
LINKS = ((0, 1), (0, -1), (1, 0), (-1, 0))
LATE = 1
SPLIT = 12
LEAD = 2
ORDER = (0, 2, 1, 3)


def shift(off, d, sign=1):
    return ((off[0] + sign * d[0]) % SIDE, (off[1] + sign * d[1]) % SIDE)


def sends_of(link):
    d = LINKS[link]
    along_y = d[0] == 0
    first = (0, 1) if along_y else (2, 3)
    second = (2, 3) if along_y else (0, 1)
    positive = sum(d) > 0
    fwd_first = first[0] if positive else first[1]
    fwd_second = second[0] if positive else second[1]

    def across(n):
        return (n % SIDE, 0) if along_y else (0, n % SIDE)

    def behind(off):
        return shift(off, d, -1)

    own = (0, 0)
    return tuple((own, q) for q in ORDER) + (
        (across(-1), second[0]),
        (across(1), second[0]),
        (behind(own), fwd_first),
        (across(-1), second[1]),
        (across(1), second[1]),
        (behind(own), fwd_second),
        (across(2), second[0]),
        (across(2), second[1]),
        (behind(across(-1)), fwd_second),
        (behind(across(1)), fwd_second),
        (behind(across(2)), fwd_second),
    )


SENDS = tuple(sends_of(link) for link in range(len(LINKS)))
SLOTS = len(SENDS[0])
UNITS = [(link, slot) for slot in range(SLOTS) for link in range(len(LINKS))]


def arriving(link, slot):
    off, quarter = SENDS[link][slot]
    return shift(off, LINKS[link], -1), quarter


ARRIVES = {arriving(*unit): unit for unit in UNITS}
assert len(ARRIVES) == len(UNITS) == (SIDE * SIDE - 1) * QUARTERS
LAST = [unit for unit in UNITS if unit[1] >= SPLIT]
GROUPS = ((0, 1), (2, 3), (6,), (4, 5, 7, 8), (10, 11), (9,), (12, 13, 14))
GROUP_OF = {slot: group for group, slots in enumerate(GROUPS) for slot in slots}
assert sorted(GROUP_OF) == list(range(SLOTS)) and GROUPS[-1] == tuple(range(SPLIT, SLOTS))
AFTER = ((4, 5), (6, 7, 8, 9), (10, 11), (12, 13), (14,))
for _group, _slots in enumerate(AFTER):
    for _slot in _slots:
        for _link in range(len(LINKS)):
            assert GROUP_OF[ARRIVES[SENDS[_link][_slot]][1]] <= _group


class Place:
    def __init__(self):
        self.row, self.col = lax.axis_index("rows"), lax.axis_index("cols")
        self.z, self.y = self.row // SIDE, self.row % SIDE
        self.x, self.core = self.col // CORES, self.col % CORES

    def at(self, off):
        return ((self.z + off[0]) % SIDE) * SIDE + (self.y + off[1]) % SIDE

    def neighbour(self, d):
        return (self.at(d), self.col)

    def partner(self):
        return (self.row, self.x * CORES + 1 - self.core)

    def plane(self, n):
        return (self.row, (self.col + n) % (SIDE * CORES))


def remote(src, dst, send_sem, recv_sem, device):
    return pltpu.make_async_remote_copy(
        src_ref=src, dst_ref=dst, send_sem=send_sem, recv_sem=recv_sem, device_id=device, device_id_type=MESH
    )


def signal_all(barrier, devices):
    for device in devices:
        pl.semaphore_signal(barrier, inc=1, device_id=device, device_id_type=MESH)


def gather_kernel(
    train_query, low_query, high_query,
    train_key, low_key, high_key,
    train_value, low_value, high_value,
    norm_train, norm_step,
    whole, norm,
    tq, lq, hq, tk, lk, hk, tv, lv, hv, nt, ns, fresh, ring, lines, ordered,
    load_sem, send_sem, recv_sem, fresh_sem, column_sem, line_sem, norm_sem,
):
    me = Place()
    wide = tq.shape[1]
    part = wide // QUARTERS
    blocks = whole.shape[0]
    top = me.z == 0
    leader = top & (me.y == LEAD)
    head = top & (me.y != LEAD)
    n_planes = lines.shape[0]
    column = [(dz, 0) for dz in range(1, SIDE)]
    heads = [(0, dy) for dy in range(1, SIDE)]

    barrier = pltpu.get_barrier_semaphore()
    peers = [me.neighbour(d) for d in LINKS] + [me.partner()]

    def greet():
        signal_all(barrier, peers)

        @pl.when(top)
        def _():
            signal_all(barrier, [me.neighbour((2, 0))])

        @pl.when(leader)
        def _():
            signal_all(barrier, [me.neighbour((0, 2))] + [me.plane(n) for n in range(1, n_planes)])

    loads = {}

    def load(name, src, dst):
        copy = pltpu.make_async_copy(src, dst, load_sem.at[len(loads)])
        copy.start()
        loads[name] = copy

    pieces = [(ORDER[0], 0, part // 2), (ORDER[0], part // 2, part)] + [(q, 0, part) for q in ORDER[1:]]
    load("lq", low_query, lq)
    load("hq", high_query, hq)
    for n, (q, start, end) in enumerate(pieces):
        cols = pl.ds(q * part + start, end - start)
        load(n, train_query.at[:, cols], tq.at[:, cols])
        if n == 0:
            greet()
            load("nt", norm_train, nt)
            load("ns", norm_step, ns)
        if n == 1:
            load("tk", train_key, tk)
            load("lk", low_key, lk)
            load("hk", high_key, hk)
        if n == 2:
            load("tv", train_value, tv)
            load("lv", low_value, lv)
            load("hv", high_value, hv)

    def merged(train, high, low):
        return train.astype(jnp.float32) + lax.dot_general(
            high, low, (((0,), (0,)), ((), ())), preferred_element_type=jnp.float32
        )

    def unit_copy(link, slot, what, rows=slice(None)):
        off, q = what
        unit = whole.at[me.at(off), q, rows]
        return remote(unit, unit, send_sem, recv_sem.at[GROUP_OF[slot]], me.neighbour(LINKS[link]))

    def send(link, slot, rows=slice(None)):
        unit_copy(link, slot, SENDS[link][slot], rows).start()

    def units(slots, sem):
        some = whole.at[pl.ds(0, slots * len(LINKS) // QUARTERS)]
        return remote(some, some, send_sem, sem, me.partner())

    def arrive(group):
        units(len(GROUPS[group]), recv_sem.at[group]).wait_recv()

    def only(core):
        return pl.when(me.core == LATE if core == LATE else me.core != LATE)

    def fresh_copy():
        return remote(fresh, ring.at[me.y * SIDE + me.z], fresh_sem.at[0], fresh_sem.at[1], (me.y, me.col))

    def column_copy():
        part_of_ring = ring.at[pl.ds(me.y * SIDE, SIDE)]
        return remote(part_of_ring, part_of_ring, column_sem.at[0], column_sem.at[1], (LEAD, me.col))

    def ring_lines(count, sem):
        some = ring.at[pl.ds(0, count)]
        return remote(some, some, sem.at[0], sem.at[1], me.partner())

    def norm_copy(off):
        return remote(norm, norm, norm_sem.at[0], norm_sem.at[1], me.neighbour(off))

    def norm_sent(count):
        some = whole.at[0, 0, pl.ds(0, count * norm.shape[0] * norm.shape[1] // whole.shape[3])]
        remote(some, some, norm_sem.at[0], norm_sem.at[1], me.partner()).wait_send()

    def make_fresh():
        loads["nt"].wait()
        loads["ns"].wait()
        values = nt[...] + ns[...]
        fresh[...] = jnp.concatenate([values, values], axis=1)

    def send_fresh():
        @pl.when(top)
        def _():
            ring[me.y * SIDE + me.z] = fresh[...]

        @pl.when(jnp.logical_not(top))
        def _():
            fresh_copy().start()

    loads["lq"].wait()
    loads["hq"].wait()
    for n, (q, start, end) in enumerate(pieces):
        cols = pl.ds(q * part + start, end - start)
        loads[n].wait()
        if n == 1:
            make_fresh()
        whole[me.row, q, start:end, :] = merged(tq[:, cols].T, hq[:, cols], lq[...]).astype(whole.dtype)
        if n == 0:

            @pl.when(leader)
            def _():
                pl.semaphore_wait(barrier, len(peers) + n_planes - 1)

            far = (me.z == 2) | (top & (me.y == (LEAD + 2) % SIDE))

            @pl.when(far)
            def _():
                pl.semaphore_wait(barrier, len(peers) + 1)

            @pl.when(jnp.logical_not(leader | far))
            def _():
                pl.semaphore_wait(barrier, len(peers))

        if end == part:
            if n == 1:
                for name in ("tk", "lk", "hk"):
                    loads[name].wait()
            if n == 2:
                for name in ("tv", "lv", "hv"):
                    loads[name].wait()
            train, low, high = (tk, lk, hk) if q < 2 else (tv, lv, hv)
            small = merged(train[...], high[...], low[...]).astype(whole.dtype)
            half = small.shape[0] // 2
            whole[me.row, q, part:, :] = small[(q % 2) * half : (q % 2 + 1) * half, :]
        for link in range(len(LINKS)):
            if n == 0:
                send(link, 0, pl.ds(0, end))
            elif n == 1:
                send(link, 0, pl.ds(start, whole.shape[2] - start))
            else:
                send(link, ORDER.index(q))
        if n == 1:
            send_fresh()

    def norm_on_its_way(group):
        if group == 0:

            @pl.when(top)
            def _():
                ring_lines(len(column), fresh_sem).wait_recv()

            @pl.when(head)
            def _():
                column_copy().start()

        if group == 1:

            @pl.when(leader)
            def _():
                ring_lines(len(heads) * SIDE, column_sem).wait_recv()
                in_order = [ring[(i % SIDE) * SIDE + i // SIDE] for i in range(blocks)]
                lines[me.col] = jnp.concatenate(in_order, axis=0)
                for n in range(1, n_planes):
                    remote(lines.at[me.col], lines.at[me.col], line_sem.at[0], line_sem.at[1], me.plane(n)).start()
                some = lines.at[pl.ds(0, n_planes - 1)]
                remote(some, some, line_sem.at[0], line_sem.at[1], me.partner()).wait()
                lane = lax.broadcasted_iota(jnp.int32, lines.shape[1:], 1)
                for x in range(SIDE):
                    both = jnp.where(lane < lines.shape[2] // CORES, lines[CORES * x], lines[CORES * x + 1])
                    ordered[pl.Slice(x, blocks, SIDE), :] = both
                norm[...] = ordered[...].astype(norm.dtype)
                for off in heads + column:
                    norm_copy(off).start()

        if group == 2:

            @pl.when(head)
            def _():
                norm_copy((1, 0)).wait_recv()
                for off in column:
                    norm_copy(off).start()

    def send_slots(slots):
        for slot in slots:
            for link in range(len(LINKS)):
                send(link, slot)

    for group, slots in enumerate(AFTER):
        arrive(group)
        norm_on_its_way(group)
        if slots[0] < SPLIT:
            send_slots(slots)
        else:

            @only(1 - LATE)
            def _():
                send_slots(slots)

    arrive(5)

    @only(1 - LATE)
    def _():
        arrive(6)
        units(SLOTS, recv_sem.at[0]).wait_send()

    @only(LATE)
    def _():
        units(SPLIT, recv_sem.at[0]).wait_send()

    @pl.when(leader)
    def _():
        norm_sent(len(heads) + len(column))

    @pl.when(head)
    def _():
        column_copy().wait_send()
        norm_sent(len(column))

    @pl.when(jnp.logical_not(top))
    def _():
        fresh_copy().wait_send()
        norm_copy((1, 0)).wait_recv()


def finish_kernel(whole, token, rest, send_sem, recv_sem):
    del token
    me = Place()

    @pl.when(me.core == LATE)
    def _():
        barrier = pltpu.get_barrier_semaphore()
        signal_all(barrier, [me.neighbour(d) for d in LINKS])
        pl.semaphore_wait(barrier, len(LINKS))
        for link, slot in LAST:
            off, q = SENDS[link][slot]
            unit = whole.at[me.at(off), q]
            remote(unit, rest.at[link, slot - SPLIT], send_sem, recv_sem, me.neighbour(LINKS[link])).start()
        remote(rest, rest, send_sem, recv_sem, me.partner()).wait()


def write_unit(source, block, quarter, outs, sems):
    out_query, out_key, out_value = outs
    rows, depth = source.shape
    part = out_query.shape[0] // QUARTERS
    half = rows - part
    at = pl.ds(pl.multiple_of(block * depth, depth), depth)
    small = (out_key if quarter < 2 else out_value).at[pl.ds((quarter % 2) * half, half), at]
    pltpu.make_async_copy(source.at[pl.ds(0, part)], out_query.at[pl.ds(quarter * part, part), at], sems[0]).start()
    pltpu.make_async_copy(source.at[pl.ds(part, half)], small, sems[1 + quarter // 2]).start()


def wait_units(count, unit_bytes, out, sem):
    rows = count * unit_bytes // (out.shape[1] * out.dtype.itemsize)
    same = out.at[pl.ds(0, rows)]
    pltpu.make_async_copy(same, same, sem).wait()


def unit_bytes_of(whole):
    return whole.shape[-2] * whole.shape[-1] * whole.dtype.itemsize


def write_kernel(whole, out_query, out_key, out_value, token, sem):
    me = Place()
    outs = (out_query, out_key, out_value)
    token[...] = jnp.zeros_like(token)
    late = {arriving(*unit) for unit in LAST}

    @pl.when(me.core == LATE)
    def _():
        count = 0
        for off in [(dz, dy) for dz in range(SIDE) for dy in range(SIDE)]:
            for q in range(QUARTERS):
                if (off, q) not in late:
                    count += 1
                    block = me.at(off)
                    write_unit(whole.at[block, q], block, q, outs, (sem, sem, sem))
        wait_units(count, unit_bytes_of(whole), out_query, sem)


def write_rest_kernel(
    whole, rest, norm, in_query, in_key, in_value, out_query, out_key, out_value, out_norm, sem, norm_sem
):
    del in_query, in_key, in_value
    me = Place()
    outs = (out_query, out_key, out_value)
    norm_copy = pltpu.make_async_copy(norm, out_norm, norm_sem)
    norm_copy.start()

    @pl.when(me.core == LATE)
    def _():
        first = sem.at[0]
        for link, slot in LAST:
            off, q = arriving(link, slot)
            write_unit(rest.at[link, slot - SPLIT], me.at(off), q, outs, (first, first, first))
        wait_units(len(LAST), unit_bytes_of(whole), out_query, first)

    @pl.when(me.core != LATE)
    def _():
        @pl.loop(0, whole.shape[0])
        def _(block):
            for q in range(QUARTERS):
                write_unit(whole.at[block, q], block, q, outs, [sem.at[n] for n in range(len(outs))])

        for n, out in enumerate(outs):
            pltpu.make_async_copy(out, out, sem.at[n]).wait()

    norm_copy.wait()


def body(
    train_query, low_query, high_query,
    train_key, low_key, high_key,
    train_value, low_value, high_value,
    norm_train, norm_step,
):
    n_rows, n_cols = lax.axis_size("rows"), lax.axis_size("cols")
    depth, wide = train_query.shape
    tall = train_key.shape[1]
    rank = low_query.shape[1]
    unit = (wide + 2 * tall) // QUARTERS
    values = norm_train.shape[0]
    line = CORES * values
    dtype = train_query.dtype
    f32 = jnp.float32
    anywhere = pl.BlockSpec(memory_space=pl.ANY)
    vmem = pl.BlockSpec(memory_space=pltpu.VMEM)
    dma = pltpu.SemaphoreType.DMA
    shape = jax.ShapeDtypeStruct

    def pin(space, *arrays):
        return [pltpu.with_memory_space_constraint(a, space) for a in arrays]

    whole, norm = pl.pallas_call(
        gather_kernel,
        out_shape=(
            shape((n_rows, QUARTERS, unit, depth), dtype),
            shape((n_rows * n_cols // CORES, line), dtype),
        ),
        in_specs=[anywhere] * 11,
        out_specs=(vmem, vmem),
        scratch_shapes=[
            pltpu.VMEM((depth, wide), dtype),
            pltpu.VMEM((rank, depth), dtype),
            pltpu.VMEM((rank, wide), dtype),
            pltpu.VMEM((tall, depth), dtype),
            pltpu.VMEM((rank, depth), dtype),
            pltpu.VMEM((rank, tall), dtype),
            pltpu.VMEM((tall, depth), dtype),
            pltpu.VMEM((rank, depth), dtype),
            pltpu.VMEM((rank, tall), dtype),
            pltpu.VMEM((1, values), f32),
            pltpu.VMEM((1, values), f32),
            pltpu.VMEM((1, line), f32),
            pltpu.VMEM((n_rows, 1, line), f32),
            pltpu.VMEM((n_cols, n_rows, line), f32),
            pltpu.VMEM((SIDE * n_rows, line), f32),
            dma((15,)),
            dma(()),
            dma((len(GROUPS),)),
            dma((2,)),
            dma((2,)),
            dma((2,)),
            dma((2,)),
        ],
        compiler_params=pltpu.CompilerParams(
            collective_id=0, has_side_effects=True, vmem_limit_bytes=24 * 2**20
        ),
        name="gather",
    )(
        *pin(
            pltpu.HBM,
            train_query, low_query.T, high_query,
            train_key.T, low_key.T, high_key,
            train_value.T, low_value.T, high_value,
            norm_train.reshape(1, -1), norm_step.reshape(1, -1),
        )
    )
    outs = [shape((wide, n_rows * depth), dtype)] + [shape((tall, n_rows * depth), dtype)] * 2
    out_query, out_key, out_value, token = pl.pallas_call(
        write_kernel,
        out_shape=(*outs, shape((8, 128), f32)),
        in_specs=[vmem],
        out_specs=[anywhere] * 3 + [vmem],
        scratch_shapes=[dma(())],
        compiler_params=pltpu.CompilerParams(vmem_limit_bytes=4 * 2**20),
        name="write",
    )(*pin(pltpu.VMEM, whole))
    (rest,) = pl.pallas_call(
        finish_kernel,
        out_shape=(shape((len(LINKS), SLOTS - SPLIT, unit, depth), dtype),),
        in_specs=[vmem] * 2,
        out_specs=(vmem,),
        scratch_shapes=[dma(()), dma(())],
        compiler_params=pltpu.CompilerParams(
            collective_id=1, has_side_effects=True, vmem_limit_bytes=8 * 2**20
        ),
        name="finish",
    )(*pin(pltpu.VMEM, whole, token))
    out_query, out_key, out_value, out_norm = pl.pallas_call(
        write_rest_kernel,
        out_shape=(*outs, shape(norm.shape, dtype)),
        in_specs=[vmem] * 3 + [anywhere] * 3,
        out_specs=[anywhere] * 4,
        input_output_aliases={3: 0, 4: 1, 5: 2},
        scratch_shapes=[dma((len(outs),)), dma(())],
        compiler_params=pltpu.CompilerParams(vmem_limit_bytes=4 * 2**20),
        name="write_rest",
    )(*pin(pltpu.VMEM, whole, rest, norm), *pin(pltpu.HBM, out_query, out_key, out_value))
    return out_query, out_key, out_value, out_norm.reshape(-1)


def solution(mesh):
    return jax.shard_map(
        body,
        mesh=mesh,
        in_specs=(
            P("rows", "cols"),
            P("rows", None),
            P(None, "cols"),
            P("rows", "cols"),
            P("rows", None),
            P(None, "cols"),
            P("rows", "cols"),
            P("rows", None),
            P(None, "cols"),
            P(("rows", "cols")),
            P(("rows", "cols")),
        ),
        out_specs=(P("cols", None), P("cols", None), P("cols", None), P()),
        check_vma=False,
    )
```

```python
import jax
import jax.numpy as jnp
from jax import lax
from jax.experimental import pallas as pl
from jax.experimental.pallas import tpu as pltpu
from jax.sharding import PartitionSpec as P

MESH = pl.DeviceIdType.MESH

SIDE = 4
QUARTERS = 4
CORES = 2
LINKS = ((0, 1), (0, -1), (1, 0), (-1, 0))
LATE = 1
SPLIT = 12
CUT = 128
LEAD = 2
ORDER = (0, 2, 1, 3)


def shift(off, d, sign=1):
    return ((off[0] + sign * d[0]) % SIDE, (off[1] + sign * d[1]) % SIDE)


def sends_of(link):
    d = LINKS[link]
    along_y = d[0] == 0
    first = (0, 1) if along_y else (2, 3)
    second = (2, 3) if along_y else (0, 1)
    positive = sum(d) > 0
    fwd_first = first[0] if positive else first[1]
    fwd_second = second[0] if positive else second[1]

    def across(n):
        return (n % SIDE, 0) if along_y else (0, n % SIDE)

    def behind(off):
        return shift(off, d, -1)

    own = (0, 0)
    return tuple((own, q) for q in ORDER) + (
        (across(-1), second[0]),
        (across(1), second[0]),
        (behind(own), fwd_first),
        (across(-1), second[1]),
        (across(1), second[1]),
        (behind(own), fwd_second),
        (across(2), second[0]),
        (across(2), second[1]),
        (behind(across(-1)), fwd_second),
        (behind(across(1)), fwd_second),
        (behind(across(2)), fwd_second),
    )


SENDS = tuple(sends_of(link) for link in range(len(LINKS)))
SLOTS = len(SENDS[0])
UNITS = [(link, slot) for slot in range(SLOTS) for link in range(len(LINKS))]


def arriving(link, slot):
    off, quarter = SENDS[link][slot]
    return shift(off, LINKS[link], -1), quarter


ARRIVES = {arriving(*unit): unit for unit in UNITS}
assert len(ARRIVES) == len(UNITS) == (SIDE * SIDE - 1) * QUARTERS
LAST = [unit for unit in UNITS if unit[1] >= SPLIT]
FINAL = SLOTS - 1
assert all(arriving(link, FINAL)[0] == (2, 2) for link in range(len(LINKS)))
GROUPS = ((0, 1), (2, 3), (6,), (4, 5, 7, 8), (10, 11), (9,), (12, 13), (14,))
GROUP_OF = {slot: group for group, slots in enumerate(GROUPS) for slot in slots}
assert sorted(GROUP_OF) == list(range(SLOTS)) and GROUPS[-2] + GROUPS[-1] == tuple(range(SPLIT, SLOTS))
AFTER = ((4, 5), (6, 7, 8, 9), (10, 11), (12, 13), (14,))
for _group, _slots in enumerate(AFTER):
    for _slot in _slots:
        for _link in range(len(LINKS)):
            assert GROUP_OF[ARRIVES[SENDS[_link][_slot]][1]] <= _group


class Place:
    def __init__(self):
        self.row, self.col = lax.axis_index("rows"), lax.axis_index("cols")
        self.z, self.y = self.row // SIDE, self.row % SIDE
        self.x, self.core = self.col // CORES, self.col % CORES

    def at(self, off):
        return ((self.z + off[0]) % SIDE) * SIDE + (self.y + off[1]) % SIDE

    def neighbour(self, d):
        return (self.at(d), self.col)

    def partner(self):
        return (self.row, self.x * CORES + 1 - self.core)

    def plane(self, n):
        return (self.row, (self.col + n) % (SIDE * CORES))


def remote(src, dst, send_sem, recv_sem, device):
    return pltpu.make_async_remote_copy(
        src_ref=src, dst_ref=dst, send_sem=send_sem, recv_sem=recv_sem, device_id=device, device_id_type=MESH
    )


def signal_all(barrier, devices):
    for device in devices:
        pl.semaphore_signal(barrier, inc=1, device_id=device, device_id_type=MESH)


def gather_kernel(
    train_query, low_query, high_query,
    train_key, low_key, high_key,
    train_value, low_value, high_value,
    norm_train, norm_step,
    whole, norm,
    tq, lq, hq, tk, lk, hk, tv, lv, hv, nt, ns, fresh, ring, lines, ordered,
    load_sem, send_sem, cut_sem, recv_sem, fresh_sem, column_sem, line_sem, norm_sem,
):
    me = Place()
    wide = tq.shape[1]
    part = wide // QUARTERS
    blocks = whole.shape[0]
    top = me.z == 0
    leader = top & (me.y == LEAD)
    head = top & (me.y != LEAD)
    n_planes = lines.shape[0]
    column = [(dz, 0) for dz in range(1, SIDE)]
    heads = [(0, dy) for dy in range(1, SIDE)]

    barrier = pltpu.get_barrier_semaphore()
    peers = [me.neighbour(d) for d in LINKS] + [me.partner()]

    def greet():
        signal_all(barrier, peers)

        @pl.when(top)
        def _():
            signal_all(barrier, [me.neighbour((2, 0))])

        @pl.when(leader)
        def _():
            signal_all(barrier, [me.neighbour((0, 2))] + [me.plane(n) for n in range(1, n_planes)])

    loads = {}

    def load(name, src, dst):
        copy = pltpu.make_async_copy(src, dst, load_sem.at[len(loads)])
        copy.start()
        loads[name] = copy

    pieces = [(ORDER[0], 0, part // 2), (ORDER[0], part // 2, part)] + [(q, 0, part) for q in ORDER[1:]]
    load("lq", low_query, lq)
    load("hq", high_query, hq)
    for n, (q, start, end) in enumerate(pieces):
        cols = pl.ds(q * part + start, end - start)
        load(n, train_query.at[:, cols], tq.at[:, cols])
        if n == 0:
            greet()
            load("nt", norm_train, nt)
            load("ns", norm_step, ns)
        if n == 1:
            load("tk", train_key, tk)
            load("lk", low_key, lk)
            load("hk", high_key, hk)
        if n == 2:
            load("tv", train_value, tv)
            load("lv", low_value, lv)
            load("hv", high_value, hv)

    def merged(train, high, low):
        return train.astype(jnp.float32) + lax.dot_general(
            high, low, (((0,), (0,)), ((), ())), preferred_element_type=jnp.float32
        )

    def unit_copy(link, slot, what, rows=slice(None)):
        off, q = what
        unit = whole.at[me.at(off), q, rows]
        sem = cut_sem if slot == FINAL else send_sem
        return remote(unit, unit, sem, recv_sem.at[GROUP_OF[slot]], me.neighbour(LINKS[link]))

    def send(link, slot, rows=slice(None)):
        unit_copy(link, slot, SENDS[link][slot], rows).start()

    def units(slots, sem):
        some = whole.at[pl.ds(0, slots * len(LINKS) // QUARTERS)]
        return remote(some, some, send_sem, sem, me.partner())

    def arrive(group):
        units(len(GROUPS[group]), recv_sem.at[group]).wait_recv()

    def only(core):
        return pl.when(me.core == LATE if core == LATE else me.core != LATE)

    def fresh_copy():
        return remote(fresh, ring.at[me.y * SIDE + me.z], fresh_sem.at[0], fresh_sem.at[1], (me.y, me.col))

    def column_copy():
        part_of_ring = ring.at[pl.ds(me.y * SIDE, SIDE)]
        return remote(part_of_ring, part_of_ring, column_sem.at[0], column_sem.at[1], (LEAD, me.col))

    def ring_lines(count, sem):
        some = ring.at[pl.ds(0, count)]
        return remote(some, some, sem.at[0], sem.at[1], me.partner())

    def norm_copy(off):
        return remote(norm, norm, norm_sem.at[0], norm_sem.at[1], me.neighbour(off))

    def norm_sent(count):
        some = whole.at[0, 0, pl.ds(0, count * norm.shape[0] * norm.shape[1] // whole.shape[3])]
        remote(some, some, norm_sem.at[0], norm_sem.at[1], me.partner()).wait_send()

    def make_fresh():
        loads["nt"].wait()
        loads["ns"].wait()
        values = nt[...] + ns[...]
        fresh[...] = jnp.concatenate([values, values], axis=1)

    def send_fresh():
        @pl.when(top)
        def _():
            ring[me.y * SIDE + me.z] = fresh[...]

        @pl.when(jnp.logical_not(top))
        def _():
            fresh_copy().start()

    loads["lq"].wait()
    loads["hq"].wait()
    for n, (q, start, end) in enumerate(pieces):
        cols = pl.ds(q * part + start, end - start)
        loads[n].wait()
        if n == 1:
            make_fresh()
        whole[me.row, q, start:end, :] = merged(tq[:, cols].T, hq[:, cols], lq[...]).astype(whole.dtype)
        if n == 0:

            @pl.when(leader)
            def _():
                pl.semaphore_wait(barrier, len(peers) + n_planes - 1)

            far = (me.z == 2) | (top & (me.y == (LEAD + 2) % SIDE))

            @pl.when(far)
            def _():
                pl.semaphore_wait(barrier, len(peers) + 1)

            @pl.when(jnp.logical_not(leader | far))
            def _():
                pl.semaphore_wait(barrier, len(peers))

        if end == part:
            if n == 1:
                for name in ("tk", "lk", "hk"):
                    loads[name].wait()
            if n == 2:
                for name in ("tv", "lv", "hv"):
                    loads[name].wait()
            train, low, high = (tk, lk, hk) if q < 2 else (tv, lv, hv)
            small = merged(train[...], high[...], low[...]).astype(whole.dtype)
            half = small.shape[0] // 2
            whole[me.row, q, part:, :] = small[(q % 2) * half : (q % 2 + 1) * half, :]
        for link in range(len(LINKS)):
            if n == 0:
                send(link, 0, pl.ds(0, end))
            elif n == 1:
                send(link, 0, pl.ds(start, whole.shape[2] - start))
            else:
                send(link, ORDER.index(q))
        if n == 1:
            send_fresh()

    def norm_on_its_way(group):
        if group == 0:

            @pl.when(top)
            def _():
                ring_lines(len(column), fresh_sem).wait_recv()

            @pl.when(head)
            def _():
                column_copy().start()

        if group == 1:

            @pl.when(leader)
            def _():
                ring_lines(len(heads) * SIDE, column_sem).wait_recv()
                in_order = [ring[(i % SIDE) * SIDE + i // SIDE] for i in range(blocks)]
                lines[me.col] = jnp.concatenate(in_order, axis=0)
                for n in range(1, n_planes):
                    remote(lines.at[me.col], lines.at[me.col], line_sem.at[0], line_sem.at[1], me.plane(n)).start()
                some = lines.at[pl.ds(0, n_planes - 1)]
                remote(some, some, line_sem.at[0], line_sem.at[1], me.partner()).wait()
                lane = lax.broadcasted_iota(jnp.int32, lines.shape[1:], 1)
                for x in range(SIDE):
                    both = jnp.where(lane < lines.shape[2] // CORES, lines[CORES * x], lines[CORES * x + 1])
                    ordered[pl.Slice(x, blocks, SIDE), :] = both
                norm[...] = ordered[...].astype(norm.dtype)
                for off in heads + column:
                    norm_copy(off).start()

        if group == 2:

            @pl.when(head)
            def _():
                norm_copy((1, 0)).wait_recv()
                for off in column:
                    norm_copy(off).start()

    def send_slots(slots):
        for slot in slots:
            for link in range(len(LINKS)):
                send(link, slot, pl.ds(0, CUT) if slot == FINAL else slice(None))

    for group, slots in enumerate(AFTER):
        arrive(group)
        norm_on_its_way(group)
        if slots[0] < SPLIT:
            send_slots(slots)
        else:

            @only(1 - LATE)
            def _():
                send_slots(slots)

    arrive(5)

    @only(1 - LATE)
    def _():
        arrive(6)
        cut = whole.at[pl.ds(0, len(LINKS)), 0, pl.ds(0, CUT)]
        remote(cut, cut, cut_sem, recv_sem.at[7], me.partner()).wait()
        units(FINAL, recv_sem.at[0]).wait_send()

    @only(LATE)
    def _():
        units(SPLIT, recv_sem.at[0]).wait_send()

    @pl.when(leader)
    def _():
        norm_sent(len(heads) + len(column))

    @pl.when(head)
    def _():
        column_copy().wait_send()
        norm_sent(len(column))

    @pl.when(jnp.logical_not(top))
    def _():
        fresh_copy().wait_send()
        norm_copy((1, 0)).wait_recv()


def finish_kernel(whole, token, rest, send_sem, recv_sem):
    del token
    me = Place()
    barrier = pltpu.get_barrier_semaphore()
    signal_all(barrier, [me.neighbour(d) for d in LINKS])
    pl.semaphore_wait(barrier, len(LINKS))

    def send(link, slot, rows):
        off, q = SENDS[link][slot]
        source, target = whole.at[me.at(off), q, rows], rest.at[link, slot - SPLIT, rows]
        remote(source, target, send_sem, recv_sem, me.neighbour(LINKS[link])).start()

    @pl.when(me.core == LATE)
    def _():
        for link, slot in LAST:
            send(link, slot, slice(None))
        remote(rest, rest, send_sem, recv_sem, me.partner()).wait()

    @pl.when(me.core != LATE)
    def _():
        left = whole.shape[2] - CUT
        for link in range(len(LINKS)):
            send(link, FINAL, pl.ds(CUT, left))
        cut = rest.at[pl.ds(0, len(LINKS)), 0, pl.ds(0, left)]
        remote(cut, cut, send_sem, recv_sem, me.partner()).wait()


def write_rows(source, block, quarter, outs, sems, start, end):
    out_query, out_key, out_value = outs
    rows, depth = source.shape
    part = out_query.shape[0] // QUARTERS
    half = rows - part
    at = pl.ds(pl.multiple_of(block * depth, depth), depth)
    if end <= part:
        target, sem = out_query.at[pl.ds(quarter * part + start, end - start), at], sems[0]
    else:
        assert (start, end) == (part, rows)
        target, sem = (out_key if quarter < 2 else out_value).at[pl.ds((quarter % 2) * half, half), at], sems[1]
    pltpu.make_async_copy(source.at[pl.ds(start, end - start)], target, sem).start()


def write_unit(source, block, quarter, outs, sems):
    part = outs[0].shape[0] // QUARTERS
    write_rows(source, block, quarter, outs, sems, 0, part)
    write_rows(source, block, quarter, outs, sems, part, source.shape[0])


def wait_rows(count, whole, out, sem):
    same = out.at[pl.ds(0, count * whole.shape[-1] // out.shape[1])]
    pltpu.make_async_copy(same, same, sem).wait()


def write_kernel(whole, out_query, out_key, out_value, token, sem):
    me = Place()
    outs = (out_query, out_key, out_value)
    blocks, _, rows, _ = whole.shape
    part = out_query.shape[0] // QUARTERS
    token[...] = jnp.zeros_like(token)
    late = {arriving(*unit) for unit in LAST}
    first, second = sem.at[0], sem.at[1]

    @pl.when(me.core == LATE)
    def _():
        count = 0
        for off in [(dz, dy) for dz in range(SIDE) for dy in range(SIDE)]:
            for q in range(QUARTERS):
                if (off, q) not in late:
                    count += 1
                    block = me.at(off)
                    write_unit(whole.at[block, q], block, q, outs, (first, first))
        wait_rows(count * rows, whole, out_query, first)

    @pl.when(me.core != LATE)
    def _():
        final = me.at((2, 2))

        @pl.loop(1, blocks)
        def _(n):
            block = (final + n) % blocks
            for q in range(QUARTERS):
                write_unit(whole.at[block, q], block, q, outs, (first, second))

        for q in range(QUARTERS):
            write_rows(whole.at[final, q], final, q, outs, (first, second), 0, CUT)
        wait_rows(QUARTERS * ((blocks - 1) * part + CUT), whole, out_query, first)
        wait_rows(QUARTERS * (blocks - 1) * (rows - part), whole, out_query, second)


def write_rest_kernel(
    whole, rest, norm, in_query, in_key, in_value, out_query, out_key, out_value, out_norm, sem, norm_sem
):
    del in_query, in_key, in_value
    me = Place()
    outs = (out_query, out_key, out_value)
    rows = whole.shape[2]
    part = out_query.shape[0] // QUARTERS
    norm_copy = pltpu.make_async_copy(norm, out_norm, norm_sem)
    norm_copy.start()

    @pl.when(me.core == LATE)
    def _():
        for link, slot in LAST:
            off, q = arriving(link, slot)
            write_unit(rest.at[link, slot - SPLIT], me.at(off), q, outs, (sem, sem))
        wait_rows(len(LAST) * rows, whole, out_query, sem)

    @pl.when(me.core != LATE)
    def _():
        for link in range(len(LINKS)):
            off, q = arriving(link, FINAL)
            source = rest.at[link, FINAL - SPLIT]
            write_rows(source, me.at(off), q, outs, (sem, sem), CUT, part)
            write_rows(source, me.at(off), q, outs, (sem, sem), part, rows)
        wait_rows(len(LINKS) * (rows - CUT), whole, out_query, sem)

    norm_copy.wait()


def body(
    train_query, low_query, high_query,
    train_key, low_key, high_key,
    train_value, low_value, high_value,
    norm_train, norm_step,
):
    n_rows, n_cols = lax.axis_size("rows"), lax.axis_size("cols")
    depth, wide = train_query.shape
    tall = train_key.shape[1]
    rank = low_query.shape[1]
    unit = (wide + 2 * tall) // QUARTERS
    values = norm_train.shape[0]
    line = CORES * values
    dtype = train_query.dtype
    f32 = jnp.float32
    anywhere = pl.BlockSpec(memory_space=pl.ANY)
    vmem = pl.BlockSpec(memory_space=pltpu.VMEM)
    dma = pltpu.SemaphoreType.DMA
    shape = jax.ShapeDtypeStruct

    def pin(space, *arrays):
        return [pltpu.with_memory_space_constraint(a, space) for a in arrays]

    whole, norm = pl.pallas_call(
        gather_kernel,
        out_shape=(
            shape((n_rows, QUARTERS, unit, depth), dtype),
            shape((n_rows * n_cols // CORES, line), dtype),
        ),
        in_specs=[anywhere] * 11,
        out_specs=(vmem, vmem),
        scratch_shapes=[
            pltpu.VMEM((depth, wide), dtype),
            pltpu.VMEM((rank, depth), dtype),
            pltpu.VMEM((rank, wide), dtype),
            pltpu.VMEM((tall, depth), dtype),
            pltpu.VMEM((rank, depth), dtype),
            pltpu.VMEM((rank, tall), dtype),
            pltpu.VMEM((tall, depth), dtype),
            pltpu.VMEM((rank, depth), dtype),
            pltpu.VMEM((rank, tall), dtype),
            pltpu.VMEM((1, values), f32),
            pltpu.VMEM((1, values), f32),
            pltpu.VMEM((1, line), f32),
            pltpu.VMEM((n_rows, 1, line), f32),
            pltpu.VMEM((n_cols, n_rows, line), f32),
            pltpu.VMEM((SIDE * n_rows, line), f32),
            dma((15,)),
            dma(()),
            dma(()),
            dma((len(GROUPS),)),
            dma((2,)),
            dma((2,)),
            dma((2,)),
            dma((2,)),
        ],
        compiler_params=pltpu.CompilerParams(
            collective_id=0, has_side_effects=True, vmem_limit_bytes=24 * 2**20
        ),
        name="gather",
    )(
        *pin(
            pltpu.HBM,
            train_query, low_query.T, high_query,
            train_key.T, low_key.T, high_key,
            train_value.T, low_value.T, high_value,
            norm_train.reshape(1, -1), norm_step.reshape(1, -1),
        )
    )
    outs = [shape((wide, n_rows * depth), dtype)] + [shape((tall, n_rows * depth), dtype)] * 2
    out_query, out_key, out_value, token = pl.pallas_call(
        write_kernel,
        out_shape=(*outs, shape((8, 128), f32)),
        in_specs=[vmem],
        out_specs=[anywhere] * 3 + [vmem],
        scratch_shapes=[dma((2,))],
        compiler_params=pltpu.CompilerParams(vmem_limit_bytes=4 * 2**20),
        name="write",
    )(*pin(pltpu.VMEM, whole))
    (rest,) = pl.pallas_call(
        finish_kernel,
        out_shape=(shape((len(LINKS), SLOTS - SPLIT, unit, depth), dtype),),
        in_specs=[vmem] * 2,
        out_specs=(vmem,),
        scratch_shapes=[dma(()), dma(())],
        compiler_params=pltpu.CompilerParams(
            collective_id=1, has_side_effects=True, vmem_limit_bytes=8 * 2**20
        ),
        name="finish",
    )(*pin(pltpu.VMEM, whole, token))
    out_query, out_key, out_value, out_norm = pl.pallas_call(
        write_rest_kernel,
        out_shape=(*outs, shape(norm.shape, dtype)),
        in_specs=[vmem] * 3 + [anywhere] * 3,
        out_specs=[anywhere] * 4,
        input_output_aliases={3: 0, 4: 1, 5: 2},
        scratch_shapes=[dma(()), dma(())],
        compiler_params=pltpu.CompilerParams(vmem_limit_bytes=4 * 2**20),
        name="write_rest",
    )(*pin(pltpu.VMEM, whole, rest, norm), *pin(pltpu.HBM, out_query, out_key, out_value))
    return out_query, out_key, out_value, out_norm.reshape(-1)


def solution(mesh):
    return jax.shard_map(
        body,
        mesh=mesh,
        in_specs=(
            P("rows", "cols"),
            P("rows", None),
            P(None, "cols"),
            P("rows", "cols"),
            P("rows", None),
            P(None, "cols"),
            P("rows", "cols"),
            P("rows", None),
            P(None, "cols"),
            P(("rows", "cols")),
            P(("rows", "cols")),
        ),
        out_specs=(P("cols", None), P("cols", None), P("cols", None), P()),
        check_vma=False,
    )
```

```python
import jax
import jax.numpy as jnp
from jax import lax
from jax.experimental import pallas as pl
from jax.experimental.pallas import tpu as pltpu
from jax.sharding import PartitionSpec as P

MESH = pl.DeviceIdType.MESH

SIDE = 4
QUARTERS = 4
CORES = 2
LINKS = ((0, 1), (0, -1), (1, 0), (-1, 0))
LATE = 1
SPLIT = 13
HEAD_START = 2900
LEAD = 2
ORDER = (0, 2, 1, 3)


def shift(off, d, sign=1):
    return ((off[0] + sign * d[0]) % SIDE, (off[1] + sign * d[1]) % SIDE)


def sends_of(link):
    d = LINKS[link]
    along_y = d[0] == 0
    first = (0, 1) if along_y else (2, 3)
    second = (2, 3) if along_y else (0, 1)
    positive = sum(d) > 0
    fwd_first = first[0] if positive else first[1]
    fwd_second = second[0] if positive else second[1]

    def across(n):
        return (n % SIDE, 0) if along_y else (0, n % SIDE)

    def behind(off):
        return shift(off, d, -1)

    own = (0, 0)
    return tuple((own, q) for q in ORDER) + (
        (across(-1), second[0]),
        (across(1), second[0]),
        (behind(own), fwd_first),
        (across(-1), second[1]),
        (across(1), second[1]),
        (behind(own), fwd_second),
        (across(2), second[0]),
        (across(2), second[1]),
        (behind(across(-1)), fwd_second),
        (behind(across(1)), fwd_second),
        (behind(across(2)), fwd_second),
    )


SENDS = tuple(sends_of(link) for link in range(len(LINKS)))
SLOTS = len(SENDS[0])
UNITS = [(link, slot) for slot in range(SLOTS) for link in range(len(LINKS))]


def arriving(link, slot):
    off, quarter = SENDS[link][slot]
    return shift(off, LINKS[link], -1), quarter


ARRIVES = {arriving(*unit): unit for unit in UNITS}
assert len(ARRIVES) == len(UNITS) == (SIDE * SIDE - 1) * QUARTERS
LAST = [unit for unit in UNITS if unit[1] >= SPLIT]
GROUPS = ((0, 1), (2, 3), (6,), (4, 5, 7, 8), (10, 11), (9, 12), (13, 14))
GROUP_OF = {slot: group for group, slots in enumerate(GROUPS) for slot in slots}
assert sorted(GROUP_OF) == list(range(SLOTS)) and GROUPS[-1] == tuple(range(SPLIT, SLOTS))
AFTER = ((4, 5), (6, 7, 8, 9), (10, 11), (12,), (13,), (14,))
NEEDS = (0, 1, 2, 3, 3, 4)
for _group, _slots in zip(NEEDS, AFTER, strict=True):
    for _slot in _slots:
        for _link in range(len(LINKS)):
            assert GROUP_OF[ARRIVES[SENDS[_link][_slot]][1]] <= _group


class Place:
    def __init__(self):
        self.row, self.col = lax.axis_index("rows"), lax.axis_index("cols")
        self.z, self.y = self.row // SIDE, self.row % SIDE
        self.x, self.core = self.col // CORES, self.col % CORES

    def at(self, off):
        return ((self.z + off[0]) % SIDE) * SIDE + (self.y + off[1]) % SIDE

    def neighbour(self, d):
        return (self.at(d), self.col)

    def partner(self):
        return (self.row, self.x * CORES + 1 - self.core)

    def plane(self, n):
        return (self.row, (self.col + n) % (SIDE * CORES))


def remote(src, dst, send_sem, recv_sem, device):
    return pltpu.make_async_remote_copy(
        src_ref=src, dst_ref=dst, send_sem=send_sem, recv_sem=recv_sem, device_id=device, device_id_type=MESH
    )


def signal_all(barrier, devices):
    for device in devices:
        pl.semaphore_signal(barrier, inc=1, device_id=device, device_id_type=MESH)


def gather_kernel(
    train_query, low_query, high_query,
    train_key, low_key, high_key,
    train_value, low_value, high_value,
    norm_train, norm_step,
    whole, norm,
    tq, lq, hq, tk, lk, hk, tv, lv, hv, nt, ns, fresh, ring, lines, ordered,
    load_sem, send_sem, recv_sem, fresh_sem, column_sem, line_sem, norm_sem,
):
    me = Place()
    wide = tq.shape[1]
    part = wide // QUARTERS
    blocks = whole.shape[0]
    top = me.z == 0
    leader = top & (me.y == LEAD)
    head = top & (me.y != LEAD)
    n_planes = lines.shape[0]
    column = [(dz, 0) for dz in range(1, SIDE)]
    heads = [(0, dy) for dy in range(1, SIDE)]

    barrier = pltpu.get_barrier_semaphore()
    peers = [me.neighbour(d) for d in LINKS] + [me.partner()]

    def greet():
        signal_all(barrier, peers)

        @pl.when(top)
        def _():
            signal_all(barrier, [me.neighbour((2, 0))])

        @pl.when(leader)
        def _():
            signal_all(barrier, [me.neighbour((0, 2))] + [me.plane(n) for n in range(1, n_planes)])

    loads = {}

    def load(name, src, dst):
        copy = pltpu.make_async_copy(src, dst, load_sem.at[len(loads)])
        copy.start()
        loads[name] = copy

    pieces = [(ORDER[0], 0, part // 2), (ORDER[0], part // 2, part)] + [(q, 0, part) for q in ORDER[1:]]
    load("lq", low_query, lq)
    load("hq", high_query, hq)
    for n, (q, start, end) in enumerate(pieces):
        cols = pl.ds(q * part + start, end - start)
        load(n, train_query.at[:, cols], tq.at[:, cols])
        if n == 0:
            greet()
            load("nt", norm_train, nt)
            load("ns", norm_step, ns)
        if n == 1:
            load("tk", train_key, tk)
            load("lk", low_key, lk)
            load("hk", high_key, hk)
        if n == 2:
            load("tv", train_value, tv)
            load("lv", low_value, lv)
            load("hv", high_value, hv)

    def merged(train, high, low):
        return train.astype(jnp.float32) + lax.dot_general(
            high, low, (((0,), (0,)), ((), ())), preferred_element_type=jnp.float32
        )

    def unit_copy(link, slot, what, rows=slice(None)):
        off, q = what
        unit = whole.at[me.at(off), q, rows]
        return remote(unit, unit, send_sem, recv_sem.at[GROUP_OF[slot]], me.neighbour(LINKS[link]))

    def send(link, slot, rows=slice(None)):
        unit_copy(link, slot, SENDS[link][slot], rows).start()

    def units(slots, sem):
        some = whole.at[pl.ds(0, slots * len(LINKS) // QUARTERS)]
        return remote(some, some, send_sem, sem, me.partner())

    def arrive(group):
        units(len(GROUPS[group]), recv_sem.at[group]).wait_recv()

    def only(core):
        return pl.when(me.core == LATE if core == LATE else me.core != LATE)

    def fresh_copy():
        return remote(fresh, ring.at[me.y * SIDE + me.z], fresh_sem.at[0], fresh_sem.at[1], (me.y, me.col))

    def column_copy():
        part_of_ring = ring.at[pl.ds(me.y * SIDE, SIDE)]
        return remote(part_of_ring, part_of_ring, column_sem.at[0], column_sem.at[1], (LEAD, me.col))

    def ring_lines(count, sem):
        some = ring.at[pl.ds(0, count)]
        return remote(some, some, sem.at[0], sem.at[1], me.partner())

    def norm_copy(off):
        return remote(norm, norm, norm_sem.at[0], norm_sem.at[1], me.neighbour(off))

    def norm_sent(count):
        some = whole.at[0, 0, pl.ds(0, count * norm.shape[0] * norm.shape[1] // whole.shape[3])]
        remote(some, some, norm_sem.at[0], norm_sem.at[1], me.partner()).wait_send()

    def make_fresh():
        loads["nt"].wait()
        loads["ns"].wait()
        values = nt[...] + ns[...]
        fresh[...] = jnp.concatenate([values, values], axis=1)

    def send_fresh():
        @pl.when(top)
        def _():
            ring[me.y * SIDE + me.z] = fresh[...]

        @pl.when(jnp.logical_not(top))
        def _():
            fresh_copy().start()

    loads["lq"].wait()
    loads["hq"].wait()
    for n, (q, start, end) in enumerate(pieces):
        cols = pl.ds(q * part + start, end - start)
        loads[n].wait()
        if n == 1:
            make_fresh()
        whole[me.row, q, start:end, :] = merged(tq[:, cols].T, hq[:, cols], lq[...]).astype(whole.dtype)
        if n == 0:

            @pl.when(leader)
            def _():
                pl.semaphore_wait(barrier, len(peers) + n_planes - 1)

            far = (me.z == 2) | (top & (me.y == (LEAD + 2) % SIDE))

            @pl.when(far)
            def _():
                pl.semaphore_wait(barrier, len(peers) + 1)

            @pl.when(jnp.logical_not(leader | far))
            def _():
                pl.semaphore_wait(barrier, len(peers))

            @only(1 - LATE)
            def _():
                pl.delay(HEAD_START)

        if end == part:
            if n == 1:
                for name in ("tk", "lk", "hk"):
                    loads[name].wait()
            if n == 2:
                for name in ("tv", "lv", "hv"):
                    loads[name].wait()
            train, low, high = (tk, lk, hk) if q < 2 else (tv, lv, hv)
            small = merged(train[...], high[...], low[...]).astype(whole.dtype)
            half = small.shape[0] // 2
            whole[me.row, q, part:, :] = small[(q % 2) * half : (q % 2 + 1) * half, :]
        for link in range(len(LINKS)):
            if n == 0:
                send(link, 0, pl.ds(0, end))
            elif n == 1:
                send(link, 0, pl.ds(start, whole.shape[2] - start))
            else:
                send(link, ORDER.index(q))
        if n == 1:
            send_fresh()

    def norm_on_its_way(group):
        if group == 0:

            @pl.when(top)
            def _():
                ring_lines(len(column), fresh_sem).wait_recv()

            @pl.when(head)
            def _():
                column_copy().start()

        if group == 1:

            @pl.when(leader)
            def _():
                ring_lines(len(heads) * SIDE, column_sem).wait_recv()
                in_order = [ring[(i % SIDE) * SIDE + i // SIDE] for i in range(blocks)]
                lines[me.col] = jnp.concatenate(in_order, axis=0)
                for n in range(1, n_planes):
                    remote(lines.at[me.col], lines.at[me.col], line_sem.at[0], line_sem.at[1], me.plane(n)).start()
                some = lines.at[pl.ds(0, n_planes - 1)]
                remote(some, some, line_sem.at[0], line_sem.at[1], me.partner()).wait()
                lane = lax.broadcasted_iota(jnp.int32, lines.shape[1:], 1)
                for x in range(SIDE):
                    both = jnp.where(lane < lines.shape[2] // CORES, lines[CORES * x], lines[CORES * x + 1])
                    ordered[pl.Slice(x, blocks, SIDE), :] = both
                norm[...] = ordered[...].astype(norm.dtype)
                for off in heads + column:
                    norm_copy(off).start()

        if group == 2:

            @pl.when(head)
            def _():
                norm_copy((1, 0)).wait_recv()
                for off in column:
                    norm_copy(off).start()

    def send_slots(slots):
        for slot in slots:
            for link in range(len(LINKS)):
                send(link, slot)

    waited = -1
    for group, slots in zip(NEEDS, AFTER, strict=True):
        if group != waited:
            waited = group
            arrive(group)
            norm_on_its_way(group)
        if slots[0] < SPLIT:
            send_slots(slots)
        else:

            @only(1 - LATE)
            def _():
                send_slots(slots)

    arrive(5)

    @only(1 - LATE)
    def _():
        arrive(6)
        units(SLOTS, recv_sem.at[0]).wait_send()

    @only(LATE)
    def _():
        units(SPLIT, recv_sem.at[0]).wait_send()

    @pl.when(leader)
    def _():
        norm_sent(len(heads) + len(column))

    @pl.when(head)
    def _():
        column_copy().wait_send()
        norm_sent(len(column))

    @pl.when(jnp.logical_not(top))
    def _():
        fresh_copy().wait_send()
        norm_copy((1, 0)).wait_recv()


def finish_kernel(whole, token, rest, send_sem, recv_sem):
    del token
    me = Place()

    @pl.when(me.core == LATE)
    def _():
        barrier = pltpu.get_barrier_semaphore()
        signal_all(barrier, [me.neighbour(d) for d in LINKS])
        pl.semaphore_wait(barrier, len(LINKS))
        for link, slot in LAST:
            off, q = SENDS[link][slot]
            unit = whole.at[me.at(off), q]
            remote(unit, rest.at[link, slot - SPLIT], send_sem, recv_sem, me.neighbour(LINKS[link])).start()
        remote(rest, rest, send_sem, recv_sem, me.partner()).wait()


def write_unit(source, block, quarter, outs, sems):
    out_query, out_key, out_value = outs
    rows, depth = source.shape
    part = out_query.shape[0] // QUARTERS
    half = rows - part
    at = pl.ds(pl.multiple_of(block * depth, depth), depth)
    small = (out_key if quarter < 2 else out_value).at[pl.ds((quarter % 2) * half, half), at]
    pltpu.make_async_copy(source.at[pl.ds(0, part)], out_query.at[pl.ds(quarter * part, part), at], sems[0]).start()
    pltpu.make_async_copy(source.at[pl.ds(part, half)], small, sems[1 + quarter // 2]).start()


def wait_units(count, unit_bytes, out, sem):
    rows = count * unit_bytes // (out.shape[1] * out.dtype.itemsize)
    same = out.at[pl.ds(0, rows)]
    pltpu.make_async_copy(same, same, sem).wait()


def unit_bytes_of(whole):
    return whole.shape[-2] * whole.shape[-1] * whole.dtype.itemsize


def write_kernel(whole, out_query, out_key, out_value, token, sem):
    me = Place()
    outs = (out_query, out_key, out_value)
    token[...] = jnp.zeros_like(token)
    late = {arriving(*unit) for unit in LAST}

    @pl.when(me.core == LATE)
    def _():
        count = 0
        for off in [(dz, dy) for dz in range(SIDE) for dy in range(SIDE)]:
            for q in range(QUARTERS):
                if (off, q) not in late:
                    count += 1
                    block = me.at(off)
                    write_unit(whole.at[block, q], block, q, outs, (sem, sem, sem))
        wait_units(count, unit_bytes_of(whole), out_query, sem)


def write_rest_kernel(
    whole, rest, norm, in_query, in_key, in_value, out_query, out_key, out_value, out_norm, sem, norm_sem
):
    del in_query, in_key, in_value
    me = Place()
    outs = (out_query, out_key, out_value)
    norm_copy = pltpu.make_async_copy(norm, out_norm, norm_sem)
    norm_copy.start()

    @pl.when(me.core == LATE)
    def _():
        first = sem.at[0]
        for link, slot in LAST:
            off, q = arriving(link, slot)
            write_unit(rest.at[link, slot - SPLIT], me.at(off), q, outs, (first, first, first))
        wait_units(len(LAST), unit_bytes_of(whole), out_query, first)

    @pl.when(me.core != LATE)
    def _():
        @pl.loop(0, whole.shape[0])
        def _(block):
            for q in range(QUARTERS):
                write_unit(whole.at[block, q], block, q, outs, [sem.at[n] for n in range(len(outs))])

        for n, out in enumerate(outs):
            pltpu.make_async_copy(out, out, sem.at[n]).wait()

    norm_copy.wait()


def body(
    train_query, low_query, high_query,
    train_key, low_key, high_key,
    train_value, low_value, high_value,
    norm_train, norm_step,
):
    n_rows, n_cols = lax.axis_size("rows"), lax.axis_size("cols")
    depth, wide = train_query.shape
    tall = train_key.shape[1]
    rank = low_query.shape[1]
    unit = (wide + 2 * tall) // QUARTERS
    values = norm_train.shape[0]
    line = CORES * values
    dtype = train_query.dtype
    f32 = jnp.float32
    anywhere = pl.BlockSpec(memory_space=pl.ANY)
    vmem = pl.BlockSpec(memory_space=pltpu.VMEM)
    dma = pltpu.SemaphoreType.DMA
    shape = jax.ShapeDtypeStruct

    def pin(space, *arrays):
        return [pltpu.with_memory_space_constraint(a, space) for a in arrays]

    whole, norm = pl.pallas_call(
        gather_kernel,
        out_shape=(
            shape((n_rows, QUARTERS, unit, depth), dtype),
            shape((n_rows * n_cols // CORES, line), dtype),
        ),
        in_specs=[anywhere] * 11,
        out_specs=(vmem, vmem),
        scratch_shapes=[
            pltpu.VMEM((depth, wide), dtype),
            pltpu.VMEM((rank, depth), dtype),
            pltpu.VMEM((rank, wide), dtype),
            pltpu.VMEM((tall, depth), dtype),
            pltpu.VMEM((rank, depth), dtype),
            pltpu.VMEM((rank, tall), dtype),
            pltpu.VMEM((tall, depth), dtype),
            pltpu.VMEM((rank, depth), dtype),
            pltpu.VMEM((rank, tall), dtype),
            pltpu.VMEM((1, values), f32),
            pltpu.VMEM((1, values), f32),
            pltpu.VMEM((1, line), f32),
            pltpu.VMEM((n_rows, 1, line), f32),
            pltpu.VMEM((n_cols, n_rows, line), f32),
            pltpu.VMEM((SIDE * n_rows, line), f32),
            dma((15,)),
            dma(()),
            dma((len(GROUPS),)),
            dma((2,)),
            dma((2,)),
            dma((2,)),
            dma((2,)),
        ],
        compiler_params=pltpu.CompilerParams(
            collective_id=0, has_side_effects=True, vmem_limit_bytes=24 * 2**20
        ),
        name="gather",
    )(
        *pin(
            pltpu.HBM,
            train_query, low_query.T, high_query,
            train_key.T, low_key.T, high_key,
            train_value.T, low_value.T, high_value,
            norm_train.reshape(1, -1), norm_step.reshape(1, -1),
        )
    )
    outs = [shape((wide, n_rows * depth), dtype)] + [shape((tall, n_rows * depth), dtype)] * 2
    out_query, out_key, out_value, token = pl.pallas_call(
        write_kernel,
        out_shape=(*outs, shape((8, 128), f32)),
        in_specs=[vmem],
        out_specs=[anywhere] * 3 + [vmem],
        scratch_shapes=[dma(())],
        compiler_params=pltpu.CompilerParams(vmem_limit_bytes=4 * 2**20),
        name="write",
    )(*pin(pltpu.VMEM, whole))
    (rest,) = pl.pallas_call(
        finish_kernel,
        out_shape=(shape((len(LINKS), SLOTS - SPLIT, unit, depth), dtype),),
        in_specs=[vmem] * 2,
        out_specs=(vmem,),
        scratch_shapes=[dma(()), dma(())],
        compiler_params=pltpu.CompilerParams(
            collective_id=1, has_side_effects=True, vmem_limit_bytes=8 * 2**20
        ),
        name="finish",
    )(*pin(pltpu.VMEM, whole, token))
    out_query, out_key, out_value, out_norm = pl.pallas_call(
        write_rest_kernel,
        out_shape=(*outs, shape(norm.shape, dtype)),
        in_specs=[vmem] * 3 + [anywhere] * 3,
        out_specs=[anywhere] * 4,
        input_output_aliases={3: 0, 4: 1, 5: 2},
        scratch_shapes=[dma((len(outs),)), dma(())],
        compiler_params=pltpu.CompilerParams(vmem_limit_bytes=4 * 2**20),
        name="write_rest",
    )(*pin(pltpu.VMEM, whole, rest, norm), *pin(pltpu.HBM, out_query, out_key, out_value))
    return out_query, out_key, out_value, out_norm.reshape(-1)


def solution(mesh):
    return jax.shard_map(
        body,
        mesh=mesh,
        in_specs=(
            P("rows", "cols"),
            P("rows", None),
            P(None, "cols"),
            P("rows", "cols"),
            P("rows", None),
            P(None, "cols"),
            P("rows", "cols"),
            P("rows", None),
            P(None, "cols"),
            P(("rows", "cols")),
            P(("rows", "cols")),
        ),
        out_specs=(P("cols", None), P("cols", None), P("cols", None), P()),
        check_vma=False,
    )
```

```python
import jax
import jax.numpy as jnp
from jax import lax
from jax.experimental import pallas as pl
from jax.experimental.pallas import tpu as pltpu
from jax.sharding import PartitionSpec as P

MESH = pl.DeviceIdType.MESH

SIDE = 4
QUARTERS = 4
CORES = 2
LINKS = ((0, 1), (0, -1), (1, 0), (-1, 0))
LATE = 1
SPLIT = 13
HEAD_START = 3800
LEAD = 2
ORDER = (0, 2, 1, 3)


def shift(off, d, sign=1):
    return ((off[0] + sign * d[0]) % SIDE, (off[1] + sign * d[1]) % SIDE)


def sends_of(link):
    d = LINKS[link]
    along_y = d[0] == 0
    first = (0, 1) if along_y else (2, 3)
    second = (2, 3) if along_y else (0, 1)
    positive = sum(d) > 0
    fwd_first = first[0] if positive else first[1]
    fwd_second = second[0] if positive else second[1]

    def across(n):
        return (n % SIDE, 0) if along_y else (0, n % SIDE)

    def behind(off):
        return shift(off, d, -1)

    own = (0, 0)
    return tuple((own, q) for q in ORDER) + (
        (across(-1), second[0]),
        (across(1), second[0]),
        (behind(own), fwd_first),
        (across(-1), second[1]),
        (across(1), second[1]),
        (behind(own), fwd_second),
        (across(2), second[0]),
        (across(2), second[1]),
        (behind(across(-1)), fwd_second),
        (behind(across(1)), fwd_second),
        (behind(across(2)), fwd_second),
    )


SENDS = tuple(sends_of(link) for link in range(len(LINKS)))
SLOTS = len(SENDS[0])
UNITS = [(link, slot) for slot in range(SLOTS) for link in range(len(LINKS))]


def arriving(link, slot):
    off, quarter = SENDS[link][slot]
    return shift(off, LINKS[link], -1), quarter


ARRIVES = {arriving(*unit): unit for unit in UNITS}
assert len(ARRIVES) == len(UNITS) == (SIDE * SIDE - 1) * QUARTERS
LAST = [unit for unit in UNITS if unit[1] >= SPLIT]
GROUPS = ((0, 1), (2, 3), (6,), (4, 5, 7, 8), (10, 11), (9, 12), (13, 14))
GROUP_OF = {slot: group for group, slots in enumerate(GROUPS) for slot in slots}
assert sorted(GROUP_OF) == list(range(SLOTS)) and GROUPS[-1] == tuple(range(SPLIT, SLOTS))
AFTER = ((4, 5), (6, 7, 8, 9), (10, 11), (12,), (13,), (14,))
NEEDS = (0, 1, 2, 3, 3, 4)
for _group, _slots in zip(NEEDS, AFTER, strict=True):
    for _slot in _slots:
        for _link in range(len(LINKS)):
            assert GROUP_OF[ARRIVES[SENDS[_link][_slot]][1]] <= _group


class Place:
    def __init__(self):
        self.row, self.col = lax.axis_index("rows"), lax.axis_index("cols")
        self.z, self.y = self.row // SIDE, self.row % SIDE
        self.x, self.core = self.col // CORES, self.col % CORES

    def at(self, off):
        return ((self.z + off[0]) % SIDE) * SIDE + (self.y + off[1]) % SIDE

    def neighbour(self, d):
        return (self.at(d), self.col)

    def partner(self):
        return (self.row, self.x * CORES + 1 - self.core)

    def plane(self, n):
        return (self.row, (self.col + n) % (SIDE * CORES))


def remote(src, dst, send_sem, recv_sem, device):
    return pltpu.make_async_remote_copy(
        src_ref=src, dst_ref=dst, send_sem=send_sem, recv_sem=recv_sem, device_id=device, device_id_type=MESH
    )


def signal_all(barrier, devices):
    for device in devices:
        pl.semaphore_signal(barrier, inc=1, device_id=device, device_id_type=MESH)


def gather_kernel(
    train_query, low_query, high_query,
    train_key, low_key, high_key,
    train_value, low_value, high_value,
    norm_train, norm_step,
    whole, norm,
    tq, lq, hq, tk, lk, hk, tv, lv, hv, nt, ns, fresh, ring, lines, ordered,
    load_sem, send_sem, recv_sem, fresh_sem, column_sem, line_sem, norm_sem,
):
    me = Place()
    wide = tq.shape[1]
    part = wide // QUARTERS
    blocks = whole.shape[0]
    top = me.z == 0
    leader = top & (me.y == LEAD)
    head = top & (me.y != LEAD)
    n_planes = lines.shape[0]
    column = [(dz, 0) for dz in range(1, SIDE)]
    heads = [(0, dy) for dy in range(1, SIDE)]

    barrier = pltpu.get_barrier_semaphore()
    peers = [me.neighbour(d) for d in LINKS] + [me.partner()]

    def greet():
        signal_all(barrier, peers)

        @pl.when(top)
        def _():
            signal_all(barrier, [me.neighbour((2, 0))])

        @pl.when(leader)
        def _():
            signal_all(barrier, [me.neighbour((0, 2))] + [me.plane(n) for n in range(1, n_planes)])

    loads = {}

    def load(name, src, dst):
        copy = pltpu.make_async_copy(src, dst, load_sem.at[len(loads)])
        copy.start()
        loads[name] = copy

    pieces = [(ORDER[0], 0, part // 2), (ORDER[0], part // 2, part)] + [(q, 0, part) for q in ORDER[1:]]
    load("lq", low_query, lq)
    load("hq", high_query, hq)
    for n, (q, start, end) in enumerate(pieces):
        cols = pl.ds(q * part + start, end - start)
        load(n, train_query.at[:, cols], tq.at[:, cols])
        if n == 0:
            greet()
            load("nt", norm_train, nt)
            load("ns", norm_step, ns)
        if n == 1:
            load("tk", train_key, tk)
            load("lk", low_key, lk)
            load("hk", high_key, hk)
        if n == 2:
            load("tv", train_value, tv)
            load("lv", low_value, lv)
            load("hv", high_value, hv)

    def merged(train, high, low):
        return train.astype(jnp.float32) + lax.dot_general(
            high, low, (((0,), (0,)), ((), ())), preferred_element_type=jnp.float32
        )

    def unit_copy(link, slot, what, rows=slice(None)):
        off, q = what
        unit = whole.at[me.at(off), q, rows]
        return remote(unit, unit, send_sem, recv_sem.at[GROUP_OF[slot]], me.neighbour(LINKS[link]))

    def send(link, slot, rows=slice(None)):
        unit_copy(link, slot, SENDS[link][slot], rows).start()

    def units(slots, sem):
        some = whole.at[pl.ds(0, slots * len(LINKS) // QUARTERS)]
        return remote(some, some, send_sem, sem, me.partner())

    def arrive(group):
        units(len(GROUPS[group]), recv_sem.at[group]).wait_recv()

    def only(core):
        return pl.when(me.core == LATE if core == LATE else me.core != LATE)

    def fresh_copy():
        return remote(fresh, ring.at[me.y * SIDE + me.z], fresh_sem.at[0], fresh_sem.at[1], (me.y, me.col))

    def column_copy():
        part_of_ring = ring.at[pl.ds(me.y * SIDE, SIDE)]
        return remote(part_of_ring, part_of_ring, column_sem.at[0], column_sem.at[1], (LEAD, me.col))

    def ring_lines(count, sem):
        some = ring.at[pl.ds(0, count)]
        return remote(some, some, sem.at[0], sem.at[1], me.partner())

    def norm_copy(off):
        return remote(norm, norm, norm_sem.at[0], norm_sem.at[1], me.neighbour(off))

    def norm_sent(count):
        some = whole.at[0, 0, pl.ds(0, count * norm.shape[0] * norm.shape[1] // whole.shape[3])]
        remote(some, some, norm_sem.at[0], norm_sem.at[1], me.partner()).wait_send()

    def make_fresh():
        loads["nt"].wait()
        loads["ns"].wait()
        values = nt[...] + ns[...]
        fresh[...] = jnp.concatenate([values, values], axis=1)

    def send_fresh():
        @pl.when(top)
        def _():
            ring[me.y * SIDE + me.z] = fresh[...]

        @pl.when(jnp.logical_not(top))
        def _():
            fresh_copy().start()

    loads["lq"].wait()
    loads["hq"].wait()
    for n, (q, start, end) in enumerate(pieces):
        cols = pl.ds(q * part + start, end - start)
        loads[n].wait()
        if n == 1:
            make_fresh()
        whole[me.row, q, start:end, :] = merged(tq[:, cols].T, hq[:, cols], lq[...]).astype(whole.dtype)
        if n == 0:

            @pl.when(leader)
            def _():
                pl.semaphore_wait(barrier, len(peers) + n_planes - 1)

            far = (me.z == 2) | (top & (me.y == (LEAD + 2) % SIDE))

            @pl.when(far)
            def _():
                pl.semaphore_wait(barrier, len(peers) + 1)

            @pl.when(jnp.logical_not(leader | far))
            def _():
                pl.semaphore_wait(barrier, len(peers))

            @only(1 - LATE)
            def _():
                pl.delay(HEAD_START)

        if end == part:
            if n == 1:
                for name in ("tk", "lk", "hk"):
                    loads[name].wait()
            if n == 2:
                for name in ("tv", "lv", "hv"):
                    loads[name].wait()
            train, low, high = (tk, lk, hk) if q < 2 else (tv, lv, hv)
            small = merged(train[...], high[...], low[...]).astype(whole.dtype)
            half = small.shape[0] // 2
            whole[me.row, q, part:, :] = small[(q % 2) * half : (q % 2 + 1) * half, :]
        for link in range(len(LINKS)):
            if n == 0:
                send(link, 0, pl.ds(0, end))
            elif n == 1:
                send(link, 0, pl.ds(start, whole.shape[2] - start))
            else:
                send(link, ORDER.index(q))
        if n == 1:
            send_fresh()

    def norm_on_its_way(group):
        if group == 0:

            @pl.when(top)
            def _():
                ring_lines(len(column), fresh_sem).wait_recv()

            @pl.when(head)
            def _():
                column_copy().start()

        if group == 1:

            @pl.when(leader)
            def _():
                ring_lines(len(heads) * SIDE, column_sem).wait_recv()
                in_order = [ring[(i % SIDE) * SIDE + i // SIDE] for i in range(blocks)]
                lines[me.col] = jnp.concatenate(in_order, axis=0)
                for n in range(1, n_planes):
                    remote(lines.at[me.col], lines.at[me.col], line_sem.at[0], line_sem.at[1], me.plane(n)).start()
                some = lines.at[pl.ds(0, n_planes - 1)]
                remote(some, some, line_sem.at[0], line_sem.at[1], me.partner()).wait()
                lane = lax.broadcasted_iota(jnp.int32, lines.shape[1:], 1)
                for x in range(SIDE):
                    both = jnp.where(lane < lines.shape[2] // CORES, lines[CORES * x], lines[CORES * x + 1])
                    ordered[pl.Slice(x, blocks, SIDE), :] = both
                norm[...] = ordered[...].astype(norm.dtype)
                for off in heads + column:
                    norm_copy(off).start()

        if group == 2:

            @pl.when(head)
            def _():
                norm_copy((1, 0)).wait_recv()
                for off in column:
                    norm_copy(off).start()

    def send_slots(slots):
        for slot in slots:
            for link in range(len(LINKS)):
                send(link, slot)

    waited = -1
    for group, slots in zip(NEEDS, AFTER, strict=True):
        if group != waited:
            waited = group
            arrive(group)
            norm_on_its_way(group)
        if slots[0] < SPLIT:
            send_slots(slots)
        else:

            @only(1 - LATE)
            def _():
                send_slots(slots)

    arrive(5)

    @only(1 - LATE)
    def _():
        arrive(6)
        units(SLOTS, recv_sem.at[0]).wait_send()

    @only(LATE)
    def _():
        units(SPLIT, recv_sem.at[0]).wait_send()

    @pl.when(leader)
    def _():
        norm_sent(len(heads) + len(column))

    @pl.when(head)
    def _():
        column_copy().wait_send()
        norm_sent(len(column))

    @pl.when(jnp.logical_not(top))
    def _():
        fresh_copy().wait_send()
        norm_copy((1, 0)).wait_recv()


def finish_kernel(whole, token, rest, send_sem, recv_sem):
    del token
    me = Place()

    @pl.when(me.core == LATE)
    def _():
        barrier = pltpu.get_barrier_semaphore()
        signal_all(barrier, [me.neighbour(d) for d in LINKS])
        pl.semaphore_wait(barrier, len(LINKS))
        for link, slot in LAST:
            off, q = SENDS[link][slot]
            unit = whole.at[me.at(off), q]
            remote(unit, rest.at[link, slot - SPLIT], send_sem, recv_sem, me.neighbour(LINKS[link])).start()
        remote(rest, rest, send_sem, recv_sem, me.partner()).wait()


def write_unit(source, block, quarter, outs, sems):
    out_query, out_key, out_value = outs
    rows, depth = source.shape
    part = out_query.shape[0] // QUARTERS
    half = rows - part
    at = pl.ds(pl.multiple_of(block * depth, depth), depth)
    small = (out_key if quarter < 2 else out_value).at[pl.ds((quarter % 2) * half, half), at]
    pltpu.make_async_copy(source.at[pl.ds(0, part)], out_query.at[pl.ds(quarter * part, part), at], sems[0]).start()
    pltpu.make_async_copy(source.at[pl.ds(part, half)], small, sems[1 + quarter // 2]).start()


def wait_units(count, unit_bytes, out, sem):
    rows = count * unit_bytes // (out.shape[1] * out.dtype.itemsize)
    same = out.at[pl.ds(0, rows)]
    pltpu.make_async_copy(same, same, sem).wait()


def unit_bytes_of(whole):
    return whole.shape[-2] * whole.shape[-1] * whole.dtype.itemsize


def write_kernel(whole, out_query, out_key, out_value, token, sem):
    me = Place()
    outs = (out_query, out_key, out_value)
    token[...] = jnp.zeros_like(token)
    late = {arriving(*unit) for unit in LAST}

    @pl.when(me.core == LATE)
    def _():
        count = 0
        for off in [(dz, dy) for dz in range(SIDE) for dy in range(SIDE)]:
            for q in range(QUARTERS):
                if (off, q) not in late:
                    count += 1
                    block = me.at(off)
                    write_unit(whole.at[block, q], block, q, outs, (sem, sem, sem))
        wait_units(count, unit_bytes_of(whole), out_query, sem)


def write_rest_kernel(
    whole, rest, norm, in_query, in_key, in_value, out_query, out_key, out_value, out_norm, sem, norm_sem
):
    del in_query, in_key, in_value
    me = Place()
    outs = (out_query, out_key, out_value)
    norm_copy = pltpu.make_async_copy(norm, out_norm, norm_sem)
    norm_copy.start()

    @pl.when(me.core == LATE)
    def _():
        first = sem.at[0]
        for link, slot in LAST:
            off, q = arriving(link, slot)
            write_unit(rest.at[link, slot - SPLIT], me.at(off), q, outs, (first, first, first))
        wait_units(len(LAST), unit_bytes_of(whole), out_query, first)

    @pl.when(me.core != LATE)
    def _():
        @pl.loop(0, whole.shape[0])
        def _(block):
            for q in range(QUARTERS):
                write_unit(whole.at[block, q], block, q, outs, [sem.at[n] for n in range(len(outs))])

        for n, out in enumerate(outs):
            pltpu.make_async_copy(out, out, sem.at[n]).wait()

    norm_copy.wait()


def body(
    train_query, low_query, high_query,
    train_key, low_key, high_key,
    train_value, low_value, high_value,
    norm_train, norm_step,
):
    n_rows, n_cols = lax.axis_size("rows"), lax.axis_size("cols")
    depth, wide = train_query.shape
    tall = train_key.shape[1]
    rank = low_query.shape[1]
    unit = (wide + 2 * tall) // QUARTERS
    values = norm_train.shape[0]
    line = CORES * values
    dtype = train_query.dtype
    f32 = jnp.float32
    anywhere = pl.BlockSpec(memory_space=pl.ANY)
    vmem = pl.BlockSpec(memory_space=pltpu.VMEM)
    dma = pltpu.SemaphoreType.DMA
    shape = jax.ShapeDtypeStruct

    def pin(space, *arrays):
        return [pltpu.with_memory_space_constraint(a, space) for a in arrays]

    whole, norm = pl.pallas_call(
        gather_kernel,
        out_shape=(
            shape((n_rows, QUARTERS, unit, depth), dtype),
            shape((n_rows * n_cols // CORES, line), dtype),
        ),
        in_specs=[anywhere] * 11,
        out_specs=(vmem, vmem),
        scratch_shapes=[
            pltpu.VMEM((depth, wide), dtype),
            pltpu.VMEM((rank, depth), dtype),
            pltpu.VMEM((rank, wide), dtype),
            pltpu.VMEM((tall, depth), dtype),
            pltpu.VMEM((rank, depth), dtype),
            pltpu.VMEM((rank, tall), dtype),
            pltpu.VMEM((tall, depth), dtype),
            pltpu.VMEM((rank, depth), dtype),
            pltpu.VMEM((rank, tall), dtype),
            pltpu.VMEM((1, values), f32),
            pltpu.VMEM((1, values), f32),
            pltpu.VMEM((1, line), f32),
            pltpu.VMEM((n_rows, 1, line), f32),
            pltpu.VMEM((n_cols, n_rows, line), f32),
            pltpu.VMEM((SIDE * n_rows, line), f32),
            dma((15,)),
            dma(()),
            dma((len(GROUPS),)),
            dma((2,)),
            dma((2,)),
            dma((2,)),
            dma((2,)),
        ],
        compiler_params=pltpu.CompilerParams(
            collective_id=0, has_side_effects=True, vmem_limit_bytes=24 * 2**20
        ),
        name="gather",
    )(
        *pin(
            pltpu.HBM,
            train_query, low_query.T, high_query,
            train_key.T, low_key.T, high_key,
            train_value.T, low_value.T, high_value,
            norm_train.reshape(1, -1), norm_step.reshape(1, -1),
        )
    )
    outs = [shape((wide, n_rows * depth), dtype)] + [shape((tall, n_rows * depth), dtype)] * 2
    out_query, out_key, out_value, token = pl.pallas_call(
        write_kernel,
        out_shape=(*outs, shape((8, 128), f32)),
        in_specs=[vmem],
        out_specs=[anywhere] * 3 + [vmem],
        scratch_shapes=[dma(())],
        compiler_params=pltpu.CompilerParams(vmem_limit_bytes=4 * 2**20),
        name="write",
    )(*pin(pltpu.VMEM, whole))
    (rest,) = pl.pallas_call(
        finish_kernel,
        out_shape=(shape((len(LINKS), SLOTS - SPLIT, unit, depth), dtype),),
        in_specs=[vmem] * 2,
        out_specs=(vmem,),
        scratch_shapes=[dma(()), dma(())],
        compiler_params=pltpu.CompilerParams(
            collective_id=1, has_side_effects=True, vmem_limit_bytes=8 * 2**20
        ),
        name="finish",
    )(*pin(pltpu.VMEM, whole, token))
    out_query, out_key, out_value, out_norm = pl.pallas_call(
        write_rest_kernel,
        out_shape=(*outs, shape(norm.shape, dtype)),
        in_specs=[vmem] * 3 + [anywhere] * 3,
        out_specs=[anywhere] * 4,
        input_output_aliases={3: 0, 4: 1, 5: 2},
        scratch_shapes=[dma((len(outs),)), dma(())],
        compiler_params=pltpu.CompilerParams(vmem_limit_bytes=4 * 2**20),
        name="write_rest",
    )(*pin(pltpu.VMEM, whole, rest, norm), *pin(pltpu.HBM, out_query, out_key, out_value))
    return out_query, out_key, out_value, out_norm.reshape(-1)


def solution(mesh):
    return jax.shard_map(
        body,
        mesh=mesh,
        in_specs=(
            P("rows", "cols"),
            P("rows", None),
            P(None, "cols"),
            P("rows", "cols"),
            P("rows", None),
            P(None, "cols"),
            P("rows", "cols"),
            P("rows", None),
            P(None, "cols"),
            P(("rows", "cols")),
            P(("rows", "cols")),
        ),
        out_specs=(P("cols", None), P("cols", None), P("cols", None), P()),
        check_vma=False,
    )
```

```python
import jax
import jax.numpy as jnp
from jax import lax
from jax.experimental import pallas as pl
from jax.experimental.pallas import tpu as pltpu
from jax.sharding import PartitionSpec as P

MESH = pl.DeviceIdType.MESH

SIDE = 4
QUARTERS = 4
CORES = 2
LINKS = ((0, 1), (0, -1), (1, 0), (-1, 0))
LATE = 1
SPLIT = 12
LEAD = 2
ORDER = (0, 2, 1, 3)


def shift(off, d, sign=1):
    return ((off[0] + sign * d[0]) % SIDE, (off[1] + sign * d[1]) % SIDE)


def sends_of(link):
    d = LINKS[link]
    along_y = d[0] == 0
    first = (0, 1) if along_y else (2, 3)
    second = (2, 3) if along_y else (0, 1)
    positive = sum(d) > 0
    fwd_first = first[0] if positive else first[1]
    fwd_second = second[0] if positive else second[1]

    def across(n):
        return (n % SIDE, 0) if along_y else (0, n % SIDE)

    def behind(off):
        return shift(off, d, -1)

    own = (0, 0)
    return tuple((own, q) for q in ORDER) + (
        (across(-1), second[0]),
        (across(1), second[0]),
        (behind(own), fwd_first),
        (across(-1), second[1]),
        (across(1), second[1]),
        (behind(own), fwd_second),
        (across(2), second[0]),
        (across(2), second[1]),
        (behind(across(-1)), fwd_second),
        (behind(across(1)), fwd_second),
        (behind(across(2)), fwd_second),
    )


SENDS = tuple(sends_of(link) for link in range(len(LINKS)))
SLOTS = len(SENDS[0])
UNITS = [(link, slot) for slot in range(SLOTS) for link in range(len(LINKS))]


def arriving(link, slot):
    off, quarter = SENDS[link][slot]
    return shift(off, LINKS[link], -1), quarter


ARRIVES = {arriving(*unit): unit for unit in UNITS}
assert len(ARRIVES) == len(UNITS) == (SIDE * SIDE - 1) * QUARTERS
LAST = [unit for unit in UNITS if unit[1] >= SPLIT]
GROUPS = ((0, 1), (2, 3), (6,), (4, 5, 7, 8), (10, 11), (9,), (12, 13, 14))
GROUP_OF = {slot: group for group, slots in enumerate(GROUPS) for slot in slots}
assert sorted(GROUP_OF) == list(range(SLOTS)) and GROUPS[-1] == tuple(range(SPLIT, SLOTS))
AFTER = ((4, 5), (6, 7, 8, 9), (10, 11), (12, 13), (14,))
for _group, _slots in enumerate(AFTER):
    for _slot in _slots:
        for _link in range(len(LINKS)):
            assert GROUP_OF[ARRIVES[SENDS[_link][_slot]][1]] <= _group


class Place:
    def __init__(self):
        self.row, self.col = lax.axis_index("rows"), lax.axis_index("cols")
        self.z, self.y = self.row // SIDE, self.row % SIDE
        self.x, self.core = self.col // CORES, self.col % CORES

    def at(self, off):
        return ((self.z + off[0]) % SIDE) * SIDE + (self.y + off[1]) % SIDE

    def neighbour(self, d):
        return (self.at(d), self.col)

    def partner(self):
        return (self.row, self.x * CORES + 1 - self.core)

    def plane(self, n):
        return (self.row, (self.col + n) % (SIDE * CORES))


def remote(src, dst, send_sem, recv_sem, device):
    return pltpu.make_async_remote_copy(
        src_ref=src, dst_ref=dst, send_sem=send_sem, recv_sem=recv_sem, device_id=device, device_id_type=MESH
    )


def signal_all(barrier, devices):
    for device in devices:
        pl.semaphore_signal(barrier, inc=1, device_id=device, device_id_type=MESH)


def gather_kernel(
    train_query, low_query, high_query,
    train_key, low_key, high_key,
    train_value, low_value, high_value,
    norm_train, norm_step,
    whole, norm,
    tq, lq, hq, tk, lk, hk, tv, lv, hv, nt, ns, fresh, ring, lines, ordered,
    load_sem, send_sem, recv_sem, small_send, small_recv, norm_send,
):
    me = Place()
    wide = tq.shape[1]
    part = wide // QUARTERS
    blocks = whole.shape[0]
    top = me.z == 0
    leader = top & (me.y == LEAD)
    head = top & (me.y != LEAD)
    n_planes = lines.shape[0]
    column = [(dz, 0) for dz in range(1, SIDE)]
    heads = [(0, dy) for dy in range(1, SIDE)]

    barrier = pltpu.get_barrier_semaphore()
    peers = [me.neighbour(d) for d in LINKS] + [me.partner()]

    def greet():
        signal_all(barrier, peers)

        @pl.when(top)
        def _():
            signal_all(barrier, [me.neighbour((2, 0))])

        @pl.when(leader)
        def _():
            signal_all(barrier, [me.neighbour((0, 2))] + [me.plane(n) for n in range(1, n_planes)])

    part_of_high = part // 2
    rest_of_high = wide - part_of_high
    pieces = [(ORDER[0], 0, part // 2), (ORDER[0], part // 2, part)] + [(q, 0, part) for q in ORDER[1:]]

    def piece_load(n):
        q, start, end = pieces[n]
        cols = pl.ds(q * part + start, end - start)
        return train_query.at[:, cols], tq.at[:, cols]

    first, rest = pl.ds(0, part_of_high), pl.ds(part_of_high, rest_of_high)
    together = [
        [(low_query, lq), (high_query.at[:, first], hq.at[:, first]), piece_load(0)],
        [(high_query.at[:, rest], hq.at[:, rest]), piece_load(1), (train_key, tk), (low_key, lk)],
        [piece_load(2), (train_value, tv), (low_value, lv)],
        [piece_load(3)],
        [piece_load(4)],
        [(high_key, hk)],
        [(high_value, hv)],
        [(norm_train, nt)],
        [(norm_step, ns)],
    ]

    def start_loads(group):
        for src, dst in together[group]:
            pltpu.make_async_copy(src, dst, load_sem.at[group]).start()

    def wait_loads(group):
        if len(together[group]) == 1:
            src, dst = together[group][0]
        else:
            size = sum(dst.shape[0] * dst.shape[1] for _, dst in together[group])
            rows = pl.ds(0, size // wide)
            assert size % (8 * wide) == 0
            src, dst = train_query.at[rows], tq.at[rows]
        pltpu.make_async_copy(src, dst, load_sem.at[group]).wait()

    start_loads(0)
    greet()
    for group in (7, 8, 1, 5, 2, 6, 3, 4):
        start_loads(group)

    def merged(train, high, low):
        return train.astype(jnp.float32) + lax.dot_general(
            high, low, (((0,), (0,)), ((), ())), preferred_element_type=jnp.float32
        )

    def unit_copy(link, slot, what, rows=slice(None)):
        off, q = what
        unit = whole.at[me.at(off), q, rows]
        return remote(unit, unit, send_sem, recv_sem.at[GROUP_OF[slot]], me.neighbour(LINKS[link]))

    def send(link, slot, rows=slice(None)):
        unit_copy(link, slot, SENDS[link][slot], rows).start()

    def units(slots, sem):
        some = whole.at[pl.ds(0, slots * len(LINKS) // QUARTERS)]
        return remote(some, some, send_sem, sem, me.partner())

    def arrive(group):
        units(len(GROUPS[group]), recv_sem.at[group]).wait_recv()

    def only(core):
        return pl.when(me.core == LATE if core == LATE else me.core != LATE)

    def fresh_copy():
        return remote(fresh, ring.at[me.y * SIDE + me.z], small_send, small_recv.at[0], (me.y, me.col))

    def column_copy():
        part_of_ring = ring.at[pl.ds(me.y * SIDE, SIDE)]
        return remote(part_of_ring, part_of_ring, small_send, small_recv.at[1], (LEAD, me.col))

    def ring_lines(count, sem):
        some = ring.at[pl.ds(0, count)]
        return remote(some, some, small_send, sem, me.partner())

    def norm_copy(off):
        return remote(norm, norm, norm_send, small_recv.at[3], me.neighbour(off))

    def norm_sent(count):
        some = whole.at[0, 0, pl.ds(0, count * norm.shape[0] * norm.shape[1] // whole.shape[3])]
        remote(some, some, norm_send, small_recv.at[3], me.partner()).wait_send()

    def make_fresh():
        wait_loads(7)
        wait_loads(8)
        values = nt[...] + ns[...]
        fresh[...] = jnp.concatenate([values, values], axis=1)

    def send_fresh():
        @pl.when(top)
        def _():
            ring[me.y * SIDE + me.z] = fresh[...]

        @pl.when(jnp.logical_not(top))
        def _():
            fresh_copy().start()

    for n, (q, start, end) in enumerate(pieces):
        cols = pl.ds(q * part + start, end - start)
        wait_loads(n)
        if n == 1:
            make_fresh()
        whole[me.row, q, start:end, :] = merged(tq[:, cols].T, hq[:, cols], lq[...]).astype(whole.dtype)
        if n == 0:

            @pl.when(leader)
            def _():
                pl.semaphore_wait(barrier, len(peers) + n_planes - 1)

            far = (me.z == 2) | (top & (me.y == (LEAD + 2) % SIDE))

            @pl.when(far)
            def _():
                pl.semaphore_wait(barrier, len(peers) + 1)

            @pl.when(jnp.logical_not(leader | far))
            def _():
                pl.semaphore_wait(barrier, len(peers))

        if end == part:
            if n == 1:
                wait_loads(5)
            if n == 2:
                wait_loads(6)
            train, low, high = (tk, lk, hk) if q < 2 else (tv, lv, hv)
            small = merged(train[...], high[...], low[...]).astype(whole.dtype)
            half = small.shape[0] // 2
            whole[me.row, q, part:, :] = small[(q % 2) * half : (q % 2 + 1) * half, :]
        for link in range(len(LINKS)):
            if n == 0:
                send(link, 0, pl.ds(0, end))
            elif n == 1:
                send(link, 0, pl.ds(start, whole.shape[2] - start))
            else:
                send(link, ORDER.index(q))
        if n == 1:
            send_fresh()

    def norm_on_its_way(group):
        if group == 0:

            @pl.when(top)
            def _():
                ring_lines(len(column), small_recv.at[0]).wait_recv()

            @pl.when(head)
            def _():
                column_copy().start()

        if group == 1:

            @pl.when(leader)
            def _():
                ring_lines(len(heads) * SIDE, small_recv.at[1]).wait_recv()
                in_order = [ring[(i % SIDE) * SIDE + i // SIDE] for i in range(blocks)]
                lines[me.col] = jnp.concatenate(in_order, axis=0)
                for n in range(1, n_planes):
                    remote(lines.at[me.col], lines.at[me.col], small_send, small_recv.at[2], me.plane(n)).start()
                some = lines.at[pl.ds(0, n_planes - 1)]
                remote(some, some, small_send, small_recv.at[2], me.partner()).wait()
                lane = lax.broadcasted_iota(jnp.int32, lines.shape[1:], 1)
                for x in range(SIDE):
                    both = jnp.where(lane < lines.shape[2] // CORES, lines[CORES * x], lines[CORES * x + 1])
                    ordered[pl.Slice(x, blocks, SIDE), :] = both
                norm[...] = ordered[...].astype(norm.dtype)
                for off in heads + column:
                    norm_copy(off).start()

        if group == 2:

            @pl.when(head)
            def _():
                norm_copy((1, 0)).wait_recv()
                for off in column:
                    norm_copy(off).start()

    def send_slots(slots):
        for slot in slots:
            for link in range(len(LINKS)):
                send(link, slot)

    for group, slots in enumerate(AFTER):
        arrive(group)
        norm_on_its_way(group)
        if slots[0] < SPLIT:
            send_slots(slots)
        else:

            @only(1 - LATE)
            def _():
                send_slots(slots)

    arrive(5)

    @only(1 - LATE)
    def _():
        arrive(6)
        units(SLOTS, recv_sem.at[0]).wait_send()

    @only(LATE)
    def _():
        units(SPLIT, recv_sem.at[0]).wait_send()

    @pl.when(leader)
    def _():
        norm_sent(len(heads) + len(column))

    @pl.when(head)
    def _():
        column_copy().wait_send()
        norm_sent(len(column))

    @pl.when(jnp.logical_not(top))
    def _():
        fresh_copy().wait_send()
        norm_copy((1, 0)).wait_recv()


def finish_kernel(whole, token, rest, send_sem, recv_sem):
    del token
    me = Place()

    @pl.when(me.core == LATE)
    def _():
        barrier = pltpu.get_barrier_semaphore()
        signal_all(barrier, [me.neighbour(d) for d in LINKS])
        pl.semaphore_wait(barrier, len(LINKS))
        for link, slot in LAST:
            off, q = SENDS[link][slot]
            unit = whole.at[me.at(off), q]
            remote(unit, rest.at[link, slot - SPLIT], send_sem, recv_sem, me.neighbour(LINKS[link])).start()
        remote(rest, rest, send_sem, recv_sem, me.partner()).wait()


def write_unit(source, block, quarter, outs, sems):
    out_query, out_key, out_value = outs
    rows, depth = source.shape
    part = out_query.shape[0] // QUARTERS
    half = rows - part
    at = pl.ds(pl.multiple_of(block * depth, depth), depth)
    small = (out_key if quarter < 2 else out_value).at[pl.ds((quarter % 2) * half, half), at]
    pltpu.make_async_copy(source.at[pl.ds(0, part)], out_query.at[pl.ds(quarter * part, part), at], sems[0]).start()
    pltpu.make_async_copy(source.at[pl.ds(part, half)], small, sems[1 + quarter // 2]).start()


def wait_units(count, unit_bytes, out, sem):
    rows = count * unit_bytes // (out.shape[1] * out.dtype.itemsize)
    same = out.at[pl.ds(0, rows)]
    pltpu.make_async_copy(same, same, sem).wait()


def unit_bytes_of(whole):
    return whole.shape[-2] * whole.shape[-1] * whole.dtype.itemsize


def write_kernel(whole, out_query, out_key, out_value, token, sem):
    me = Place()
    outs = (out_query, out_key, out_value)
    token[...] = jnp.zeros_like(token)
    late = {arriving(*unit) for unit in LAST}

    @pl.when(me.core == LATE)
    def _():
        count = 0
        for off in [(dz, dy) for dz in range(SIDE) for dy in range(SIDE)]:
            for q in range(QUARTERS):
                if (off, q) not in late:
                    count += 1
                    block = me.at(off)
                    write_unit(whole.at[block, q], block, q, outs, (sem, sem, sem))
        wait_units(count, unit_bytes_of(whole), out_query, sem)


def write_rest_kernel(
    whole, rest, norm, in_query, in_key, in_value, out_query, out_key, out_value, out_norm, sem, norm_sem
):
    del in_query, in_key, in_value
    me = Place()
    outs = (out_query, out_key, out_value)
    norm_copy = pltpu.make_async_copy(norm, out_norm, norm_sem)
    norm_copy.start()

    @pl.when(me.core == LATE)
    def _():
        first = sem.at[0]
        for link, slot in LAST:
            off, q = arriving(link, slot)
            write_unit(rest.at[link, slot - SPLIT], me.at(off), q, outs, (first, first, first))
        wait_units(len(LAST), unit_bytes_of(whole), out_query, first)

    @pl.when(me.core != LATE)
    def _():
        @pl.loop(0, whole.shape[0])
        def _(block):
            for q in range(QUARTERS):
                write_unit(whole.at[block, q], block, q, outs, [sem.at[n] for n in range(len(outs))])

        for n, out in enumerate(outs):
            pltpu.make_async_copy(out, out, sem.at[n]).wait()

    norm_copy.wait()


def body(
    train_query, low_query, high_query,
    train_key, low_key, high_key,
    train_value, low_value, high_value,
    norm_train, norm_step,
):
    n_rows, n_cols = lax.axis_size("rows"), lax.axis_size("cols")
    depth, wide = train_query.shape
    tall = train_key.shape[1]
    rank = low_query.shape[1]
    unit = (wide + 2 * tall) // QUARTERS
    values = norm_train.shape[0]
    line = CORES * values
    dtype = train_query.dtype
    f32 = jnp.float32
    anywhere = pl.BlockSpec(memory_space=pl.ANY)
    vmem = pl.BlockSpec(memory_space=pltpu.VMEM)
    dma = pltpu.SemaphoreType.DMA
    shape = jax.ShapeDtypeStruct

    def pin(space, *arrays):
        return [pltpu.with_memory_space_constraint(a, space) for a in arrays]

    whole, norm = pl.pallas_call(
        gather_kernel,
        out_shape=(
            shape((n_rows, QUARTERS, unit, depth), dtype),
            shape((n_rows * n_cols // CORES, line), dtype),
        ),
        in_specs=[anywhere] * 11,
        out_specs=(vmem, vmem),
        scratch_shapes=[
            pltpu.VMEM((depth, wide), dtype),
            pltpu.VMEM((rank, depth), dtype),
            pltpu.VMEM((rank, wide), dtype),
            pltpu.VMEM((tall, depth), dtype),
            pltpu.VMEM((rank, depth), dtype),
            pltpu.VMEM((rank, tall), dtype),
            pltpu.VMEM((tall, depth), dtype),
            pltpu.VMEM((rank, depth), dtype),
            pltpu.VMEM((rank, tall), dtype),
            pltpu.VMEM((1, values), f32),
            pltpu.VMEM((1, values), f32),
            pltpu.VMEM((1, line), f32),
            pltpu.VMEM((n_rows, 1, line), f32),
            pltpu.VMEM((n_cols, n_rows, line), f32),
            pltpu.VMEM((SIDE * n_rows, line), f32),
            dma((9,)),
            dma(()),
            dma((len(GROUPS),)),
            dma(()),
            dma((4,)),
            dma(()),
        ],
        compiler_params=pltpu.CompilerParams(
            collective_id=0, has_side_effects=True, vmem_limit_bytes=24 * 2**20
        ),
        name="gather",
    )(
        *pin(
            pltpu.HBM,
            train_query, low_query.T, high_query,
            train_key.T, low_key.T, high_key,
            train_value.T, low_value.T, high_value,
            norm_train.reshape(1, -1), norm_step.reshape(1, -1),
        )
    )
    outs = [shape((wide, n_rows * depth), dtype)] + [shape((tall, n_rows * depth), dtype)] * 2
    out_query, out_key, out_value, token = pl.pallas_call(
        write_kernel,
        out_shape=(*outs, shape((8, 128), f32)),
        in_specs=[vmem],
        out_specs=[anywhere] * 3 + [vmem],
        scratch_shapes=[dma(())],
        compiler_params=pltpu.CompilerParams(vmem_limit_bytes=4 * 2**20),
        name="write",
    )(*pin(pltpu.VMEM, whole))
    (rest,) = pl.pallas_call(
        finish_kernel,
        out_shape=(shape((len(LINKS), SLOTS - SPLIT, unit, depth), dtype),),
        in_specs=[vmem] * 2,
        out_specs=(vmem,),
        scratch_shapes=[dma(()), dma(())],
        compiler_params=pltpu.CompilerParams(
            collective_id=1, has_side_effects=True, vmem_limit_bytes=8 * 2**20
        ),
        name="finish",
    )(*pin(pltpu.VMEM, whole, token))
    out_query, out_key, out_value, out_norm = pl.pallas_call(
        write_rest_kernel,
        out_shape=(*outs, shape(norm.shape, dtype)),
        in_specs=[vmem] * 3 + [anywhere] * 3,
        out_specs=[anywhere] * 4,
        input_output_aliases={3: 0, 4: 1, 5: 2},
        scratch_shapes=[dma((len(outs),)), dma(())],
        compiler_params=pltpu.CompilerParams(vmem_limit_bytes=4 * 2**20),
        name="write_rest",
    )(*pin(pltpu.VMEM, whole, rest, norm), *pin(pltpu.HBM, out_query, out_key, out_value))
    return out_query, out_key, out_value, out_norm.reshape(-1)


def solution(mesh):
    return jax.shard_map(
        body,
        mesh=mesh,
        in_specs=(
            P("rows", "cols"),
            P("rows", None),
            P(None, "cols"),
            P("rows", "cols"),
            P("rows", None),
            P(None, "cols"),
            P("rows", "cols"),
            P("rows", None),
            P(None, "cols"),
            P(("rows", "cols")),
            P(("rows", "cols")),
        ),
        out_specs=(P("cols", None), P("cols", None), P("cols", None), P()),
        check_vma=False,
    )
```

```python
import jax
import jax.numpy as jnp
from jax import lax
from jax.experimental import pallas as pl
from jax.experimental.pallas import tpu as pltpu
from jax.sharding import PartitionSpec as P

MESH = pl.DeviceIdType.MESH

SIDE = 4
QUARTERS = 4
CORES = 2
LINKS = ((0, 1), (0, -1), (1, 0), (-1, 0))
LATE = 0
SPLIT = 12
LEAD = 2
ORDER = (0, 2, 1, 3)


def shift(off, d, sign=1):
    return ((off[0] + sign * d[0]) % SIDE, (off[1] + sign * d[1]) % SIDE)


def sends_of(link):
    d = LINKS[link]
    along_y = d[0] == 0
    first = (0, 1) if along_y else (2, 3)
    second = (2, 3) if along_y else (0, 1)
    positive = sum(d) > 0
    fwd_first = first[0] if positive else first[1]
    fwd_second = second[0] if positive else second[1]

    def across(n):
        return (n % SIDE, 0) if along_y else (0, n % SIDE)

    def behind(off):
        return shift(off, d, -1)

    own = (0, 0)
    return tuple((own, q) for q in ORDER) + (
        (across(-1), second[0]),
        (across(1), second[0]),
        (behind(own), fwd_first),
        (across(-1), second[1]),
        (across(1), second[1]),
        (behind(own), fwd_second),
        (across(2), second[0]),
        (across(2), second[1]),
        (behind(across(-1)), fwd_second),
        (behind(across(1)), fwd_second),
        (behind(across(2)), fwd_second),
    )


SENDS = tuple(sends_of(link) for link in range(len(LINKS)))
SLOTS = len(SENDS[0])
UNITS = [(link, slot) for slot in range(SLOTS) for link in range(len(LINKS))]


def arriving(link, slot):
    off, quarter = SENDS[link][slot]
    return shift(off, LINKS[link], -1), quarter


ARRIVES = {arriving(*unit): unit for unit in UNITS}
assert len(ARRIVES) == len(UNITS) == (SIDE * SIDE - 1) * QUARTERS
LAST = [unit for unit in UNITS if unit[1] >= SPLIT]
GROUPS = ((0, 1), (2, 3), (6,), (4, 5, 7, 8), (10, 11), (9,), (12, 13, 14))
GROUP_OF = {slot: group for group, slots in enumerate(GROUPS) for slot in slots}
assert sorted(GROUP_OF) == list(range(SLOTS)) and GROUPS[-1] == tuple(range(SPLIT, SLOTS))
AFTER = ((4, 5), (6, 7, 8, 9), (10, 11), (12, 13), (14,))
for _group, _slots in enumerate(AFTER):
    for _slot in _slots:
        for _link in range(len(LINKS)):
            assert GROUP_OF[ARRIVES[SENDS[_link][_slot]][1]] <= _group


class Place:
    def __init__(self):
        self.row, self.col = lax.axis_index("rows"), lax.axis_index("cols")
        self.z, self.y = self.row // SIDE, self.row % SIDE
        self.x, self.core = self.col // CORES, self.col % CORES

    def at(self, off):
        return ((self.z + off[0]) % SIDE) * SIDE + (self.y + off[1]) % SIDE

    def neighbour(self, d):
        return (self.at(d), self.col)

    def partner(self):
        return (self.row, self.x * CORES + 1 - self.core)

    def plane(self, n):
        return (self.row, (self.col + n) % (SIDE * CORES))


def remote(src, dst, send_sem, recv_sem, device):
    return pltpu.make_async_remote_copy(
        src_ref=src, dst_ref=dst, send_sem=send_sem, recv_sem=recv_sem, device_id=device, device_id_type=MESH
    )


def signal_all(barrier, devices):
    for device in devices:
        pl.semaphore_signal(barrier, inc=1, device_id=device, device_id_type=MESH)


def gather_kernel(
    train_query, low_query, high_query,
    train_key, low_key, high_key,
    train_value, low_value, high_value,
    norm_train, norm_step,
    whole, norm,
    tq, lq, hq, tk, lk, hk, tv, lv, hv, nt, ns, fresh, ring, lines, ordered,
    load_sem, send_sem, recv_sem, small_send, small_recv, norm_send,
):
    me = Place()
    wide = tq.shape[1]
    part = wide // QUARTERS
    blocks = whole.shape[0]
    top = me.z == 0
    leader = top & (me.y == LEAD)
    head = top & (me.y != LEAD)
    n_planes = lines.shape[0]
    column = [(dz, 0) for dz in range(1, SIDE)]
    heads = [(0, dy) for dy in range(1, SIDE)]

    barrier = pltpu.get_barrier_semaphore()
    peers = [me.neighbour(d) for d in LINKS] + [me.partner()]

    def greet():
        signal_all(barrier, peers)

        @pl.when(top)
        def _():
            signal_all(barrier, [me.neighbour((2, 0))])

        @pl.when(leader)
        def _():
            signal_all(barrier, [me.neighbour((0, 2))] + [me.plane(n) for n in range(1, n_planes)])

    part_of_high = part // 2
    rest_of_high = wide - part_of_high
    pieces = [(ORDER[0], 0, part // 2), (ORDER[0], part // 2, part)] + [(q, 0, part) for q in ORDER[1:]]

    def piece_load(n):
        q, start, end = pieces[n]
        cols = pl.ds(q * part + start, end - start)
        return train_query.at[:, cols], tq.at[:, cols]

    first, rest = pl.ds(0, part_of_high), pl.ds(part_of_high, rest_of_high)
    together = [
        [(low_query, lq), (high_query.at[:, first], hq.at[:, first]), piece_load(0)],
        [(high_query.at[:, rest], hq.at[:, rest]), piece_load(1), (train_key, tk), (low_key, lk)],
        [piece_load(2), (train_value, tv), (low_value, lv)],
        [piece_load(3)],
        [piece_load(4)],
        [(high_key, hk)],
        [(high_value, hv)],
        [(norm_train, nt)],
        [(norm_step, ns)],
    ]

    def start_loads(group):
        for src, dst in together[group]:
            pltpu.make_async_copy(src, dst, load_sem.at[group]).start()

    def wait_loads(group):
        if len(together[group]) == 1:
            src, dst = together[group][0]
        else:
            size = sum(dst.shape[0] * dst.shape[1] for _, dst in together[group])
            rows = pl.ds(0, size // wide)
            assert size % (8 * wide) == 0
            src, dst = train_query.at[rows], tq.at[rows]
        pltpu.make_async_copy(src, dst, load_sem.at[group]).wait()

    start_loads(0)
    greet()
    for group in (7, 8, 1, 5, 2, 6, 3, 4):
        start_loads(group)

    def merged(train, high, low):
        return train.astype(jnp.float32) + lax.dot_general(
            high, low, (((0,), (0,)), ((), ())), preferred_element_type=jnp.float32
        )

    def unit_copy(link, slot, what, rows=slice(None)):
        off, q = what
        unit = whole.at[me.at(off), q, rows]
        return remote(unit, unit, send_sem, recv_sem.at[GROUP_OF[slot]], me.neighbour(LINKS[link]))

    def send(link, slot, rows=slice(None)):
        unit_copy(link, slot, SENDS[link][slot], rows).start()

    def units(slots, sem):
        some = whole.at[pl.ds(0, slots * len(LINKS) // QUARTERS)]
        return remote(some, some, send_sem, sem, me.partner())

    def arrive(group):
        units(len(GROUPS[group]), recv_sem.at[group]).wait_recv()

    def only(core):
        return pl.when(me.core == LATE if core == LATE else me.core != LATE)

    def fresh_copy():
        return remote(fresh, ring.at[me.y * SIDE + me.z], small_send, small_recv.at[0], (me.y, me.col))

    def column_copy():
        part_of_ring = ring.at[pl.ds(me.y * SIDE, SIDE)]
        return remote(part_of_ring, part_of_ring, small_send, small_recv.at[1], (LEAD, me.col))

    def ring_lines(count, sem):
        some = ring.at[pl.ds(0, count)]
        return remote(some, some, small_send, sem, me.partner())

    def norm_copy(off):
        return remote(norm, norm, norm_send, small_recv.at[3], me.neighbour(off))

    def norm_sent(count):
        some = whole.at[0, 0, pl.ds(0, count * norm.shape[0] * norm.shape[1] // whole.shape[3])]
        remote(some, some, norm_send, small_recv.at[3], me.partner()).wait_send()

    def make_fresh():
        wait_loads(7)
        wait_loads(8)
        values = nt[...] + ns[...]
        fresh[...] = jnp.concatenate([values, values], axis=1)

    def send_fresh():
        @pl.when(top)
        def _():
            ring[me.y * SIDE + me.z] = fresh[...]

        @pl.when(jnp.logical_not(top))
        def _():
            fresh_copy().start()

    for n, (q, start, end) in enumerate(pieces):
        cols = pl.ds(q * part + start, end - start)
        wait_loads(n)
        if n == 1:
            make_fresh()
        whole[me.row, q, start:end, :] = merged(tq[:, cols].T, hq[:, cols], lq[...]).astype(whole.dtype)
        if n == 0:

            @pl.when(leader)
            def _():
                pl.semaphore_wait(barrier, len(peers) + n_planes - 1)

            far = (me.z == 2) | (top & (me.y == (LEAD + 2) % SIDE))

            @pl.when(far)
            def _():
                pl.semaphore_wait(barrier, len(peers) + 1)

            @pl.when(jnp.logical_not(leader | far))
            def _():
                pl.semaphore_wait(barrier, len(peers))

        if end == part:
            if n == 1:
                wait_loads(5)
            if n == 2:
                wait_loads(6)
            train, low, high = (tk, lk, hk) if q < 2 else (tv, lv, hv)
            small = merged(train[...], high[...], low[...]).astype(whole.dtype)
            half = small.shape[0] // 2
            whole[me.row, q, part:, :] = small[(q % 2) * half : (q % 2 + 1) * half, :]
        for link in range(len(LINKS)):
            if n == 0:
                send(link, 0, pl.ds(0, end))
            elif n == 1:
                send(link, 0, pl.ds(start, whole.shape[2] - start))
            else:
                send(link, ORDER.index(q))
        if n == 1:
            send_fresh()

    def norm_on_its_way(group):
        if group == 0:

            @pl.when(top)
            def _():
                ring_lines(len(column), small_recv.at[0]).wait_recv()

            @pl.when(head)
            def _():
                column_copy().start()

        if group == 1:

            @pl.when(leader)
            def _():
                ring_lines(len(heads) * SIDE, small_recv.at[1]).wait_recv()
                in_order = [ring[(i % SIDE) * SIDE + i // SIDE] for i in range(blocks)]
                lines[me.col] = jnp.concatenate(in_order, axis=0)
                for n in range(1, n_planes):
                    remote(lines.at[me.col], lines.at[me.col], small_send, small_recv.at[2], me.plane(n)).start()
                some = lines.at[pl.ds(0, n_planes - 1)]
                remote(some, some, small_send, small_recv.at[2], me.partner()).wait()
                lane = lax.broadcasted_iota(jnp.int32, lines.shape[1:], 1)
                for x in range(SIDE):
                    both = jnp.where(lane < lines.shape[2] // CORES, lines[CORES * x], lines[CORES * x + 1])
                    ordered[pl.Slice(x, blocks, SIDE), :] = both
                norm[...] = ordered[...].astype(norm.dtype)
                for off in heads + column:
                    norm_copy(off).start()

        if group == 2:

            @pl.when(head)
            def _():
                norm_copy((1, 0)).wait_recv()
                for off in column:
                    norm_copy(off).start()

    def send_slots(slots):
        for slot in slots:
            for link in range(len(LINKS)):
                send(link, slot)

    for group, slots in enumerate(AFTER):
        arrive(group)
        norm_on_its_way(group)
        if slots[0] < SPLIT:
            send_slots(slots)
        else:

            @only(1 - LATE)
            def _():
                send_slots(slots)

    arrive(5)

    @only(1 - LATE)
    def _():
        arrive(6)
        units(SLOTS, recv_sem.at[0]).wait_send()

    @only(LATE)
    def _():
        units(SPLIT, recv_sem.at[0]).wait_send()

    @pl.when(leader)
    def _():
        norm_sent(len(heads) + len(column))

    @pl.when(head)
    def _():
        column_copy().wait_send()
        norm_sent(len(column))

    @pl.when(jnp.logical_not(top))
    def _():
        fresh_copy().wait_send()
        norm_copy((1, 0)).wait_recv()


def finish_kernel(whole, token, rest, send_sem, recv_sem):
    del token
    me = Place()

    @pl.when(me.core == LATE)
    def _():
        barrier = pltpu.get_barrier_semaphore()
        signal_all(barrier, [me.neighbour(d) for d in LINKS])
        pl.semaphore_wait(barrier, len(LINKS))
        for link, slot in LAST:
            off, q = SENDS[link][slot]
            unit = whole.at[me.at(off), q]
            remote(unit, rest.at[link, slot - SPLIT], send_sem, recv_sem, me.neighbour(LINKS[link])).start()
        remote(rest, rest, send_sem, recv_sem, me.partner()).wait()


def write_unit(source, block, quarter, outs, sems):
    out_query, out_key, out_value = outs
    rows, depth = source.shape
    part = out_query.shape[0] // QUARTERS
    half = rows - part
    at = pl.ds(pl.multiple_of(block * depth, depth), depth)
    small = (out_key if quarter < 2 else out_value).at[pl.ds((quarter % 2) * half, half), at]
    pltpu.make_async_copy(source.at[pl.ds(0, part)], out_query.at[pl.ds(quarter * part, part), at], sems[0]).start()
    pltpu.make_async_copy(source.at[pl.ds(part, half)], small, sems[1 + quarter // 2]).start()


def wait_units(count, unit_bytes, out, sem):
    rows = count * unit_bytes // (out.shape[1] * out.dtype.itemsize)
    same = out.at[pl.ds(0, rows)]
    pltpu.make_async_copy(same, same, sem).wait()


def unit_bytes_of(whole):
    return whole.shape[-2] * whole.shape[-1] * whole.dtype.itemsize


def write_kernel(whole, out_query, out_key, out_value, token, sem):
    me = Place()
    outs = (out_query, out_key, out_value)
    token[...] = jnp.zeros_like(token)
    late = {arriving(*unit) for unit in LAST}

    @pl.when(me.core == LATE)
    def _():
        count = 0
        for off in [(dz, dy) for dz in range(SIDE) for dy in range(SIDE)]:
            for q in range(QUARTERS):
                if (off, q) not in late:
                    count += 1
                    block = me.at(off)
                    write_unit(whole.at[block, q], block, q, outs, (sem, sem, sem))
        wait_units(count, unit_bytes_of(whole), out_query, sem)


def write_rest_kernel(
    whole, rest, norm, in_query, in_key, in_value, out_query, out_key, out_value, out_norm, sem, norm_sem
):
    del in_query, in_key, in_value
    me = Place()
    outs = (out_query, out_key, out_value)
    norm_copy = pltpu.make_async_copy(norm, out_norm, norm_sem)
    norm_copy.start()

    @pl.when(me.core == LATE)
    def _():
        first = sem.at[0]
        for link, slot in LAST:
            off, q = arriving(link, slot)
            write_unit(rest.at[link, slot - SPLIT], me.at(off), q, outs, (first, first, first))
        wait_units(len(LAST), unit_bytes_of(whole), out_query, first)

    @pl.when(me.core != LATE)
    def _():
        @pl.loop(0, whole.shape[0])
        def _(block):
            for q in range(QUARTERS):
                write_unit(whole.at[block, q], block, q, outs, [sem.at[n] for n in range(len(outs))])

        for n, out in enumerate(outs):
            pltpu.make_async_copy(out, out, sem.at[n]).wait()

    norm_copy.wait()


def body(
    train_query, low_query, high_query,
    train_key, low_key, high_key,
    train_value, low_value, high_value,
    norm_train, norm_step,
):
    n_rows, n_cols = lax.axis_size("rows"), lax.axis_size("cols")
    depth, wide = train_query.shape
    tall = train_key.shape[1]
    rank = low_query.shape[1]
    unit = (wide + 2 * tall) // QUARTERS
    values = norm_train.shape[0]
    line = CORES * values
    dtype = train_query.dtype
    f32 = jnp.float32
    anywhere = pl.BlockSpec(memory_space=pl.ANY)
    vmem = pl.BlockSpec(memory_space=pltpu.VMEM)
    dma = pltpu.SemaphoreType.DMA
    shape = jax.ShapeDtypeStruct

    def pin(space, *arrays):
        return [pltpu.with_memory_space_constraint(a, space) for a in arrays]

    whole, norm = pl.pallas_call(
        gather_kernel,
        out_shape=(
            shape((n_rows, QUARTERS, unit, depth), dtype),
            shape((n_rows * n_cols // CORES, line), dtype),
        ),
        in_specs=[anywhere] * 11,
        out_specs=(vmem, vmem),
        scratch_shapes=[
            pltpu.VMEM((depth, wide), dtype),
            pltpu.VMEM((rank, depth), dtype),
            pltpu.VMEM((rank, wide), dtype),
            pltpu.VMEM((tall, depth), dtype),
            pltpu.VMEM((rank, depth), dtype),
            pltpu.VMEM((rank, tall), dtype),
            pltpu.VMEM((tall, depth), dtype),
            pltpu.VMEM((rank, depth), dtype),
            pltpu.VMEM((rank, tall), dtype),
            pltpu.VMEM((1, values), f32),
            pltpu.VMEM((1, values), f32),
            pltpu.VMEM((1, line), f32),
            pltpu.VMEM((n_rows, 1, line), f32),
            pltpu.VMEM((n_cols, n_rows, line), f32),
            pltpu.VMEM((SIDE * n_rows, line), f32),
            dma((9,)),
            dma(()),
            dma((len(GROUPS),)),
            dma(()),
            dma((4,)),
            dma(()),
        ],
        compiler_params=pltpu.CompilerParams(
            collective_id=0, has_side_effects=True, vmem_limit_bytes=24 * 2**20
        ),
        name="gather",
    )(
        *pin(
            pltpu.HBM,
            train_query, low_query.T, high_query,
            train_key.T, low_key.T, high_key,
            train_value.T, low_value.T, high_value,
            norm_train.reshape(1, -1), norm_step.reshape(1, -1),
        )
    )
    outs = [shape((wide, n_rows * depth), dtype)] + [shape((tall, n_rows * depth), dtype)] * 2
    out_query, out_key, out_value, token = pl.pallas_call(
        write_kernel,
        out_shape=(*outs, shape((8, 128), f32)),
        in_specs=[vmem],
        out_specs=[anywhere] * 3 + [vmem],
        scratch_shapes=[dma(())],
        compiler_params=pltpu.CompilerParams(vmem_limit_bytes=4 * 2**20),
        name="write",
    )(*pin(pltpu.VMEM, whole))
    (rest,) = pl.pallas_call(
        finish_kernel,
        out_shape=(shape((len(LINKS), SLOTS - SPLIT, unit, depth), dtype),),
        in_specs=[vmem] * 2,
        out_specs=(vmem,),
        scratch_shapes=[dma(()), dma(())],
        compiler_params=pltpu.CompilerParams(
            collective_id=1, has_side_effects=True, vmem_limit_bytes=8 * 2**20
        ),
        name="finish",
    )(*pin(pltpu.VMEM, whole, token))
    out_query, out_key, out_value, out_norm = pl.pallas_call(
        write_rest_kernel,
        out_shape=(*outs, shape(norm.shape, dtype)),
        in_specs=[vmem] * 3 + [anywhere] * 3,
        out_specs=[anywhere] * 4,
        input_output_aliases={3: 0, 4: 1, 5: 2},
        scratch_shapes=[dma((len(outs),)), dma(())],
        compiler_params=pltpu.CompilerParams(vmem_limit_bytes=4 * 2**20),
        name="write_rest",
    )(*pin(pltpu.VMEM, whole, rest, norm), *pin(pltpu.HBM, out_query, out_key, out_value))
    return out_query, out_key, out_value, out_norm.reshape(-1)


def solution(mesh):
    return jax.shard_map(
        body,
        mesh=mesh,
        in_specs=(
            P("rows", "cols"),
            P("rows", None),
            P(None, "cols"),
            P("rows", "cols"),
            P("rows", None),
            P(None, "cols"),
            P("rows", "cols"),
            P("rows", None),
            P(None, "cols"),
            P(("rows", "cols")),
            P(("rows", "cols")),
        ),
        out_specs=(P("cols", None), P("cols", None), P("cols", None), P()),
        check_vma=False,
    )
```

```python
import jax
import jax.numpy as jnp
from jax import lax
from jax.experimental import pallas as pl
from jax.experimental.pallas import tpu as pltpu
from jax.sharding import PartitionSpec as P

MESH = pl.DeviceIdType.MESH

SIDE = 4
QUARTERS = 4
CORES = 2
LINKS = ((0, 1), (0, -1), (1, 0), (-1, 0))
LATE = 1
SPLIT = 12
LEAD = 2
ORDER = (0, 2, 1, 3)


def shift(off, d, sign=1):
    return ((off[0] + sign * d[0]) % SIDE, (off[1] + sign * d[1]) % SIDE)


def sends_of(link):
    d = LINKS[link]
    along_y = d[0] == 0
    first = (0, 1) if along_y else (2, 3)
    second = (2, 3) if along_y else (0, 1)
    positive = sum(d) > 0
    fwd_first = first[0] if positive else first[1]
    fwd_second = second[0] if positive else second[1]

    def across(n):
        return (n % SIDE, 0) if along_y else (0, n % SIDE)

    def behind(off):
        return shift(off, d, -1)

    own = (0, 0)
    return tuple((own, q) for q in ORDER) + (
        (across(-1), second[0]),
        (across(1), second[0]),
        (behind(own), fwd_first),
        (across(-1), second[1]),
        (across(1), second[1]),
        (behind(own), fwd_second),
        (across(2), second[0]),
        (across(2), second[1]),
        (behind(across(-1)), fwd_second),
        (behind(across(1)), fwd_second),
        (behind(across(2)), fwd_second),
    )


SENDS = tuple(sends_of(link) for link in range(len(LINKS)))
SLOTS = len(SENDS[0])
UNITS = [(link, slot) for slot in range(SLOTS) for link in range(len(LINKS))]


def arriving(link, slot):
    off, quarter = SENDS[link][slot]
    return shift(off, LINKS[link], -1), quarter


ARRIVES = {arriving(*unit): unit for unit in UNITS}
assert len(ARRIVES) == len(UNITS) == (SIDE * SIDE - 1) * QUARTERS
LAST = [unit for unit in UNITS if unit[1] >= SPLIT]
GROUPS = ((0, 1), (2, 3), (6,), (4, 5, 7, 8), (10, 11), (9,), (12, 13, 14))
GROUP_OF = {slot: group for group, slots in enumerate(GROUPS) for slot in slots}
assert sorted(GROUP_OF) == list(range(SLOTS)) and GROUPS[-1] == tuple(range(SPLIT, SLOTS))
AFTER = ((4, 5), (6, 7, 8, 9), (10, 11), (12, 13), (14,))
for _group, _slots in enumerate(AFTER):
    for _slot in _slots:
        for _link in range(len(LINKS)):
            assert GROUP_OF[ARRIVES[SENDS[_link][_slot]][1]] <= _group


class Place:
    def __init__(self):
        self.row, self.col = lax.axis_index("rows"), lax.axis_index("cols")
        self.z, self.y = self.row // SIDE, self.row % SIDE
        self.x, self.core = self.col // CORES, self.col % CORES

    def at(self, off):
        return ((self.z + off[0]) % SIDE) * SIDE + (self.y + off[1]) % SIDE

    def neighbour(self, d):
        return (self.at(d), self.col)

    def partner(self):
        return (self.row, self.x * CORES + 1 - self.core)

    def plane(self, n):
        return (self.row, (self.col + n) % (SIDE * CORES))


def remote(src, dst, send_sem, recv_sem, device):
    return pltpu.make_async_remote_copy(
        src_ref=src, dst_ref=dst, send_sem=send_sem, recv_sem=recv_sem, device_id=device, device_id_type=MESH
    )


def signal_all(barrier, devices):
    for device in devices:
        pl.semaphore_signal(barrier, inc=1, device_id=device, device_id_type=MESH)


def gather_kernel(
    train_query, low_query, high_query,
    train_key, low_key, high_key,
    train_value, low_value, high_value,
    norm_train, norm_step,
    whole, norm,
    tq, lq, hq, tk, lk, hk, tv, lv, hv, nt, ns, fresh, ring, lines, ordered,
    load_sem, send_sem, recv_sem, small_send, small_recv, norm_send,
):
    me = Place()
    wide = tq.shape[1]
    part = wide // QUARTERS
    blocks = whole.shape[0]
    top = me.z == 0
    leader = top & (me.y == LEAD)
    head = top & (me.y != LEAD)
    n_planes = lines.shape[0]
    column = [(dz, 0) for dz in range(1, SIDE)]
    heads = [(0, dy) for dy in range(1, SIDE)]

    barrier = pltpu.get_barrier_semaphore()
    peers = [me.neighbour(d) for d in LINKS] + [me.partner()]

    def greet():
        signal_all(barrier, peers)

        @pl.when(top)
        def _():
            signal_all(barrier, [me.neighbour((2, 0))])

        @pl.when(leader)
        def _():
            signal_all(barrier, [me.neighbour((0, 2))] + [me.plane(n) for n in range(1, n_planes)])

    part_of_high = part // 2
    rest_of_high = wide - part_of_high
    pieces = [(ORDER[0], 0, part // 2), (ORDER[0], part // 2, part)] + [(q, 0, part) for q in ORDER[1:]]

    def piece_load(n):
        q, start, end = pieces[n]
        cols = pl.ds(q * part + start, end - start)
        return train_query.at[:, cols], tq.at[:, cols]

    first, rest = pl.ds(0, part_of_high), pl.ds(part_of_high, rest_of_high)
    together = [
        [(low_query, lq), (high_query.at[:, first], hq.at[:, first]), piece_load(0)],
        [(high_query.at[:, rest], hq.at[:, rest]), piece_load(1), (train_key, tk), (low_key, lk)],
        [piece_load(2), (train_value, tv), (low_value, lv)],
        [piece_load(3)],
        [piece_load(4)],
        [(high_key, hk)],
        [(high_value, hv)],
        [(norm_train, nt)],
        [(norm_step, ns)],
    ]

    def start_loads(group):
        for src, dst in together[group]:
            pltpu.make_async_copy(src, dst, load_sem.at[group]).start()

    def wait_loads(group):
        if len(together[group]) == 1:
            src, dst = together[group][0]
        else:
            size = sum(dst.shape[0] * dst.shape[1] for _, dst in together[group])
            rows = pl.ds(0, size // wide)
            assert size % (8 * wide) == 0
            src, dst = train_query.at[rows], tq.at[rows]
        pltpu.make_async_copy(src, dst, load_sem.at[group]).wait()

    start_loads(0)
    greet()
    for group in (7, 8, 1, 5, 2, 6, 3, 4):
        start_loads(group)

    def merged(train, high, low):
        return train.astype(jnp.float32) + lax.dot_general(
            high, low, (((0,), (0,)), ((), ())), preferred_element_type=jnp.float32
        )

    def unit_copy(link, slot, what, rows=slice(None)):
        off, q = what
        unit = whole.at[me.at(off), q, rows]
        return remote(unit, unit, send_sem, recv_sem.at[GROUP_OF[slot]], me.neighbour(LINKS[link]))

    def send(link, slot, rows=slice(None)):
        unit_copy(link, slot, SENDS[link][slot], rows).start()

    def units(slots, sem):
        some = whole.at[pl.ds(0, slots * len(LINKS) // QUARTERS)]
        return remote(some, some, send_sem, sem, me.partner())

    def arrive(group):
        units(len(GROUPS[group]), recv_sem.at[group]).wait_recv()

    def only(core):
        return pl.when(me.core == LATE if core == LATE else me.core != LATE)

    def fresh_copy():
        return remote(fresh, ring.at[me.y * SIDE + me.z], small_send, small_recv.at[0], (me.y, me.col))

    def column_copy():
        part_of_ring = ring.at[pl.ds(me.y * SIDE, SIDE)]
        return remote(part_of_ring, part_of_ring, small_send, small_recv.at[1], (LEAD, me.col))

    def ring_lines(count, sem):
        some = ring.at[pl.ds(0, count)]
        return remote(some, some, small_send, sem, me.partner())

    def norm_copy(off):
        return remote(norm, norm, norm_send, small_recv.at[3], me.neighbour(off))

    def norm_sent(count):
        some = whole.at[0, 0, pl.ds(0, count * norm.shape[0] * norm.shape[1] // whole.shape[3])]
        remote(some, some, norm_send, small_recv.at[3], me.partner()).wait_send()

    def make_fresh():
        wait_loads(7)
        wait_loads(8)
        values = nt[...] + ns[...]
        fresh[...] = jnp.concatenate([values, values], axis=1)

    def send_fresh():
        @pl.when(top)
        def _():
            ring[me.y * SIDE + me.z] = fresh[...]

        @pl.when(jnp.logical_not(top))
        def _():
            fresh_copy().start()

    for n, (q, start, end) in enumerate(pieces):
        cols = pl.ds(q * part + start, end - start)
        wait_loads(n)
        if n == 1:
            make_fresh()
        whole[me.row, q, start:end, :] = merged(tq[:, cols].T, hq[:, cols], lq[...]).astype(whole.dtype)
        if n == 0:

            @pl.when(leader)
            def _():
                pl.semaphore_wait(barrier, len(peers) + n_planes - 1)

            far = (me.z == 2) | (top & (me.y == (LEAD + 2) % SIDE))

            @pl.when(far)
            def _():
                pl.semaphore_wait(barrier, len(peers) + 1)

            @pl.when(jnp.logical_not(leader | far))
            def _():
                pl.semaphore_wait(barrier, len(peers))

        if end == part:
            if n == 1:
                wait_loads(5)
            if n == 2:
                wait_loads(6)
            train, low, high = (tk, lk, hk) if q < 2 else (tv, lv, hv)
            small = merged(train[...], high[...], low[...]).astype(whole.dtype)
            half = small.shape[0] // 2
            whole[me.row, q, part:, :] = small[(q % 2) * half : (q % 2 + 1) * half, :]
        for link in range(len(LINKS)):
            if n == 0:
                send(link, 0, pl.ds(0, end))
            elif n == 1:
                send(link, 0, pl.ds(start, whole.shape[2] - start))
            else:
                send(link, ORDER.index(q))
        if n == 1:
            send_fresh()

    def norm_on_its_way(group):
        if group == 0:

            @pl.when(top)
            def _():
                ring_lines(len(column), small_recv.at[0]).wait_recv()

            @pl.when(head)
            def _():
                column_copy().start()

        if group == 1:

            @pl.when(leader)
            def _():
                ring_lines(len(heads) * SIDE, small_recv.at[1]).wait_recv()
                in_order = [ring[(i % SIDE) * SIDE + i // SIDE] for i in range(blocks)]
                lines[me.col] = jnp.concatenate(in_order, axis=0)
                for n in range(1, n_planes):
                    remote(lines.at[me.col], lines.at[me.col], small_send, small_recv.at[2], me.plane(n)).start()
                some = lines.at[pl.ds(0, n_planes - 1)]
                remote(some, some, small_send, small_recv.at[2], me.partner()).wait()
                lane = lax.broadcasted_iota(jnp.int32, lines.shape[1:], 1)
                for x in range(SIDE):
                    both = jnp.where(lane < lines.shape[2] // CORES, lines[CORES * x], lines[CORES * x + 1])
                    ordered[pl.Slice(x, blocks, SIDE), :] = both
                norm[...] = ordered[...].astype(norm.dtype)
                for off in heads + column:
                    norm_copy(off).start()

        if group == 2:

            @pl.when(head)
            def _():
                norm_copy((1, 0)).wait_recv()
                for off in column:
                    norm_copy(off).start()

    def send_slots(slots):
        for slot in slots:
            for link in range(len(LINKS)):
                send(link, slot)

    for group, slots in enumerate(AFTER):
        arrive(group)
        norm_on_its_way(group)
        if slots[0] < SPLIT:
            send_slots(slots)
        else:

            @only(1 - LATE)
            def _():
                send_slots(slots)

    arrive(5)

    @only(1 - LATE)
    def _():
        arrive(6)
        units(SLOTS, recv_sem.at[0]).wait_send()

    @only(LATE)
    def _():
        units(SPLIT, recv_sem.at[0]).wait_send()

    @pl.when(leader)
    def _():
        norm_sent(len(heads) + len(column))

    @pl.when(head)
    def _():
        column_copy().wait_send()
        norm_sent(len(column))

    @pl.when(jnp.logical_not(top))
    def _():
        fresh_copy().wait_send()
        norm_copy((1, 0)).wait_recv()


def finish_kernel(whole, token, rest, send_sem, recv_sem):
    del token
    me = Place()

    @pl.when(me.core == LATE)
    def _():
        barrier = pltpu.get_barrier_semaphore()
        signal_all(barrier, [me.neighbour(d) for d in LINKS])
        pl.semaphore_wait(barrier, len(LINKS))
        for link, slot in LAST:
            off, q = SENDS[link][slot]
            unit = whole.at[me.at(off), q]
            remote(unit, rest.at[link, slot - SPLIT], send_sem, recv_sem, me.neighbour(LINKS[link])).start()
        remote(rest, rest, send_sem, recv_sem, me.partner()).wait()


def write_unit(source, block, quarter, outs, sems, large=None):
    out_query, out_key, out_value = outs
    rows, depth = source.shape
    part = out_query.shape[0] // QUARTERS
    half = rows - part
    at = pl.ds(pl.multiple_of(block * depth, depth), depth)
    small = (out_key if quarter < 2 else out_value).at[pl.ds((quarter % 2) * half, half), at]
    if large is not False:
        query = out_query.at[pl.ds(quarter * part, part), at]
        pltpu.make_async_copy(source.at[pl.ds(0, part)], query, sems[0]).start()
    if large is not True:
        pltpu.make_async_copy(source.at[pl.ds(part, half)], small, sems[1 + quarter // 2]).start()


def wait_units(count, unit_bytes, out, sem):
    rows = count * unit_bytes // (out.shape[1] * out.dtype.itemsize)
    same = out.at[pl.ds(0, rows)]
    pltpu.make_async_copy(same, same, sem).wait()


def unit_bytes_of(whole):
    return whole.shape[-2] * whole.shape[-1] * whole.dtype.itemsize


def write_kernel(whole, out_query, out_key, out_value, token, sem):
    me = Place()
    outs = (out_query, out_key, out_value)
    token[...] = jnp.zeros_like(token)
    late = {arriving(*unit) for unit in LAST}

    @pl.when(me.core == LATE)
    def _():
        count = 0
        for off in [(dz, dy) for dz in range(SIDE) for dy in range(SIDE)]:
            for q in range(QUARTERS):
                if (off, q) not in late:
                    count += 1
                    block = me.at(off)
                    write_unit(whole.at[block, q], block, q, outs, (sem, sem, sem))
        wait_units(count, unit_bytes_of(whole), out_query, sem)


def write_rest_kernel(
    whole, rest, norm, in_query, in_key, in_value, out_query, out_key, out_value, out_norm, sem, norm_sem
):
    del in_query, in_key, in_value
    me = Place()
    outs = (out_query, out_key, out_value)
    norm_copy = pltpu.make_async_copy(norm, out_norm, norm_sem)
    norm_copy.start()

    @pl.when(me.core == LATE)
    def _():
        first = sem.at[0]
        for large in (True, False):
            for link, slot in LAST:
                off, q = arriving(link, slot)
                write_unit(rest.at[link, slot - SPLIT], me.at(off), q, outs, (first, first, first), large)
        wait_units(len(LAST), unit_bytes_of(whole), out_query, first)

    @pl.when(me.core != LATE)
    def _():
        @pl.loop(0, whole.shape[0])
        def _(block):
            for q in range(QUARTERS):
                write_unit(whole.at[block, q], block, q, outs, [sem.at[n] for n in range(len(outs))])

        for n, out in enumerate(outs):
            pltpu.make_async_copy(out, out, sem.at[n]).wait()

    norm_copy.wait()


def body(
    train_query, low_query, high_query,
    train_key, low_key, high_key,
    train_value, low_value, high_value,
    norm_train, norm_step,
):
    n_rows, n_cols = lax.axis_size("rows"), lax.axis_size("cols")
    depth, wide = train_query.shape
    tall = train_key.shape[1]
    rank = low_query.shape[1]
    unit = (wide + 2 * tall) // QUARTERS
    values = norm_train.shape[0]
    line = CORES * values
    dtype = train_query.dtype
    f32 = jnp.float32
    anywhere = pl.BlockSpec(memory_space=pl.ANY)
    vmem = pl.BlockSpec(memory_space=pltpu.VMEM)
    dma = pltpu.SemaphoreType.DMA
    shape = jax.ShapeDtypeStruct

    def pin(space, *arrays):
        return [pltpu.with_memory_space_constraint(a, space) for a in arrays]

    whole, norm = pl.pallas_call(
        gather_kernel,
        out_shape=(
            shape((n_rows, QUARTERS, unit, depth), dtype),
            shape((n_rows * n_cols // CORES, line), dtype),
        ),
        in_specs=[anywhere] * 11,
        out_specs=(vmem, vmem),
        scratch_shapes=[
            pltpu.VMEM((depth, wide), dtype),
            pltpu.VMEM((rank, depth), dtype),
            pltpu.VMEM((rank, wide), dtype),
            pltpu.VMEM((tall, depth), dtype),
            pltpu.VMEM((rank, depth), dtype),
            pltpu.VMEM((rank, tall), dtype),
            pltpu.VMEM((tall, depth), dtype),
            pltpu.VMEM((rank, depth), dtype),
            pltpu.VMEM((rank, tall), dtype),
            pltpu.VMEM((1, values), f32),
            pltpu.VMEM((1, values), f32),
            pltpu.VMEM((1, line), f32),
            pltpu.VMEM((n_rows, 1, line), f32),
            pltpu.VMEM((n_cols, n_rows, line), f32),
            pltpu.VMEM((SIDE * n_rows, line), f32),
            dma((9,)),
            dma(()),
            dma((len(GROUPS),)),
            dma(()),
            dma((4,)),
            dma(()),
        ],
        compiler_params=pltpu.CompilerParams(
            collective_id=0, has_side_effects=True, vmem_limit_bytes=24 * 2**20
        ),
        name="gather",
    )(
        *pin(
            pltpu.HBM,
            train_query, low_query.T, high_query,
            train_key.T, low_key.T, high_key,
            train_value.T, low_value.T, high_value,
            norm_train.reshape(1, -1), norm_step.reshape(1, -1),
        )
    )
    outs = [shape((wide, n_rows * depth), dtype)] + [shape((tall, n_rows * depth), dtype)] * 2
    out_query, out_key, out_value, token = pl.pallas_call(
        write_kernel,
        out_shape=(*outs, shape((8, 128), f32)),
        in_specs=[vmem],
        out_specs=[anywhere] * 3 + [vmem],
        scratch_shapes=[dma(())],
        compiler_params=pltpu.CompilerParams(vmem_limit_bytes=4 * 2**20),
        name="write",
    )(*pin(pltpu.VMEM, whole))
    (rest,) = pl.pallas_call(
        finish_kernel,
        out_shape=(shape((len(LINKS), SLOTS - SPLIT, unit, depth), dtype),),
        in_specs=[vmem] * 2,
        out_specs=(vmem,),
        scratch_shapes=[dma(()), dma(())],
        compiler_params=pltpu.CompilerParams(
            collective_id=1, has_side_effects=True, vmem_limit_bytes=8 * 2**20
        ),
        name="finish",
    )(*pin(pltpu.VMEM, whole, token))
    out_query, out_key, out_value, out_norm = pl.pallas_call(
        write_rest_kernel,
        out_shape=(*outs, shape(norm.shape, dtype)),
        in_specs=[vmem] * 3 + [anywhere] * 3,
        out_specs=[anywhere] * 4,
        input_output_aliases={3: 0, 4: 1, 5: 2},
        scratch_shapes=[dma((len(outs),)), dma(())],
        compiler_params=pltpu.CompilerParams(vmem_limit_bytes=4 * 2**20),
        name="write_rest",
    )(*pin(pltpu.VMEM, whole, rest, norm), *pin(pltpu.HBM, out_query, out_key, out_value))
    return out_query, out_key, out_value, out_norm.reshape(-1)


def solution(mesh):
    return jax.shard_map(
        body,
        mesh=mesh,
        in_specs=(
            P("rows", "cols"),
            P("rows", None),
            P(None, "cols"),
            P("rows", "cols"),
            P("rows", None),
            P(None, "cols"),
            P("rows", "cols"),
            P("rows", None),
            P(None, "cols"),
            P(("rows", "cols")),
            P(("rows", "cols")),
        ),
        out_specs=(P("cols", None), P("cols", None), P("cols", None), P()),
        check_vma=False,
    )
```
